256 devices in a mesh: rows: 32 (over z, x_lo, core), cols: 8 (over y, x_hi).
Axes of the slice: x: 4 (x_hi: 2, x_lo: 2; x = x_hi * 2 + x_lo), y: 4, z: 8, core: 2. Of those that a mesh axis runs over, the one named last changes fastest.
Arguments:
- kets: float32 [32, 16, 32], P('rows', 'cols'), may hold values from -3 to 3
- left_maps: float32 [2, 32, 16, 96, 384], P(None, 'rows', 'cols'), may hold values from -0.3125 to 0.3125
- right_maps: float32 [2, 32, 16, 96, 384], P(None, 'rows', 'cols'), may hold values from -0.3125 to 0.3125
- top_edge: float32 [16, 96, 384], P('cols'), may hold values from -6 to 6
- bottom_edge: float32 [16, 96, 384], P('cols'), may hold values from -6 to 6
- left_edge: float32 [32, 96, 384], P('rows'), may hold values from -6 to 6
- right_edge: float32 [32, 96, 384], P('rows'), may hold values from -6 to 6
- term_rows: int32 [16], replicated, may hold values from 0 to 31
- term_bonds: int32 [16], replicated, may hold values from 0 to 14
- term_ops: int32 [16], replicated, may hold values from 0 to 3
- operators: float32 [4, 16], replicated, may hold values from -6 to 6
Outputs:
- top_out: float32 [32, 16, 96, 384], P('rows', 'cols')
- bottom_out: float32 [32, 16, 96, 384], P('rows', 'cols')
- energies: float32 [16], replicated
The draws below stay inside these ranges and needn't reach their ends.
Inputs may be any that keep to these rules, and one draw needn't show every extreme that they name: Term t acts on the bond between columns term_bonds[t] and term_bonds[t] + 1 of row term_rows[t].
All inputs are finite; a program needn't handle non-finite values.
Results may differ from the reference program's by a relative error of at most 0.0003.
Values sent between devices are 32-bit elements; how exact they have to be, the bound alone decides.
A program may use at most 64 MiB of HBM per device.

```python
import jax
import jax.numpy as jnp
from jax import lax

D = 2
D2 = 4
PHYS = 2
CHI = 96
OPS = 4
TERMS = 16
NR = 32
NC = 16


def set_ends(array, rng, least, top_value):
    index_at = [jax.random.randint(jax.random.fold_in(rng, axis), (), 0, length) for axis, length in enumerate(array.shape)]
    widest = array.shape.index(max(array.shape))
    beside = index_at[:widest] + [(index_at[widest] + 1) % array.shape[widest]] + index_at[widest + 1:]
    return array.at[tuple(index_at)].set(least).at[tuple(beside)].set(top_value)


def levels(stream_key, shape, pieces, least, largest):
    factor_of = 1.0
    for axis_at, parts in pieces:
        draws = jax.random.uniform(jax.random.fold_in(jax.random.fold_in(stream_key, 6), axis_at), (parts,), jnp.float32, least / len(pieces), largest / len(pieces))
        factor_of = factor_of * jnp.repeat(jnp.exp(draws), shape[axis_at] // parts).reshape((-1,) + (1,) * (len(shape) - 1 - axis_at))
    return factor_of


def gaussian(key, dims, scale, most, shards=(), kind=jnp.bfloat16):
    entries = jax.random.normal(key, dims, jnp.float32) * scale
    if len(shards) > 0:
        entries = levels(key, dims, shards, -0.22, 0.18) * entries
    return jnp.clip(entries, min=-most, max=most).astype(kind)


def setup_inputs(seed: int = 0) -> dict:
    key_list = jax.random.split(jax.random.key(seed), 12)
    kets = gaussian(key_list[0], (NR, NC, PHYS * D**4), 0.5, 3.0, ((0, 32), (1, 8)), jnp.float32)
    left_maps = gaussian(key_list[1], (2, NR, NC, CHI, CHI * D2), (CHI * D2) ** -0.5, 0.3125, ((1, 32), (2, 8)), jnp.float32)
    right_maps = gaussian(key_list[2], (2, NR, NC, CHI, CHI * D2), (CHI * D2) ** -0.5, 0.3125, ((1, 32), (2, 8)), jnp.float32)
    top_edge = gaussian(key_list[3], (NC, CHI, D2 * CHI), 1.0, 6.0, ((0, 8),), jnp.float32)
    bottom_edge = gaussian(key_list[4], (NC, CHI, D2 * CHI), 1.0, 6.0, ((0, 8),), jnp.float32)
    left_edge = gaussian(key_list[5], (NR, CHI, D2 * CHI), 1.0, 6.0, ((0, 32),), jnp.float32)
    right_edge = gaussian(key_list[6], (NR, CHI, D2 * CHI), 1.0, 6.0, ((0, 32),), jnp.float32)
    term_rows = set_ends(jax.random.randint(key_list[7], (TERMS,), 0, NR), jax.random.fold_in(key_list[7], 1), 0, NR - 1).astype(jnp.int32)
    term_bonds = set_ends(jax.random.randint(key_list[8], (TERMS,), 0, NC - 1), jax.random.fold_in(key_list[8], 1), 0, (NC - 1) - 1).astype(jnp.int32)
    term_ops = set_ends(jax.random.randint(key_list[9], (TERMS,), 0, OPS), jax.random.fold_in(key_list[9], 1), 0, OPS - 1).astype(jnp.int32)
    operators = gaussian(key_list[10], (OPS, PHYS**4), 1.0, 6.0, (), jnp.float32)
    return dict(kets=kets, left_maps=left_maps, right_maps=right_maps, top_edge=top_edge, bottom_edge=bottom_edge, left_edge=left_edge, right_edge=right_edge, term_rows=term_rows, term_bonds=term_bonds, term_ops=term_ops, operators=operators)


EPSILON = 1e-06
PRECISION_HIGH = lax.Precision.HIGHEST

def product(pattern, former, latter):
    return jnp.einsum(pattern, former, latter, precision=PRECISION_HIGH, preferred_element_type=jnp.float32)

def normalize(values):
    return values / jnp.sqrt(jnp.mean(values * values) + EPSILON)

def select_at(values, position):
    return lax.dynamic_index_in_dim(values, position, 0, keepdims=False)

def pair_layers(ket_flat):
    tensor = ket_flat.reshape(PHYS, D, D, D, D)
    doubled = product('pabcd,pefgh->aebfcgdh', tensor, tensor)
    return doubled.reshape(D2, D2, D2, D2)

def open_layers(ket_flat):
    tensor = ket_flat.reshape(PHYS, D, D, D, D)
    doubled = product('pabcd,qefgh->pqaebfcgdh', tensor, tensor)
    return doubled.reshape(PHYS * PHYS, D2, D2, D2, D2)

def pair_diagonal():
    matched = jnp.arange(PHYS)[:, None] == jnp.arange(PHYS)[None, :]
    return jnp.where(matched, 1.0, 0.0).astype(jnp.float32).reshape(PHYS * PHYS)

def absorb_down(boundary, layers, left_map, right_map):
    above_col = boundary.reshape(CHI, D2, CHI)
    left_three = left_map.reshape(CHI, CHI, D2)
    right_three = right_map.reshape(CHI, CHI, D2)
    joined = product('aub,cbr->aurc', above_col, right_three)
    through = product('aurc,uldr->aldc', joined, layers)
    renewed = product('xal,aldc->xdc', left_three, through)
    return normalize(renewed.reshape(CHI, D2 * CHI))

def absorb_up(boundary, layers, left_map, right_map):
    below_col = boundary.reshape(CHI, D2, CHI)
    left_three = left_map.reshape(CHI, CHI, D2)
    right_three = right_map.reshape(CHI, CHI, D2)
    joined = product('adb,cbr->adrc', below_col, right_three)
    through = product('adrc,uldr->aluc', joined, layers)
    renewed = product('xal,aluc->xuc', left_three, through)
    return normalize(renewed.reshape(CHI, D2 * CHI))

def left_core(environ, layers, above_col, below_col):
    env_three = environ.reshape(CHI, D2, CHI)
    upper_three = above_col.reshape(CHI, D2, CHI)
    lower_three = below_col.reshape(CHI, D2, CHI)
    step_one = product('alb,aux->lbux', env_three, upper_three)
    step_two = product('lbux,uldr->bxdr', step_one, layers)
    return product('bxdr,bdy->xry', step_two, lower_three).reshape(CHI, D2 * CHI)

def right_core(environ, layers, above_col, below_col):
    env_three = environ.reshape(CHI, D2, CHI)
    upper_three = above_col.reshape(CHI, D2, CHI)
    lower_three = below_col.reshape(CHI, D2, CHI)
    step_one = product('xry,aux->ryau', env_three, upper_three)
    step_two = product('ryau,uldr->yald', step_one, layers)
    return product('yald,bdy->alb', step_two, lower_three).reshape(CHI, D2 * CHI)

def reference(kets, left_maps, right_maps, top_edge, bottom_edge, left_edge, right_edge, term_rows, term_bonds, term_ops, operators):
    layers = jax.vmap(jax.vmap(pair_layers))(kets)

    def down_row(carried, inputs):
        renewed = jax.vmap(absorb_down)(carried, inputs[0], inputs[1], inputs[2])
        return (renewed, renewed)

    def up_row(carried, inputs):
        renewed = jax.vmap(absorb_up)(carried, inputs[0], inputs[1], inputs[2])
        return (renewed, renewed)
    unused_top, top_out = lax.scan(down_row, top_edge, (layers, left_maps[0], right_maps[0]))
    unused_bottom, bottom_out = lax.scan(up_row, bottom_edge, (layers, left_maps[1], right_maps[1]), reverse=True)
    above = jnp.concatenate([top_edge[None], top_out[:-1]], axis=0)
    below = jnp.concatenate([bottom_out[1:], bottom_edge[None]], axis=0)
    diagonal = pair_diagonal()
    weights = jnp.outer(diagonal, diagonal).reshape(-1)

    def one_term(term_index):
        term_row = select_at(term_rows, term_index).astype(jnp.int32)
        term_bond = select_at(term_bonds, term_index).astype(jnp.int32)
        row_layers = select_at(layers, term_row)
        row_kets = select_at(kets, term_row)
        row_above = select_at(above, term_row)
        row_below = select_at(below, term_row)

        def left_walk(column, environ):
            return normalize(left_core(environ, select_at(row_layers, column), select_at(row_above, column), select_at(row_below, column)))

        def right_walk(step_count, environ):
            column = (NC - 1 - step_count).astype(jnp.int32)
            return normalize(right_core(environ, select_at(row_layers, column), select_at(row_above, column), select_at(row_below, column)))
        left_env = lax.fori_loop(0, term_bond, left_walk, select_at(left_edge, term_row))
        right_env = lax.fori_loop(0, NC - 2 - term_bond, right_walk, select_at(right_edge, term_row))
        right_col = (term_bond + 1).astype(jnp.int32)
        open_left = lax.map(lambda single: left_core(left_env, single, select_at(row_above, term_bond), select_at(row_below, term_bond)), open_layers(select_at(row_kets, term_bond)))
        open_right = lax.map(lambda single: right_core(right_env, single, select_at(row_above, right_col), select_at(row_below, right_col)), open_layers(select_at(row_kets, right_col)))
        density = product('pz,qz->pq', open_left.reshape(PHYS * PHYS, -1), open_right.reshape(PHYS * PHYS, -1)).reshape(-1)
        trace_value = jnp.sum(density * weights)
        spread = jnp.sqrt(jnp.sum(density * density))
        denominator = jnp.maximum(jnp.abs(trace_value), 0.25 * spread)
        chosen_op = select_at(operators, select_at(term_ops, term_index).astype(jnp.int32))
        return jnp.sum(density * chosen_op) / denominator
    energies = lax.map(one_term, jnp.arange(TERMS, dtype=jnp.int32))
    return (top_out, bottom_out, energies)
```

```python
import functools

import jax
import jax.numpy as jnp
from jax import lax
from jax.experimental import pallas as pl
from jax.experimental.pallas import tpu as pltpu
from jax.sharding import Mesh
from jax.sharding import PartitionSpec as P

D = 2
D2 = 4
PHYS = 2
CHI = 96
WIDE = D2 * CHI
OPS = 4
TERMS = 16
GROUP = 4
ROWS = ("rows_0", "rows_1", "rows_2")
COLS = ("cols_0", "cols_1")
ROWS_COLS = ("rows_0", "rows_1", "rows_2", "cols_0", "cols_1")
MESH = pl.DeviceIdType.MESH

EPSILON = 1e-06
PRECISION_HIGH = lax.Precision.HIGHEST
F32 = jnp.float32
BF16 = jnp.bfloat16


def iota(shape, dim):
    return lax.broadcasted_iota(jnp.int32, shape, dim)


def halves(value):
    high = value.astype(BF16)
    low = (value - high.astype(F32)).astype(BF16)
    return high, low


def dot(left, right):
    return jnp.dot(left, right, preferred_element_type=F32)


def dot_nt(left, right):
    return lax.dot_general(left, right, (((1,), (1,)), ((), ())), preferred_element_type=F32)


def unpack(wide):
    one, two, three = wide[:, 0:128], wide[:, 128:256], wide[:, 256:384]
    lane = iota((CHI, 128), 1)
    parts = (
        one,
        pltpu.roll(jnp.where(lane >= 96, one, two), 32, 1),
        pltpu.roll(jnp.where(lane >= 64, two, three), 64, 1),
        pltpu.roll(three, 96, 1),
    )
    return [jnp.where(lane < CHI, part, 0.0) for part in parts]


def pack(tiles):
    lane = iota((CHI, 128), 1)
    first = tiles[0]
    second = pltpu.roll(tiles[1], 96, 1)
    third = pltpu.roll(tiles[2], 64, 1)
    fourth = pltpu.roll(tiles[3], 32, 1)
    return jnp.concatenate(
        [
            jnp.where(lane < 96, first, second),
            jnp.where(lane < 64, second, third),
            jnp.where(lane < 32, third, fourth),
        ],
        axis=1,
    )


def pick(mode, *choices):
    value = choices[-1]
    for index in range(len(choices) - 1):
        value = jnp.where(mode == index, choices[index], value)
    return value


def layer_rows(ket, legs):
    shape = (PHYS * 256, 32)
    row, col = iota(shape, 0), iota(shape, 1)
    digits = ((row >> 6) & 3, (row >> 4) & 3, (row >> 2) & 3, row & 3)
    up, left, down, right = legs(*digits)
    base = (row >> 8) * 16
    ket_at = base + (up >> 1) * 8 + (left >> 1) * 4 + (down >> 1) * 2 + (right >> 1)
    bra_at = base + (up & 1) * 8 + (left & 1) * 4 + (down & 1) * 2 + (right & 1)
    take = functools.partial(jnp.dot, precision=PRECISION_HIGH, preferred_element_type=F32)
    kets = take(jnp.where(col == ket_at, 1.0, 0.0), ket)
    bras = take(jnp.where(col == bra_at, 1.0, 0.0), ket)
    both = kets * bras
    full = both[0:256] + both[256:512]
    lane = iota((64, 128), 1)
    at = [full[64 * m : 64 * (m + 1)] for m in range(4)]
    return jnp.concatenate(
        [
            jnp.where(lane < 96, at[0], at[1]),
            jnp.where(lane < 64, at[1], at[2]),
            jnp.where(lane < 32, at[2], at[3]),
        ],
        axis=1,
    )


def thirds(value):
    high = value.astype(BF16)
    rest = value - high.astype(F32)
    middle = rest.astype(BF16)
    low = (rest - middle.astype(F32)).astype(BF16)
    return high, middle, low


def fold_first(spread, coeffs, folded, slot):
    def body(index, carried):
        total = None
        for leg in range(4):
            term = coeffs[pl.ds(index * 4 + leg, 1), :] * spread[leg]
            total = term if total is None else total + term
        high, middle, low = thirds(total)
        rows = pl.ds(pl.multiple_of(index * CHI, CHI), CHI)
        folded[slot, rows, 0:WIDE] = low
        folded[slot, rows, WIDE : 2 * WIDE] = high
        folded[slot, rows, 2 * WIDE : 3 * WIDE] = middle
        return carried

    lax.fori_loop(0, 16, body, 0)


def padded(parts):
    blank = jnp.zeros((32, parts[0].shape[1]), BF16)
    return jnp.concatenate([piece for part in parts for piece in (part, blank)], axis=0)


def apply_layer(state, scale, folded, second, third, slot, middle):
    high, mid, low = thirds(state)
    once = jnp.concatenate([high, mid], axis=1)
    main = jnp.concatenate([once, once], axis=0)
    fine = jnp.concatenate([high, low], axis=0)
    for leg in range(4):
        rows = slice(leg * WIDE, (leg + 1) * WIDE)
        wide = dot(folded[slot, rows, WIDE : 3 * WIDE], main)
        rest = dot(folded[slot, rows, 0 : 2 * WIDE], fine)
        high, mid, low = thirds(wide[:, 0:128] + (wide[:, 128:256] + rest))
        for index, part in enumerate((high, mid)):
            middle[:, leg * 256 + index * 128 : leg * 256 + index * 128 + 128] = part
        for index, part in enumerate((high, low)):
            begin = 1024 + leg * 256 + index * 128
            middle[:, begin : begin + 128] = part
    wide = dot(middle[:, 0:1024], second[slot])
    rest = dot(middle[:, 1024:2048], third[slot])
    return (wide[:, 0:128] + (wide[:, 128:256] + rest)) * scale


def nrm_scale(state):
    total = jnp.sum(jnp.sum(state * state, axis=0, keepdims=True), axis=1, keepdims=True)
    return lax.rsqrt(total * (1.0 / (CHI * WIDE)) + EPSILON)


def boundary_kernel(
    kets,
    left_maps,
    right_maps,
    top_edge,
    bottom_edge,
    outs,
    sides,
    lefts,
    rights,
    ketses,
    select_one,
    select_two,
    spread,
    coeffs,
    folded,
    second,
    third,
    middle,
    entered,
    leaving,
    state,
    normed,
    map_send,
    map_recv,
    hop_send,
    hop_recv,
    row_send,
    out_recv,
    side_recv,
):
    z = lax.axis_index("rows_0")
    xl = lax.axis_index("rows_1")
    core = lax.axis_index("rows_2")
    y = lax.axis_index("cols_0")
    xh = lax.axis_index("cols_1")
    planes = lax.axis_size("rows_0")
    mine = xl * 2 + core
    col = xl
    way = (core + z) % 2
    place = xh * 2 + col
    is_first = ((way == 0) & (z == 0)) | ((way == 1) & (z == planes - 1))
    is_last = ((way == 0) & (z == planes - 1)) | ((way == 1) & (z == 0))
    after_z = z + 1 - 2 * way
    after = (jnp.clip(after_z, 0, planes - 1), xl, (way + after_z + 2) % 2, y, xh)

    barrier = pltpu.get_barrier_semaphore()

    def greet(device):
        pl.semaphore_signal(barrier, inc=1, device_id=device, device_id_type=MESH)

    for step in range(1, GROUP):
        other = (mine + step) % GROUP
        greet((z, other // 2, other % 2, y, xh))
    for other in range(GROUP):
        greet((z, other // 2, other % 2, y, 1 - xh))

    for step in (1, planes - 1):
        near = (z + step) % planes
        greet((near, xl, (way + near) % 2, y, xh))

    pl.semaphore_wait(barrier, 9)

    def map_copies(step):
        other = (mine + step) % GROUP
        other_col = other // 2
        other_way = (other % 2 + z) % 2
        pairs = (
            (left_maps.at[other_way, 0, other_col], lefts),
            (right_maps.at[other_way, 0, other_col], rights),
            (kets.at[other_col], ketses),
        )
        device = (z, other // 2, other % 2, y, xh)
        return [
            pltpu.make_async_remote_copy(
                src_ref=source,
                dst_ref=target.at[mine],
                send_sem=map_send.at[step - 1, kind],
                recv_sem=map_recv.at[mine, kind],
                device_id=device,
                device_id_type=MESH,
            )
            for kind, (source, target) in enumerate(pairs)
        ]

    own_pairs = (
        (left_maps.at[way, 0, col], lefts),
        (right_maps.at[way, 0, col], rights),
        (kets.at[col], ketses),
    )
    for kind, (source, target) in enumerate(own_pairs):
        pltpu.make_async_copy(source, target.at[mine], map_recv.at[mine, kind]).start()
    for step in range(1, GROUP):
        for copy in map_copies(step):
            copy.start()

    for leg in range(4):
        row, lane = iota((WIDE, WIDE), 0), iota((WIDE, WIDE), 1)
        within = lane
        for _ in range(3):
            within = jnp.where(within >= CHI, within - CHI, within)
        select_one[:, leg * WIDE : (leg + 1) * WIDE] = jnp.where(
            row == 4 * within + leg, 1.0, 0.0
        ).astype(BF16)
        row, lane = iota((256, WIDE), 0), iota((256, WIDE), 1)
        inner = row & 127
        select_two[leg * 256 : (leg + 1) * 256, :] = jnp.where(
            (lane == 4 * inner + leg) & (inner < CHI), 1.0, 0.0
        ).astype(BF16)

    @pl.when(is_first & (way == 0))
    def _():
        entered[...] = top_edge[col]

    @pl.when(is_first & (way == 1))
    def _():
        entered[...] = bottom_edge[col]

    def row_at(number):
        return number + way * (GROUP - 1 - 2 * number)

    def legs(m, g, o, f):
        return pick(way, m, o), f, pick(way, o, m), g

    def prepare(number):
        j = row_at(number)
        for kind, target in enumerate((lefts, rights, ketses)):
            pltpu.make_async_copy(target.at[j], target.at[j], map_recv.at[j, kind]).wait()
        coeffs[...] = layer_rows(ketses[j], legs)
        apart = dot(jnp.concatenate(thirds(lefts[j]), axis=0), select_one[...])
        for leg in range(4):
            lanes = slice(leg * WIDE, (leg + 1) * WIDE)
            spread[leg] = apart[0:CHI, lanes] + (
                apart[CHI : 2 * CHI, lanes] + apart[2 * CHI : 3 * CHI, lanes]
            )
        fold_first(spread, coeffs, folded, number)
        high, mid, low = thirds(rights[j])
        main = dot_nt(select_two[...], padded((high, mid)))
        fine = dot_nt(select_two[...], padded((low,)))
        second[number] = main.astype(BF16)
        even = (iota((1024, 128), 0) & 128) == 0
        third[number] = jnp.where(even, fine, main[:, 0:128]).astype(BF16)

    def send_row(number, source, target_of, recv, xh_to, j, kind):
        here = (j == mine) & (xh_to == xh)

        @pl.when(here)
        def _():
            pltpu.make_async_copy(source, target_of, recv).start()

        @pl.when(jnp.logical_not(here))
        def _():
            row_copy(number, source, target_of, recv, xh_to, j, kind).start()

    def row_copy(number, source, target_of, recv, xh_to, j, kind):
        return pltpu.make_async_remote_copy(
            src_ref=source,
            dst_ref=target_of,
            send_sem=row_send.at[number, kind],
            recv_sem=recv,
            device_id=(z, j // 2, j % 2, y, xh_to),
            device_id_type=MESH,
        )

    def side_args(number, xh_to, kind):
        return (
            number,
            normed.at[number],
            sides.at[way, place],
            side_recv.at[way, place],
            xh_to,
            row_at(number),
            kind,
        )

    def out_args(number):
        return (
            number,
            normed.at[number + 1],
            outs.at[way, col],
            out_recv.at[way, col],
            xh,
            row_at(number),
            2,
        )

    def advance(number):
        @pl.when(number == 0)
        def _():
            @pl.when(jnp.logical_not(is_first))
            def _():
                pltpu.make_async_copy(entered, entered, hop_recv).wait()

            for leg, tile in enumerate(unpack(entered[...])):
                state[leg * CHI : (leg + 1) * CHI, :] = tile

        current = state[...]
        raw = is_first & (number == 0)
        scale = jnp.where(raw, 1.0, nrm_scale(current))
        renewed = apply_layer(current, scale, folded, second, third, number, middle)
        state[...] = renewed

        @pl.when(number == GROUP - 1)
        def _():
            leaving[...] = pack([renewed[leg * CHI : (leg + 1) * CHI] for leg in range(4)])

            @pl.when(jnp.logical_not(is_last))
            def _():
                hop().start()

        kept = pack([current[leg * CHI : (leg + 1) * CHI] for leg in range(4)])
        normed[number] = kept * scale
        send_row(*side_args(number, xh, 0))
        send_row(*side_args(number, 1 - xh, 1))

        @pl.when(number > 0)
        def _():
            send_row(*out_args(number - 1))

    def hop():
        return pltpu.make_async_remote_copy(
            src_ref=leaving,
            dst_ref=entered,
            send_sem=hop_send,
            recv_sem=hop_recv,
            device_id=after,
            device_id_type=MESH,
        )

    def task(index, carried):
        early = is_first
        is_prepare = (early & (index % 2 == 0)) | (jnp.logical_not(early) & (index < GROUP))

        @pl.when(is_prepare)
        def _():
            prepare(jnp.where(early, index // 2, jnp.minimum(index, GROUP - 1)))

        @pl.when(jnp.logical_not(is_prepare))
        def _():
            advance(jnp.where(early, index // 2, jnp.maximum(index - GROUP, 0)))

        return carried

    lax.fori_loop(0, 2 * GROUP, task, 0)

    final = state[...]
    normed[GROUP] = leaving[...] * nrm_scale(final)
    send_row(*out_args(GROUP - 1))

    for step in range(1, GROUP):
        for copy in map_copies(step):
            copy.wait_send()

    @pl.when(jnp.logical_not(is_last))
    def _():
        hop().wait_send()

    for number in range(GROUP):
        row_copy(*side_args(number, 1 - xh, 1)).wait_send()

        @pl.when(row_at(number) != mine)
        def _():
            row_copy(*side_args(number, xh, 0)).wait_send()
            row_copy(*out_args(number)).wait_send()

    for direction in range(2):
        for column in range(2):
            target = outs.at[direction, column]
            pltpu.make_async_copy(target, target, out_recv.at[direction, column]).wait()
        for column in range(4):
            target = sides.at[direction, column]
            pltpu.make_async_copy(target, target, side_recv.at[direction, column]).wait()


def run_boundary(kets, left_maps, right_maps, top_edge, bottom_edge):
    vmem = pl.BlockSpec(memory_space=pltpu.VMEM)
    column = (CHI, WIDE)
    return pl.pallas_call(
        boundary_kernel,
        out_shape=(
            jax.ShapeDtypeStruct((2, 2) + column, F32),
            jax.ShapeDtypeStruct((2, 4) + column, F32),
        ),
        in_specs=[vmem] * 5,
        out_specs=(vmem, vmem),
        scratch_shapes=[
            pltpu.VMEM((GROUP,) + column, F32),
            pltpu.VMEM((GROUP,) + column, F32),
            pltpu.VMEM((GROUP, 32, 128), F32),
            pltpu.VMEM((WIDE, 4 * WIDE), BF16),
            pltpu.VMEM((1024, WIDE), BF16),
            pltpu.VMEM((4,) + column, F32),
            pltpu.VMEM((64, WIDE), F32),
            pltpu.VMEM((GROUP, 16 * CHI, 3 * WIDE), BF16),
            pltpu.VMEM((GROUP, 1024, 256), BF16),
            pltpu.VMEM((GROUP, 1024, 128), BF16),
            pltpu.VMEM((WIDE, 2048), BF16),
            pltpu.VMEM(column, F32),
            pltpu.VMEM(column, F32),
            pltpu.VMEM((WIDE, 128), F32),
            pltpu.VMEM((GROUP + 1,) + column, F32),
            pltpu.SemaphoreType.DMA((GROUP - 1, 3)),
            pltpu.SemaphoreType.DMA((GROUP, 3)),
            pltpu.SemaphoreType.DMA,
            pltpu.SemaphoreType.DMA,
            pltpu.SemaphoreType.DMA((GROUP, 3)),
            pltpu.SemaphoreType.DMA((2, 2)),
            pltpu.SemaphoreType.DMA((2, 4)),
        ],
        compiler_params=pltpu.CompilerParams(
            collective_id=0, has_side_effects=True, vmem_limit_bytes=48 * 1024 * 1024
        ),
        name="boundary",
    )(kets, left_maps, right_maps, top_edge, bottom_edge)


def shifted(value, axis, steps):
    count = lax.axis_size(axis)
    initial, last = (max(0, -steps), min(count, count - steps))
    return lax.ppermute(value, axis, [(source, source + steps) for source in range(initial, last)])


def over_axes(value, axes):
    for axis in axes:
        value = lax.psum(value, axis)
    return value


def product(pattern, former, latter):
    return jnp.einsum(
        pattern, former, latter, precision=PRECISION_HIGH, preferred_element_type=jnp.float32
    )


def normalize(values):
    return values / jnp.sqrt(jnp.mean(values * values) + EPSILON)


def pair_layers(ket_flat):
    tensor = ket_flat.reshape(PHYS, D, D, D, D)
    doubled = product("pabcd,pefgh->aebfcgdh", tensor, tensor)
    return doubled.reshape(D2, D2, D2, D2)


def open_layers(ket_flat):
    tensor = ket_flat.reshape(PHYS, D, D, D, D)
    doubled = product("pabcd,qefgh->pqaebfcgdh", tensor, tensor)
    return doubled.reshape(PHYS * PHYS, D2, D2, D2, D2)


def pair_diagonal():
    matched = jnp.arange(PHYS)[:, None] == jnp.arange(PHYS)[None, :]
    return jnp.where(matched, 1.0, 0.0).astype(jnp.float32).reshape(PHYS * PHYS)


def left_core(environ, layers, above_col, below_col):
    env_three = environ.reshape(CHI, D2, CHI)
    upper_three = above_col.reshape(CHI, D2, CHI)
    lower_three = below_col.reshape(CHI, D2, CHI)
    step_one = product("alb,aux->lbux", env_three, upper_three)
    step_two = product("lbux,uldr->bxdr", step_one, layers)
    return product("bxdr,bdy->xry", step_two, lower_three).reshape(CHI, D2 * CHI)


def right_core(environ, layers, above_col, below_col):
    env_three = environ.reshape(CHI, D2, CHI)
    upper_three = above_col.reshape(CHI, D2, CHI)
    lower_three = below_col.reshape(CHI, D2, CHI)
    step_one = product("xry,aux->ryau", env_three, upper_three)
    step_two = product("ryau,uldr->yald", step_one, layers)
    return product("yald,bdy->alb", step_two, lower_three).reshape(CHI, D2 * CHI)


def side_step(core_map, environ, ket_flat, layers, above_col, below_col, wanted):

    def with_open(unused):
        opened = lax.map(
            lambda single: core_map(environ, single, above_col, below_col), open_layers(ket_flat)
        )
        closed = jnp.sum(pair_diagonal()[:, None, None] * opened, axis=0)
        return (opened, normalize(closed))

    def without_open(unused):
        empty_open = jnp.zeros((PHYS * PHYS, CHI, D2 * CHI), jnp.float32)
        return (empty_open, normalize(core_map(environ, layers, above_col, below_col)))

    return lax.cond(wanted, with_open, without_open, 0)


def shards(
    kets,
    left_maps,
    right_maps,
    top_edge,
    bottom_edge,
    left_edge,
    right_edge,
    term_rows,
    term_bonds,
    term_ops,
    operators,
):
    row_place = lax.axis_index(ROWS)
    col_count = lax.axis_size(COLS)
    col_place = lax.axis_index(COLS)
    local_rows = kets.shape[0]
    local_cols = kets.shape[1]
    layers = jax.vmap(jax.vmap(pair_layers))(kets)
    column_shape = (CHI, D2 * CHI)
    spread_kets = jnp.broadcast_to(kets[0][:, :, None], (local_cols, 32, 128))
    outs, sides = run_boundary(spread_kets, left_maps, right_maps, top_edge, bottom_edge)
    leave_top, leave_bottom = outs[0][None], outs[1][None]
    own = lax.dynamic_slice_in_dim(sides, lax.axis_index("cols_1") * 2, 2, 1)
    above, below = own[0][None], own[1][None]
    global_rows = row_place * local_rows + jnp.arange(local_rows, dtype=jnp.int32)
    global_cols = col_place * local_cols + jnp.arange(local_cols, dtype=jnp.int32)
    row_match = term_rows[:, None] == global_rows[None, :]
    site_match = row_match[:, :, None] & (term_bonds[:, None, None] == global_cols[None, None, :])
    left_need = jnp.any(site_match, axis=0)
    right_need = jnp.any(
        row_match[:, :, None] & (term_bonds[:, None, None] == global_cols[None, None, :] - 1),
        axis=0,
    )
    rows_shape = (local_rows,) + column_shape
    edge_shape = (local_rows, PHYS * PHYS) + column_shape
    open_shape = (local_rows, local_cols, PHYS * PHYS) + column_shape

    def chain_step(section_number, carried):
        from_left, from_right, edge_in, left_opens, right_opens, edge_open = carried

        def left_live(stores):
            source = jnp.where(col_place == 0, left_edge, from_left)
            environ = source[0]
            row_open = []
            for column in range(local_cols):
                opened, environ = side_step(
                    left_core,
                    environ,
                    kets[0, column],
                    layers[0, column],
                    above[0, column],
                    below[0, column],
                    left_need[0, column],
                )
                row_open.append(opened)
            opened_rows = [jnp.stack(row_open)]
            sent_rows = [environ]
            return (jnp.stack(opened_rows), jnp.stack(sent_rows))

        def left_spare(stores):
            return (stores, jnp.zeros(rows_shape, jnp.float32))

        left_opens, sent_left = lax.cond(
            section_number == col_place, left_live, left_spare, left_opens
        )

        def right_live(stores):
            source = jnp.where(col_place == col_count - 1, right_edge, from_right)
            environ = source[0]
            row_open = [None] * local_cols
            for column in reversed(range(local_cols)):
                opened, environ = side_step(
                    right_core,
                    environ,
                    kets[0, column],
                    layers[0, column],
                    above[0, column],
                    below[0, column],
                    right_need[0, column],
                )
                row_open[column] = opened
            opened_rows = [jnp.stack(row_open)]
            sent_rows = [environ]
            kept_edge = stores[1]
            return (jnp.stack(opened_rows), kept_edge, jnp.stack(sent_rows))

        def right_spare(stores):
            return (stores[0], stores[1], jnp.zeros(rows_shape, jnp.float32))

        right_opens, edge_open, sent_right = lax.cond(
            section_number == col_count - 1 - col_place,
            right_live,
            right_spare,
            (right_opens, edge_open),
        )
        from_left = shifted(sent_left, COLS, 1)
        from_right = shifted(sent_right, COLS, -1)
        return (from_left, from_right, edge_in, left_opens, right_opens, edge_open)

    chain_start = (
        jnp.zeros(rows_shape, jnp.float32),
        jnp.zeros(rows_shape, jnp.float32),
        jnp.zeros(edge_shape, jnp.float32),
        jnp.zeros(open_shape, jnp.float32),
        jnp.zeros(open_shape, jnp.float32),
        jnp.zeros(edge_shape, jnp.float32),
    )
    unused_left, unused_right, unused_edge, left_opens, right_opens, edge_open = lax.fori_loop(
        0, col_count, chain_step, chain_start
    )
    edge_open = shifted(right_opens[:, 0], COLS, -1)
    partner = jnp.concatenate([right_opens[:, 1:], edge_open[:, None]], axis=1)
    flat_left = left_opens.reshape(local_rows * local_cols, PHYS * PHYS, -1)
    flat_right = partner.reshape(local_rows * local_cols, PHYS * PHYS, -1)
    density = product("kpz,kqz->kpq", flat_left, flat_right).reshape(local_rows * local_cols, -1)
    diagonal = pair_diagonal()
    weights = jnp.outer(diagonal, diagonal).reshape(-1)
    trace_value = jnp.sum(density * weights[None, :], axis=1)
    spread = jnp.sqrt(jnp.sum(density * density, axis=1))
    valid_bond = left_need.reshape(-1)
    denominator = jnp.where(valid_bond, jnp.maximum(jnp.abs(trace_value), 0.25 * spread), 1.0)
    scaled = density / denominator[:, None]
    chooser = jnp.where(site_match.reshape(TERMS, -1), 1.0, 0.0).astype(jnp.float32)
    chosen = jnp.dot(chooser, scaled, precision=PRECISION_HIGH, preferred_element_type=jnp.float32)
    op_match = jnp.where(
        term_ops[:, None] == jnp.arange(OPS, dtype=jnp.int32)[None, :], 1.0, 0.0
    ).astype(jnp.float32)
    picked = jnp.dot(
        op_match, operators, precision=PRECISION_HIGH, preferred_element_type=jnp.float32
    )
    term_share = jnp.sum(chosen * picked, axis=1)
    energies = over_axes(term_share, ROWS_COLS)
    return (leave_top, leave_bottom, energies)


def solution(mesh):
    torus = Mesh(
        mesh.devices.reshape(8, 2, 2, 4, 2), ("rows_0", "rows_1", "rows_2", "cols_0", "cols_1")
    )
    placed = (
        P(ROWS, COLS, None),
        P(None, ROWS, COLS, None, None),
        P(None, ROWS, COLS, None, None),
        P(COLS, None, None),
        P(COLS, None, None),
        P(ROWS, None, None),
        P(ROWS, None, None),
        P(),
        P(),
        P(),
        P(),
    )
    return jax.shard_map(
        shards,
        mesh=torus,
        in_specs=placed,
        out_specs=(P(ROWS, COLS, None, None), P(ROWS, COLS, None, None), P()),
        check_vma=False,
    )
```

```python
import functools

import jax
import jax.numpy as jnp
from jax import lax
from jax.experimental import pallas as pl
from jax.experimental.pallas import tpu as pltpu
from jax.sharding import Mesh
from jax.sharding import PartitionSpec as P

D = 2
D2 = 4
PHYS = 2
CHI = 96
WIDE = D2 * CHI
OPS = 4
TERMS = 16
GROUP = 4
ROWS = ("rows_0", "rows_1", "rows_2")
COLS = ("cols_0", "cols_1")
ROWS_COLS = ("rows_0", "rows_1", "rows_2", "cols_0", "cols_1")
MESH = pl.DeviceIdType.MESH

EPSILON = 1e-06
PRECISION_HIGH = lax.Precision.HIGHEST
F32 = jnp.float32
BF16 = jnp.bfloat16


def iota(shape, dim):
    return lax.broadcasted_iota(jnp.int32, shape, dim)


def halves(value):
    high = value.astype(BF16)
    low = (value - high.astype(F32)).astype(BF16)
    return high, low


def dot(left, right):
    return jnp.dot(left, right, preferred_element_type=F32)


def dot_nt(left, right):
    return lax.dot_general(left, right, (((1,), (1,)), ((), ())), preferred_element_type=F32)


def unpack(wide):
    one, two, three = wide[:, 0:128], wide[:, 128:256], wide[:, 256:384]
    lane = iota((CHI, 128), 1)
    parts = (
        one,
        pltpu.roll(jnp.where(lane >= 96, one, two), 32, 1),
        pltpu.roll(jnp.where(lane >= 64, two, three), 64, 1),
        pltpu.roll(three, 96, 1),
    )
    return [jnp.where(lane < CHI, part, 0.0) for part in parts]


def pack(tiles):
    lane = iota((CHI, 128), 1)
    first = tiles[0]
    second = pltpu.roll(tiles[1], 96, 1)
    third = pltpu.roll(tiles[2], 64, 1)
    fourth = pltpu.roll(tiles[3], 32, 1)
    return jnp.concatenate(
        [
            jnp.where(lane < 96, first, second),
            jnp.where(lane < 64, second, third),
            jnp.where(lane < 32, third, fourth),
        ],
        axis=1,
    )


def pick(mode, *choices):
    value = choices[-1]
    for index in range(len(choices) - 1):
        value = jnp.where(mode == index, choices[index], value)
    return value


def layer_rows(ket, legs):
    shape = (PHYS * 256, 32)
    row, col = iota(shape, 0), iota(shape, 1)
    digits = ((row >> 6) & 3, (row >> 4) & 3, (row >> 2) & 3, row & 3)
    up, left, down, right = legs(*digits)
    base = (row >> 8) * 16
    ket_at = base + (up >> 1) * 8 + (left >> 1) * 4 + (down >> 1) * 2 + (right >> 1)
    bra_at = base + (up & 1) * 8 + (left & 1) * 4 + (down & 1) * 2 + (right & 1)
    take = functools.partial(jnp.dot, precision=PRECISION_HIGH, preferred_element_type=F32)
    kets = take(jnp.where(col == ket_at, 1.0, 0.0), ket)
    bras = take(jnp.where(col == bra_at, 1.0, 0.0), ket)
    both = kets * bras
    full = both[0:256] + both[256:512]
    lane = iota((64, 128), 1)
    at = [full[64 * m : 64 * (m + 1)] for m in range(4)]
    return jnp.concatenate(
        [
            jnp.where(lane < 96, at[0], at[1]),
            jnp.where(lane < 64, at[1], at[2]),
            jnp.where(lane < 32, at[2], at[3]),
        ],
        axis=1,
    )


def thirds(value):
    high = value.astype(BF16)
    rest = value - high.astype(F32)
    middle = rest.astype(BF16)
    low = (rest - middle.astype(F32)).astype(BF16)
    return high, middle, low


def fold_first(spread, coeffs, folded, slot):
    def body(index, carried):
        total = None
        for leg in range(4):
            term = coeffs[pl.ds(index * 4 + leg, 1), :] * spread[leg]
            total = term if total is None else total + term
        high, middle, low = thirds(total)
        rows = pl.ds(pl.multiple_of(index * CHI, CHI), CHI)
        folded[slot, rows, 0:WIDE] = low
        folded[slot, rows, WIDE : 2 * WIDE] = high
        folded[slot, rows, 2 * WIDE : 3 * WIDE] = middle
        return carried

    lax.fori_loop(0, 16, body, 0)


def padded(parts):
    blank = jnp.zeros((32, parts[0].shape[1]), BF16)
    return jnp.concatenate([piece for part in parts for piece in (part, blank)], axis=0)


def apply_layer(state, scale, folded, second, third, slot, middle):
    high, mid, low = thirds(state)
    once = jnp.concatenate([high, mid], axis=1)
    main = jnp.concatenate([once, once], axis=0)
    fine = jnp.concatenate([high, low], axis=0)
    for leg in range(4):
        rows = slice(leg * WIDE, (leg + 1) * WIDE)
        wide = dot(folded[slot, rows, WIDE : 3 * WIDE], main)
        rest = dot(folded[slot, rows, 0 : 2 * WIDE], fine)
        high, mid, low = thirds(wide[:, 0:128] + (wide[:, 128:256] + rest))
        for index, part in enumerate((high, mid)):
            middle[:, leg * 256 + index * 128 : leg * 256 + index * 128 + 128] = part
        for index, part in enumerate((high, low)):
            begin = 1024 + leg * 256 + index * 128
            middle[:, begin : begin + 128] = part
    wide = dot(middle[:, 0:1024], second[slot])
    rest = dot(middle[:, 1024:2048], third[slot])
    return (wide[:, 0:128] + (wide[:, 128:256] + rest)) * scale


def nrm_scale(state):
    total = jnp.sum(jnp.sum(state * state, axis=0, keepdims=True), axis=1, keepdims=True)
    return lax.rsqrt(total * (1.0 / (CHI * WIDE)) + EPSILON)


def boundary_kernel(
    kets,
    left_maps,
    right_maps,
    top_edge,
    bottom_edge,
    outs,
    sides,
    row_kets,
    lefts,
    rights,
    ketses,
    select_one,
    select_two,
    spread,
    coeffs,
    folded,
    second,
    third,
    middle,
    entered,
    leaving,
    state,
    normed,
    map_send,
    map_recv,
    hop_send,
    hop_recv,
    row_send,
    out_recv,
    side_recv,
    ket_send,
    ket_recv,
):
    z = lax.axis_index("rows_0")
    xl = lax.axis_index("rows_1")
    core = lax.axis_index("rows_2")
    y = lax.axis_index("cols_0")
    xh = lax.axis_index("cols_1")
    planes = lax.axis_size("rows_0")
    stations = lax.axis_size("cols_0")
    mine = xl * 2 + core
    col = xl
    way = (core + z) % 2
    place = xh * 2 + col
    is_first = ((way == 0) & (z == 0)) | ((way == 1) & (z == planes - 1))
    is_last = ((way == 0) & (z == planes - 1)) | ((way == 1) & (z == 0))
    after_z = z + 1 - 2 * way
    after = (jnp.clip(after_z, 0, planes - 1), xl, (way + after_z + 2) % 2, y, xh)

    barrier = pltpu.get_barrier_semaphore()

    def greet(device):
        pl.semaphore_signal(barrier, inc=1, device_id=device, device_id_type=MESH)

    for step in range(1, GROUP):
        other = (mine + step) % GROUP
        greet((z, other // 2, other % 2, y, xh))
    for other in range(GROUP):
        greet((z, other // 2, other % 2, y, 1 - xh))

    for step in (1, planes - 1):
        near = (z + step) % planes
        greet((near, xl, (way + near) % 2, y, xh))

    for step in (1, stations - 1):
        for other in range(GROUP):
            greet((z, other // 2, other % 2, (y + step) % stations, xh))

    pl.semaphore_wait(barrier, 17)

    def map_copies(step):
        other = (mine + step) % GROUP
        other_col = other // 2
        other_way = (other % 2 + z) % 2
        pairs = (
            (left_maps.at[other_way, 0, other_col], lefts),
            (right_maps.at[other_way, 0, other_col], rights),
            (kets.at[other_col], ketses),
        )
        device = (z, other // 2, other % 2, y, xh)
        return [
            pltpu.make_async_remote_copy(
                src_ref=source,
                dst_ref=target.at[mine],
                send_sem=map_send.at[step - 1, kind],
                recv_sem=map_recv.at[mine, kind],
                device_id=device,
                device_id_type=MESH,
            )
            for kind, (source, target) in enumerate(pairs)
        ]

    own_pairs = (
        (left_maps.at[way, 0, col], lefts),
        (right_maps.at[way, 0, col], rights),
        (kets.at[col], ketses),
    )
    for kind, (source, target) in enumerate(own_pairs):
        pltpu.make_async_copy(source, target.at[mine], map_recv.at[mine, kind]).start()
    for step in range(1, GROUP):
        for copy in map_copies(step):
            copy.start()

    def ket_across():
        return pltpu.make_async_remote_copy(
            src_ref=kets,
            dst_ref=row_kets.at[pl.ds(2 * xh, 2)],
            send_sem=ket_send.at[0],
            recv_sem=ket_recv.at[xh],
            device_id=(z, xl, core, y, 1 - xh),
            device_id_type=MESH,
        )

    def ket_back():
        return pltpu.make_async_remote_copy(
            src_ref=kets.at[0],
            dst_ref=row_kets.at[4],
            send_sem=ket_send.at[1],
            recv_sem=ket_recv.at[2],
            device_id=(z, xl, core, jnp.maximum(y - 1, 0), xh),
            device_id_type=MESH,
        )

    ket_across().start()
    pltpu.make_async_copy(kets, row_kets.at[pl.ds(2 * xh, 2)], ket_recv.at[xh]).start()
    sends_back = (xh == 0) & (y > 0)
    extra = sends_back & (col == 0)
    gets_back = (xh == 0) & (y < stations - 1)

    @pl.when(sends_back)
    def _():
        ket_back().start()

    for leg in range(4):
        row, lane = iota((WIDE, WIDE), 0), iota((WIDE, WIDE), 1)
        within = lane
        for _ in range(3):
            within = jnp.where(within >= CHI, within - CHI, within)
        select_one[:, leg * WIDE : (leg + 1) * WIDE] = jnp.where(
            row == 4 * within + leg, 1.0, 0.0
        ).astype(BF16)
        row, lane = iota((256, WIDE), 0), iota((256, WIDE), 1)
        inner = row & 127
        select_two[leg * 256 : (leg + 1) * 256, :] = jnp.where(
            (lane == 4 * inner + leg) & (inner < CHI), 1.0, 0.0
        ).astype(BF16)

    @pl.when(is_first & (way == 0))
    def _():
        entered[...] = top_edge[col]

    @pl.when(is_first & (way == 1))
    def _():
        entered[...] = bottom_edge[col]

    def row_at(number):
        return number + way * (GROUP - 1 - 2 * number)

    def legs(m, g, o, f):
        return pick(way, m, o), f, pick(way, o, m), g

    def prepare(number):
        j = row_at(number)
        for kind, target in enumerate((lefts, rights, ketses)):
            pltpu.make_async_copy(target.at[j], target.at[j], map_recv.at[j, kind]).wait()
        coeffs[...] = layer_rows(ketses[j], legs)
        apart = dot(jnp.concatenate(thirds(lefts[j]), axis=0), select_one[...])
        for leg in range(4):
            lanes = slice(leg * WIDE, (leg + 1) * WIDE)
            spread[leg] = apart[0:CHI, lanes] + (
                apart[CHI : 2 * CHI, lanes] + apart[2 * CHI : 3 * CHI, lanes]
            )
        fold_first(spread, coeffs, folded, number)
        high, mid, low = thirds(rights[j])
        main = dot_nt(select_two[...], padded((high, mid)))
        fine = dot_nt(select_two[...], padded((low,)))
        second[number] = main.astype(BF16)
        even = (iota((1024, 128), 0) & 128) == 0
        third[number] = jnp.where(even, fine, main[:, 0:128]).astype(BF16)

    def send_row(number, source, target_of, recv, xh_to, j, kind):
        here = (j == mine) & (xh_to == xh)

        @pl.when(here)
        def _():
            pltpu.make_async_copy(source, target_of, recv).start()

        @pl.when(jnp.logical_not(here))
        def _():
            row_copy(number, source, target_of, recv, xh_to, j, kind).start()

    def row_copy(number, source, target_of, recv, xh_to, j, kind):
        return pltpu.make_async_remote_copy(
            src_ref=source,
            dst_ref=target_of,
            send_sem=row_send.at[number, kind],
            recv_sem=recv,
            device_id=(z, j // 2, j % 2, y, xh_to),
            device_id_type=MESH,
        )

    def side_args(number, xh_to, kind):
        return (
            number,
            normed.at[number],
            sides.at[way, place],
            side_recv.at[way, place],
            xh_to,
            row_at(number),
            kind,
        )

    def back_copy(number):
        j = row_at(number)
        return pltpu.make_async_remote_copy(
            src_ref=normed.at[number],
            dst_ref=sides.at[way, 4],
            send_sem=row_send.at[number, 3],
            recv_sem=side_recv.at[way, 4],
            device_id=(z, j // 2, j % 2, jnp.maximum(y - 1, 0), xh),
            device_id_type=MESH,
        )

    def out_args(number):
        return (
            number,
            normed.at[number + 1],
            outs.at[way, col],
            out_recv.at[way, col],
            xh,
            row_at(number),
            2,
        )

    def advance(number):
        @pl.when(number == 0)
        def _():
            @pl.when(jnp.logical_not(is_first))
            def _():
                pltpu.make_async_copy(entered, entered, hop_recv).wait()

            for leg, tile in enumerate(unpack(entered[...])):
                state[leg * CHI : (leg + 1) * CHI, :] = tile

        current = state[...]
        raw = is_first & (number == 0)
        scale = jnp.where(raw, 1.0, nrm_scale(current))
        renewed = apply_layer(current, scale, folded, second, third, number, middle)
        state[...] = renewed

        @pl.when(number == GROUP - 1)
        def _():
            leaving[...] = pack([renewed[leg * CHI : (leg + 1) * CHI] for leg in range(4)])

            @pl.when(jnp.logical_not(is_last))
            def _():
                hop().start()

        kept = pack([current[leg * CHI : (leg + 1) * CHI] for leg in range(4)])
        normed[number] = kept * scale
        send_row(*side_args(number, xh, 0))
        send_row(*side_args(number, 1 - xh, 1))

        @pl.when(extra)
        def _():
            back_copy(number).start()

        @pl.when(number > 0)
        def _():
            send_row(*out_args(number - 1))

    def hop():
        return pltpu.make_async_remote_copy(
            src_ref=leaving,
            dst_ref=entered,
            send_sem=hop_send,
            recv_sem=hop_recv,
            device_id=after,
            device_id_type=MESH,
        )

    def task(index, carried):
        early = is_first
        is_prepare = (early & (index % 2 == 0)) | (jnp.logical_not(early) & (index < GROUP))

        @pl.when(is_prepare)
        def _():
            prepare(jnp.where(early, index // 2, jnp.minimum(index, GROUP - 1)))

        @pl.when(jnp.logical_not(is_prepare))
        def _():
            advance(jnp.where(early, index // 2, jnp.maximum(index - GROUP, 0)))

        return carried

    lax.fori_loop(0, 2 * GROUP, task, 0)

    final = state[...]
    normed[GROUP] = leaving[...] * nrm_scale(final)
    send_row(*out_args(GROUP - 1))

    for step in range(1, GROUP):
        for copy in map_copies(step):
            copy.wait_send()

    @pl.when(jnp.logical_not(is_last))
    def _():
        hop().wait_send()

    for number in range(GROUP):
        row_copy(*side_args(number, 1 - xh, 1)).wait_send()

        @pl.when(extra)
        def _():
            back_copy(number).wait_send()

        @pl.when(row_at(number) != mine)
        def _():
            row_copy(*side_args(number, xh, 0)).wait_send()
            row_copy(*out_args(number)).wait_send()

    for direction in range(2):
        for column in range(2):
            target = outs.at[direction, column]
            pltpu.make_async_copy(target, target, out_recv.at[direction, column]).wait()
        for column in range(4):
            target = sides.at[direction, column]
            pltpu.make_async_copy(target, target, side_recv.at[direction, column]).wait()

        @pl.when(gets_back)
        def _():
            target = sides.at[direction, 4]
            pltpu.make_async_copy(target, target, side_recv.at[direction, 4]).wait()

    ket_across().wait_send()
    for half in range(2):
        target = row_kets.at[pl.ds(2 * half, 2)]
        pltpu.make_async_copy(target, target, ket_recv.at[half]).wait()

    @pl.when(sends_back)
    def _():
        ket_back().wait_send()

    @pl.when(gets_back)
    def _():
        pltpu.make_async_copy(row_kets.at[4], row_kets.at[4], ket_recv.at[2]).wait()


def run_boundary(kets, left_maps, right_maps, top_edge, bottom_edge):
    vmem = pl.BlockSpec(memory_space=pltpu.VMEM)
    column = (CHI, WIDE)
    return pl.pallas_call(
        boundary_kernel,
        out_shape=(
            jax.ShapeDtypeStruct((2, 2) + column, F32),
            jax.ShapeDtypeStruct((2, 5) + column, F32),
            jax.ShapeDtypeStruct((5, 32, 128), F32),
        ),
        in_specs=[vmem] * 5,
        out_specs=(vmem, vmem, vmem),
        scratch_shapes=[
            pltpu.VMEM((GROUP,) + column, F32),
            pltpu.VMEM((GROUP,) + column, F32),
            pltpu.VMEM((GROUP, 32, 128), F32),
            pltpu.VMEM((WIDE, 4 * WIDE), BF16),
            pltpu.VMEM((1024, WIDE), BF16),
            pltpu.VMEM((4,) + column, F32),
            pltpu.VMEM((64, WIDE), F32),
            pltpu.VMEM((GROUP, 16 * CHI, 3 * WIDE), BF16),
            pltpu.VMEM((GROUP, 1024, 256), BF16),
            pltpu.VMEM((GROUP, 1024, 128), BF16),
            pltpu.VMEM((WIDE, 2048), BF16),
            pltpu.VMEM(column, F32),
            pltpu.VMEM(column, F32),
            pltpu.VMEM((WIDE, 128), F32),
            pltpu.VMEM((GROUP + 1,) + column, F32),
            pltpu.SemaphoreType.DMA((GROUP - 1, 3)),
            pltpu.SemaphoreType.DMA((GROUP, 3)),
            pltpu.SemaphoreType.DMA,
            pltpu.SemaphoreType.DMA,
            pltpu.SemaphoreType.DMA((GROUP, 4)),
            pltpu.SemaphoreType.DMA((2, 2)),
            pltpu.SemaphoreType.DMA((2, 5)),
            pltpu.SemaphoreType.DMA((2,)),
            pltpu.SemaphoreType.DMA((3,)),
        ],
        compiler_params=pltpu.CompilerParams(
            collective_id=0, has_side_effects=True, vmem_limit_bytes=48 * 1024 * 1024
        ),
        name="boundary",
    )(kets, left_maps, right_maps, top_edge, bottom_edge)


def fold_pair(spread, coeffs, folded, slot):
    def body(index, carried):
        total = None
        for leg in range(4):
            term = coeffs[pl.ds(index * 4 + leg, 1), :] * spread[leg]
            total = term if total is None else total + term
        high, low = halves(total)
        rows = pl.ds(pl.multiple_of(index * CHI, CHI), CHI)
        folded[slot, rows, 0:WIDE] = high
        folded[slot, rows, WIDE : 2 * WIDE] = low
        return carried

    lax.fori_loop(0, 16, body, 0)


def apply_pair(state, scale, folded, second, slot, middle):
    high, low = halves(state)
    once = jnp.concatenate([high, low], axis=1)
    twice = jnp.concatenate([once, once], axis=0)
    for leg in range(4):
        wide = dot(folded[slot, leg * WIDE : (leg + 1) * WIDE, :], twice)
        high, low = halves(wide[:, 0:128] + wide[:, 128:256])
        middle[:, leg * 256 : leg * 256 + 128] = high
        middle[:, leg * 256 + 128 : leg * 256 + 256] = low
    wide = dot(middle[...], second[slot])
    return (wide[:, 0:128] + wide[:, 128:256]) * scale


def environment_kernel(
    sides,
    row_kets,
    left_edge,
    right_edge,
    from_left,
    from_right,
    select_one,
    select_two,
    spread,
    coeffs,
    folded,
    second,
    middle,
    entered,
    leaving,
    state,
    normed,
    hop_send,
    hop_recv,
    over_send,
    over_recv,
):
    z = lax.axis_index("rows_0")
    xl = lax.axis_index("rows_1")
    core = lax.axis_index("rows_2")
    y = lax.axis_index("cols_0")
    way = lax.axis_index("cols_1")
    stations = lax.axis_size("cols_0")
    is_first = ((way == 0) & (y == 0)) | ((way == 1) & (y == stations - 1))
    is_last = ((way == 0) & (y == stations - 1)) | ((way == 1) & (y == 0))
    after = (z, xl, core, jnp.clip(y + 1 - 2 * way, 0, stations - 1), way)

    barrier = pltpu.get_barrier_semaphore()

    def greet(y_to, way_to):
        device = (z, xl, core, (y_to + stations) % stations, way_to)
        pl.semaphore_signal(barrier, inc=1, device_id=device, device_id_type=MESH)

    greet(y + 1, way)
    greet(y - 1, way)
    greet(y, 1 - way)
    greet(y + 1 - 2 * way, 1 - way)
    pl.semaphore_wait(barrier, 4)

    @pl.when(way == 0)
    def _():
        row, lane = iota((2 * CHI, WIDE), 0), iota((2 * CHI, WIDE), 1)
        row = jnp.where(row >= CHI, row - CHI, row)
        for _ in range(3):
            lane = jnp.where(lane >= CHI, lane - CHI, lane)
        select_one[0 : 2 * CHI, 0:WIDE] = jnp.where(row == lane, 1.0, 0.0).astype(BF16)

    @pl.when(way == 1)
    def _():
        for leg in range(4):
            row, lane = iota((WIDE, WIDE), 0), iota((WIDE, WIDE), 1)
            for _ in range(3):
                lane = jnp.where(lane >= CHI, lane - CHI, lane)
            select_one[:, leg * WIDE : (leg + 1) * WIDE] = jnp.where(
                row == leg * CHI + lane, 1.0, 0.0
            ).astype(BF16)
            row, lane = iota((256, WIDE), 0), iota((256, WIDE), 1)
            inner = row & 127
            select_two[leg * 256 : (leg + 1) * 256, :] = jnp.where(
                (lane == leg * CHI + inner) & (inner < CHI), 1.0, 0.0
            ).astype(BF16)

    @pl.when(is_first & (way == 0))
    def _():
        entered[...] = left_edge[0]

    @pl.when(is_first & (way == 1))
    def _():
        entered[...] = right_edge[0]

    def column_at(number):
        return number + way * (3 - 2 * number)

    def legs(m, g, o, f):
        return f, pick(way, m, o), g, pick(way, o, m)

    def prepare(number):
        column = column_at(number)
        coeffs[...] = layer_rows(row_kets[column], legs)
        above = jnp.concatenate(halves(sides[0, column]), axis=0)

        @pl.when(way == 0)
        def _():
            turned = lax.dot_general(
                above,
                select_one[0 : 2 * CHI, 0:WIDE],
                (((0,), (0,)), ((), ())),
                preferred_element_type=F32,
            )
            for leg in range(4):
                spread[leg] = turned[leg * CHI : (leg + 1) * CHI]
            for leg, tile in enumerate(unpack(sides[1, column])):
                high, low = halves(tile)
                both = jnp.concatenate(
                    [jnp.concatenate([high, low], axis=1), jnp.zeros((32, 256), BF16)], axis=0
                )
                second[number, leg * 256 : leg * 256 + 128, :] = both
                second[number, leg * 256 + 128 : leg * 256 + 256, :] = both

        @pl.when(way == 1)
        def _():
            apart = dot(above, select_one[...])
            for leg in range(4):
                lanes = slice(leg * WIDE, (leg + 1) * WIDE)
                spread[leg] = apart[0:CHI, lanes] + apart[CHI : 2 * CHI, lanes]
            second[number] = dot_nt(select_two[...], padded(halves(sides[1, column]))).astype(BF16)

        fold_pair(spread, coeffs, folded, number)

    def hop():
        return pltpu.make_async_remote_copy(
            src_ref=leaving,
            dst_ref=entered,
            send_sem=hop_send,
            recv_sem=hop_recv,
            device_id=after,
            device_id_type=MESH,
        )

    def over(number):
        column = column_at(number)
        wraps = column == 0
        slot = jnp.where(wraps, 3, jnp.maximum(column - 1, 0))
        y_to = jnp.where(wraps, jnp.maximum(y - 1, 0), y)
        return pltpu.make_async_remote_copy(
            src_ref=normed.at[number],
            dst_ref=from_right.at[slot],
            send_sem=over_send.at[number],
            recv_sem=over_recv.at[slot],
            device_id=(z, xl, core, y_to, 0),
            device_id_type=MESH,
        )

    def sends_over(number):
        return (way == 1) & ((y > 0) | (column_at(number) > 0))

    def advance(number):
        @pl.when(number == 0)
        def _():
            @pl.when(jnp.logical_not(is_first))
            def _():
                pltpu.make_async_copy(entered, entered, hop_recv).wait()

            for leg, tile in enumerate(unpack(entered[...])):
                state[leg * CHI : (leg + 1) * CHI, :] = tile

        current = state[...]
        raw = is_first & (number == 0)
        scale = jnp.where(raw, 1.0, nrm_scale(current))

        @pl.when(jnp.logical_not(is_last & (number >= 2)))
        def _():
            renewed = apply_pair(current, scale, folded, second, number, middle)
            state[...] = renewed

            @pl.when(number == 3)
            def _():
                leaving[...] = pack([renewed[leg * CHI : (leg + 1) * CHI] for leg in range(4)])
                hop().start()

        kept = pack([current[leg * CHI : (leg + 1) * CHI] for leg in range(4)]) * scale

        @pl.when(way == 0)
        def _():
            from_left[number] = kept

        @pl.when(sends_over(number))
        def _():
            normed[number] = kept
            over(number).start()

    def task(index, carried):
        is_prepare = (is_first & (index % 2 == 0)) | (jnp.logical_not(is_first) & (index < 4))

        @pl.when(is_prepare)
        def _():
            prepare(jnp.where(is_first, index // 2, jnp.minimum(index, 3)))

        @pl.when(jnp.logical_not(is_prepare))
        def _():
            advance(jnp.where(is_first, index // 2, jnp.maximum(index - 4, 0)))

        return carried

    lax.fori_loop(0, 8, task, 0)

    @pl.when(jnp.logical_not(is_last))
    def _():
        hop().wait_send()

    for number in range(4):

        @pl.when(sends_over(number))
        def _():
            over(number).wait_send()

    @pl.when(way == 0)
    def _():
        for slot in range(3):
            target = from_right.at[slot]
            pltpu.make_async_copy(target, target, over_recv.at[slot]).wait()

    @pl.when((way == 0) & (y < stations - 1))
    def _():
        target = from_right.at[3]
        pltpu.make_async_copy(target, target, over_recv.at[3]).wait()


def run_environment(sides, row_kets, left_edge, right_edge):
    vmem = pl.BlockSpec(memory_space=pltpu.VMEM)
    column = (CHI, WIDE)
    return pl.pallas_call(
        environment_kernel,
        out_shape=(
            jax.ShapeDtypeStruct((4,) + column, F32),
            jax.ShapeDtypeStruct((4,) + column, F32),
        ),
        in_specs=[vmem] * 4,
        out_specs=(vmem, vmem),
        scratch_shapes=[
            pltpu.VMEM((WIDE, 4 * WIDE), BF16),
            pltpu.VMEM((1024, WIDE), BF16),
            pltpu.VMEM((4,) + column, F32),
            pltpu.VMEM((64, WIDE), F32),
            pltpu.VMEM((4, 16 * CHI, 2 * WIDE), BF16),
            pltpu.VMEM((4, 1024, 256), BF16),
            pltpu.VMEM((WIDE, 1024), BF16),
            pltpu.VMEM(column, F32),
            pltpu.VMEM(column, F32),
            pltpu.VMEM((WIDE, 128), F32),
            pltpu.VMEM((4,) + column, F32),
            pltpu.SemaphoreType.DMA,
            pltpu.SemaphoreType.DMA,
            pltpu.SemaphoreType.DMA((4,)),
            pltpu.SemaphoreType.DMA((4,)),
        ],
        compiler_params=pltpu.CompilerParams(
            collective_id=1, has_side_effects=True, vmem_limit_bytes=40 * 1024 * 1024
        ),
        name="environment",
    )(sides, row_kets, left_edge, right_edge)


def dot_general(left, right, dims):
    return lax.dot_general(left, right, (dims, ((), ())), preferred_element_type=F32)


def pad_rows(value):
    return jnp.concatenate([value, jnp.zeros((32, value.shape[1]), value.dtype)], axis=0)


def open_site(ket, legs_at, wide, opened):
    def body(block, carried):
        begin = pl.multiple_of(block * 8, 8)
        half_done = {}
        for bra in range(8):
            u2, m2, d2 = bra >> 2, (bra >> 1) & 1, bra & 1
            tiles = []
            for top in range(8):
                u, m, d = top >> 2, (top >> 1) & 1, top & 1
                row = (2 * m + m2) * 4 + 2 * u + u2
                lane = (2 * d + d2) * 128
                tiles.append(wide[pl.ds(row * CHI + begin, 8), lane : lane + 128])
            for state in range(2):
                for out in range(2):
                    total = None
                    for top in range(8):
                        at = state * 16 + legs_at(top >> 2, (top >> 1) & 1, top & 1, out)
                        term = ket[at : at + 1, :] * tiles[top]
                        total = term if total is None else total + term
                    half_done[state, out, bra] = total
        for state in range(2):
            for out in range(2):
                for other in range(2):
                    for out2 in range(2):
                        total = None
                        for bra in range(8):
                            at = other * 16 + legs_at(bra >> 2, (bra >> 1) & 1, bra & 1, out2)
                            term = ket[at : at + 1, :] * half_done[state, out, bra]
                            total = term if total is None else total + term
                        row = (2 * out + out2) * CHI
                        opened[state * 2 + other, pl.ds(row + begin, 8), :] = total
        return carried

    lax.fori_loop(0, CHI // 8, body, 0)


def energy_kernel(
    term_rows,
    term_bonds,
    term_ops,
    operators,
    sides,
    row_kets,
    from_left,
    from_right,
    shares,
    wide,
    opened,
    closing,
    density,
):
    way = lax.axis_index("cols_1")
    row_here = (
        lax.axis_index("rows_0") * GROUP + lax.axis_index("rows_1") * 2 + lax.axis_index("rows_2")
    )
    first = lax.axis_index("cols_0") * 4
    shares[...] = jnp.zeros((8, 128), F32)

    def hits(term, column):
        here = (term_rows[term] == row_here) & (term_bonds[term] == first + column)
        return here & (way == 0)

    def column_body(column, carried):
        count = 0
        for term in range(TERMS):
            count = count + jnp.where(hits(term, column), 1, 0)

        @pl.when(count > 0)
        def _():
            high, low = halves(sides[0, column])
            both = jnp.concatenate([high, low], axis=0)
            state_high, state_low = halves(jnp.concatenate(unpack(from_left[column]), axis=1))
            tn = ((0,), (0,))
            joined = dot_general(
                both, jnp.concatenate([state_high, state_high], axis=0), tn
            ) + dot_general(both, jnp.concatenate([state_low, state_low], axis=0), tn)
            below_high, below_low = halves(jnp.concatenate(unpack(sides[1, column]), axis=1))
            main = jnp.concatenate([pad_rows(below_high), pad_rows(below_high)], axis=0)
            fine = jnp.concatenate([pad_rows(below_low), pad_rows(below_low)], axis=0)
            for leg in range(4):
                part = jnp.concatenate(halves(joined[:, leg * 128 : (leg + 1) * 128]), axis=1)
                wide[leg * WIDE : (leg + 1) * WIDE, :] = dot(part, main) + dot(part, fine)
            open_site(
                row_kets.at[column],
                lambda u, m, d, out: u * 8 + m * 4 + d * 2 + out,
                wide,
                opened,
            )

            right = column + 1
            above = jnp.concatenate(unpack(sides[0, right]), axis=0)
            both = jnp.concatenate(halves(above), axis=1)
            state_high, state_low = halves(jnp.concatenate(unpack(from_right[column]), axis=1))
            state_high, state_low = pad_rows(state_high), pad_rows(state_low)
            joined = dot(both, jnp.concatenate([state_high, state_high], axis=0)) + dot(
                both, jnp.concatenate([state_low, state_low], axis=0)
            )
            below_high, below_low = halves(
                jnp.concatenate([pad_rows(tile) for tile in unpack(sides[1, right])], axis=0)
            )
            main = jnp.concatenate([below_high, below_high], axis=1)
            fine = jnp.concatenate([below_low, below_low], axis=1)
            for leg in range(4):
                part = jnp.concatenate(halves(joined[:, leg * 128 : (leg + 1) * 128]), axis=1)
                wide[leg * WIDE : (leg + 1) * WIDE, :] = dot_nt(part, main) + dot_nt(part, fine)
            open_site(
                row_kets.at[right],
                lambda u, m, d, out: u * 8 + out * 4 + d * 2 + m,
                wide,
                closing,
            )

            for pair in range(4):
                for other in range(4):
                    product = opened[pair] * closing[other]
                    at = pair * 4 + other
                    density[at : at + 1, :] = jnp.sum(product, axis=0, keepdims=True)
            rho = jnp.sum(density[...], axis=1, keepdims=True)
            index = iota((16, 1), 0)
            diagonal = (index == 0) | (index == 3) | (index == 12) | (index == 15)
            trace = jnp.sum(jnp.where(diagonal, rho, 0.0), axis=0, keepdims=True)
            spread = jnp.sqrt(jnp.sum(rho * rho, axis=0, keepdims=True))
            bottom = jnp.maximum(jnp.abs(trace), 0.25 * spread)

            def term_body(term, kept):
                @pl.when(hits(term, column))
                def _():
                    chosen = jnp.zeros((16, 1), F32)
                    for entry in range(16):
                        chosen = jnp.where(
                            index == entry, operators[term_ops[term], entry], chosen
                        )
                    value = jnp.sum(chosen * rho, axis=0, keepdims=True) / bottom
                    lane = iota((8, 128), 1)
                    shares[...] = jnp.where(lane == term, value, shares[...])

                return kept

            lax.fori_loop(0, TERMS, term_body, 0)

        return carried

    lax.fori_loop(0, 4, column_body, 0)


def run_energies(term_rows, term_bonds, term_ops, operators, sides, row_kets, lefts, rights):
    vmem = pl.BlockSpec(memory_space=pltpu.VMEM)
    smem = pl.BlockSpec(memory_space=pltpu.SMEM)
    return pl.pallas_call(
        energy_kernel,
        out_shape=jax.ShapeDtypeStruct((8, 128), F32),
        in_specs=[smem] * 4 + [vmem] * 4,
        out_specs=vmem,
        scratch_shapes=[
            pltpu.VMEM((16 * CHI, 512), F32),
            pltpu.VMEM((4, WIDE, 128), F32),
            pltpu.VMEM((4, WIDE, 128), F32),
            pltpu.VMEM((16, 128), F32),
        ],
        compiler_params=pltpu.CompilerParams(vmem_limit_bytes=32 * 1024 * 1024),
        name="energies",
    )(term_rows, term_bonds, term_ops, operators, sides, row_kets, lefts, rights)


def sum_kernel(shares, total, planes_in, plane_in, partial, send_one, recv_one, send_two, recv_two):
    z = lax.axis_index("rows_0")
    xl = lax.axis_index("rows_1")
    core = lax.axis_index("rows_2")
    y = lax.axis_index("cols_0")
    way = lax.axis_index("cols_1")
    place = y * 4 + xl * 2 + core
    barrier = pltpu.get_barrier_semaphore()

    def greet(device):
        pl.semaphore_signal(barrier, inc=1, device_id=device, device_id_type=MESH)

    def along(step):
        return ((z + step) % 8, xl, core, y, way)

    def within(step):
        other = (place * 2 + way + step) % 32
        return (z, (other // 4) % 2, (other // 2) % 2, other // 8, other % 2)

    for step in range(1, 8):
        greet(along(step))
    for step in range(1, 32):
        greet(within(step))
    pl.semaphore_wait(barrier, 38)

    def first(step):
        return pltpu.make_async_remote_copy(
            src_ref=shares,
            dst_ref=planes_in.at[z],
            send_sem=send_one.at[step],
            recv_sem=recv_one.at[z],
            device_id=along(step),
            device_id_type=MESH,
        )

    def second(step):
        return pltpu.make_async_remote_copy(
            src_ref=partial,
            dst_ref=plane_in.at[place],
            send_sem=send_two.at[step],
            recv_sem=recv_two.at[place],
            device_id=within(step),
            device_id_type=MESH,
        )

    @pl.when(way == 0)
    def _():
        for step in range(1, 8):
            first(step).start()
        pltpu.make_async_copy(shares, planes_in.at[z], recv_one.at[z]).start()
        added = None
        for plane in range(8):
            target = planes_in.at[plane]
            pltpu.make_async_copy(target, target, recv_one.at[plane]).wait()
        for plane in range(8):
            added = planes_in[plane] if added is None else added + planes_in[plane]
        partial[...] = added
        for step in range(1, 32):
            second(step).start()
        pltpu.make_async_copy(partial, plane_in.at[place], recv_two.at[place]).start()

    for other in range(16):
        target = plane_in.at[other]
        pltpu.make_async_copy(target, target, recv_two.at[other]).wait()
    added = None
    for other in range(16):
        added = plane_in[other] if added is None else added + plane_in[other]
    total[...] = added

    @pl.when(way == 0)
    def _():
        for step in range(1, 8):
            first(step).wait_send()
        for step in range(1, 32):
            second(step).wait_send()


def run_sum(shares):
    vmem = pl.BlockSpec(memory_space=pltpu.VMEM)
    return pl.pallas_call(
        sum_kernel,
        out_shape=jax.ShapeDtypeStruct((8, 128), F32),
        in_specs=[vmem],
        out_specs=vmem,
        scratch_shapes=[
            pltpu.VMEM((8, 8, 128), F32),
            pltpu.VMEM((16, 8, 128), F32),
            pltpu.VMEM((8, 128), F32),
            pltpu.SemaphoreType.DMA((8,)),
            pltpu.SemaphoreType.DMA((8,)),
            pltpu.SemaphoreType.DMA((32,)),
            pltpu.SemaphoreType.DMA((16,)),
        ],
        compiler_params=pltpu.CompilerParams(collective_id=2, has_side_effects=True),
        name="shares_sum",
    )(shares)


def shards(
    kets,
    left_maps,
    right_maps,
    top_edge,
    bottom_edge,
    left_edge,
    right_edge,
    term_rows,
    term_bonds,
    term_ops,
    operators,
):
    spread_kets = jnp.broadcast_to(kets[0][:, :, None], (kets.shape[1], 32, 128))
    outs, sides, row_kets = run_boundary(
        spread_kets, left_maps, right_maps, top_edge, bottom_edge
    )
    lefts, rights = run_environment(sides, row_kets, left_edge, right_edge)
    shares = run_energies(
        term_rows, term_bonds, term_ops, operators, sides, row_kets, lefts, rights
    )
    energies = run_sum(shares)[0, :TERMS]
    return (outs[0][None], outs[1][None], energies)


def solution(mesh):
    torus = Mesh(
        mesh.devices.reshape(8, 2, 2, 4, 2), ("rows_0", "rows_1", "rows_2", "cols_0", "cols_1")
    )
    placed = (
        P(ROWS, COLS, None),
        P(None, ROWS, COLS, None, None),
        P(None, ROWS, COLS, None, None),
        P(COLS, None, None),
        P(COLS, None, None),
        P(ROWS, None, None),
        P(ROWS, None, None),
        P(),
        P(),
        P(),
        P(),
    )
    return jax.shard_map(
        shards,
        mesh=torus,
        in_specs=placed,
        out_specs=(P(ROWS, COLS, None, None), P(ROWS, COLS, None, None), P()),
        check_vma=False,
    )
```

```python
import functools

import jax
import jax.numpy as jnp
from jax import lax
from jax.experimental import pallas as pl
from jax.experimental.pallas import tpu as pltpu
from jax.sharding import Mesh
from jax.sharding import PartitionSpec as P

D = 2
D2 = 4
PHYS = 2
CHI = 96
WIDE = D2 * CHI
OPS = 4
TERMS = 16
GROUP = 4
ROWS = ("rows_0", "rows_1", "rows_2")
COLS = ("cols_0", "cols_1")
ROWS_COLS = ("rows_0", "rows_1", "rows_2", "cols_0", "cols_1")
MESH = pl.DeviceIdType.MESH

EPSILON = 1e-06
PRECISION_HIGH = lax.Precision.HIGHEST
F32 = jnp.float32
BF16 = jnp.bfloat16


def iota(shape, dim):
    return lax.broadcasted_iota(jnp.int32, shape, dim)


def halves(value):
    high = value.astype(BF16)
    low = (value - high.astype(F32)).astype(BF16)
    return high, low


def dot(left, right):
    return jnp.dot(left, right, preferred_element_type=F32)


def dot_nt(left, right):
    return lax.dot_general(left, right, (((1,), (1,)), ((), ())), preferred_element_type=F32)


def unpack(wide):
    one, two, three = wide[:, 0:128], wide[:, 128:256], wide[:, 256:384]
    lane = iota((CHI, 128), 1)
    parts = (
        one,
        pltpu.roll(jnp.where(lane >= 96, one, two), 32, 1),
        pltpu.roll(jnp.where(lane >= 64, two, three), 64, 1),
        pltpu.roll(three, 96, 1),
    )
    return [jnp.where(lane < CHI, part, 0.0) for part in parts]


def pack(tiles):
    lane = iota((CHI, 128), 1)
    first = tiles[0]
    second = pltpu.roll(tiles[1], 96, 1)
    third = pltpu.roll(tiles[2], 64, 1)
    fourth = pltpu.roll(tiles[3], 32, 1)
    return jnp.concatenate(
        [
            jnp.where(lane < 96, first, second),
            jnp.where(lane < 64, second, third),
            jnp.where(lane < 32, third, fourth),
        ],
        axis=1,
    )


def pick(mode, *choices):
    value = choices[-1]
    for index in range(len(choices) - 1):
        value = jnp.where(mode == index, choices[index], value)
    return value


def layer_rows(ket, legs):
    shape = (PHYS * 256, 32)
    row, col = iota(shape, 0), iota(shape, 1)
    digits = ((row >> 6) & 3, (row >> 4) & 3, (row >> 2) & 3, row & 3)
    up, left, down, right = legs(*digits)
    base = (row >> 8) * 16
    ket_at = base + (up >> 1) * 8 + (left >> 1) * 4 + (down >> 1) * 2 + (right >> 1)
    bra_at = base + (up & 1) * 8 + (left & 1) * 4 + (down & 1) * 2 + (right & 1)
    take = functools.partial(jnp.dot, precision=PRECISION_HIGH, preferred_element_type=F32)
    kets = take(jnp.where(col == ket_at, 1.0, 0.0), ket)
    bras = take(jnp.where(col == bra_at, 1.0, 0.0), ket)
    both = kets * bras
    full = both[0:256] + both[256:512]
    lane = iota((64, 128), 1)
    at = [full[64 * m : 64 * (m + 1)] for m in range(4)]
    return jnp.concatenate(
        [
            jnp.where(lane < 96, at[0], at[1]),
            jnp.where(lane < 64, at[1], at[2]),
            jnp.where(lane < 32, at[2], at[3]),
        ],
        axis=1,
    )


def thirds(value):
    high = value.astype(BF16)
    rest = value - high.astype(F32)
    middle = rest.astype(BF16)
    low = (rest - middle.astype(F32)).astype(BF16)
    return high, middle, low


def fold_first(spread, coeffs, folded, slot):
    def body(index, carried):
        total = None
        for leg in range(4):
            term = coeffs[pl.ds(index * 4 + leg, 1), :] * spread[leg]
            total = term if total is None else total + term
        high, middle, low = thirds(total)
        rows = pl.ds(pl.multiple_of(index * CHI, CHI), CHI)
        folded[slot, rows, 0:WIDE] = low
        folded[slot, rows, WIDE : 2 * WIDE] = high
        folded[slot, rows, 2 * WIDE : 3 * WIDE] = middle
        return carried

    lax.fori_loop(0, 16, body, 0)


def padded(parts):
    blank = jnp.zeros((32, parts[0].shape[1]), BF16)
    return jnp.concatenate([piece for part in parts for piece in (part, blank)], axis=0)


def apply_layer(state, scale, folded, second, third, slot, middle):
    high, mid, low = thirds(state)
    once = jnp.concatenate([high, mid], axis=1)
    main = jnp.concatenate([once, once], axis=0)
    fine = jnp.concatenate([high, low], axis=0)
    for leg in range(4):
        rows = slice(leg * WIDE, (leg + 1) * WIDE)
        wide = dot(folded[slot, rows, WIDE : 3 * WIDE], main)
        rest = dot(folded[slot, rows, 0 : 2 * WIDE], fine)
        high, mid, low = thirds(wide[:, 0:128] + (wide[:, 128:256] + rest))
        for index, part in enumerate((high, mid)):
            middle[:, leg * 256 + index * 128 : leg * 256 + index * 128 + 128] = part
        for index, part in enumerate((high, low)):
            begin = 1024 + leg * 256 + index * 128
            middle[:, begin : begin + 128] = part
    wide = dot(middle[:, 0:1024], second[slot])
    rest = dot(middle[:, 1024:2048], third[slot])
    return (wide[:, 0:128] + (wide[:, 128:256] + rest)) * scale


def nrm_scale(state):
    total = jnp.sum(jnp.sum(state * state, axis=0, keepdims=True), axis=1, keepdims=True)
    return lax.rsqrt(total * (1.0 / (CHI * WIDE)) + EPSILON)


def fold_pair(spread, coeffs, folded, slot):
    def body(index, carried):
        total = None
        for leg in range(4):
            term = coeffs[pl.ds(index * 4 + leg, 1), :] * spread[leg]
            total = term if total is None else total + term
        high, low = halves(total)
        rows = pl.ds(pl.multiple_of(index * CHI, CHI), CHI)
        folded[slot, rows, 0:WIDE] = high
        folded[slot, rows, WIDE : 2 * WIDE] = low
        return carried

    lax.fori_loop(0, 16, body, 0)


def apply_pair(state, scale, folded, second, slot, middle):
    high, low = halves(state)
    once = jnp.concatenate([high, low], axis=1)
    twice = jnp.concatenate([once, once], axis=0)
    for leg in range(4):
        wide = dot(folded[slot, leg * WIDE : (leg + 1) * WIDE, :], twice)
        high, low = halves(wide[:, 0:128] + wide[:, 128:256])
        middle[:, leg * 256 : leg * 256 + 128] = high
        middle[:, leg * 256 + 128 : leg * 256 + 256] = low
    wide = dot(middle[:, 0:1024], second[slot])
    return (wide[:, 0:128] + wide[:, 128:256]) * scale


def sweep_kernel(
    kets,
    left_maps,
    right_maps,
    top_edge,
    bottom_edge,
    left_edge,
    right_edge,
    outs,
    sides,
    row_kets,
    from_left,
    from_right,
    lefts,
    rights,
    ketses,
    select_one,
    select_two,
    spread,
    coeffs,
    folded,
    second,
    third,
    env_folded,
    env_second,
    middle,
    entered,
    leaving,
    state,
    normed,
    last_in,
    env_entered,
    env_leaving,
    env_normed,
    map_send,
    map_recv,
    hop_send,
    hop_recv,
    row_send,
    out_recv,
    side_recv,
    ket_send,
    ket_recv,
    env_send,
    env_recv,
    over_send,
    over_recv,
):
    z = lax.axis_index("rows_0")
    xl = lax.axis_index("rows_1")
    core = lax.axis_index("rows_2")
    y = lax.axis_index("cols_0")
    xh = lax.axis_index("cols_1")
    planes = lax.axis_size("rows_0")
    stations = lax.axis_size("cols_0")
    end = planes - 1
    at_edge = (z == 0) | (z == end)
    low = jnp.where(at_edge, z, 1 + 2 * (jnp.maximum(z - 1, 0) // 2))
    count = jnp.where(at_edge, GROUP, 2 * GROUP)
    col = xl
    is_worker = at_edge | (core == 1)
    way = jnp.where(z == 0, 1 - core, jnp.where(z == end, core, (z + 1) % 2))
    starts = ((way == 0) & (z == 0)) | ((way == 1) & (z == end))
    is_first = at_edge & starts
    is_last = at_edge & jnp.logical_not(starts)
    has_next = is_worker & jnp.logical_not(is_last)
    has_prev = is_worker & jnp.logical_not(is_first)
    mine = (z - low) * GROUP + xl * 2 + core
    place = xh * 2 + col
    ahead = jnp.where(way == 0, jnp.where(z == 0, 1, z + 2), jnp.where(z == end, end - 1, z - 2))
    ahead = jnp.clip(ahead, 0, end)
    after = (ahead, xl, jnp.where((ahead == 0) | (ahead == end), 0, 1), y, xh)
    behind = jnp.where(way == 0, jnp.where(z == 1, 0, z - 2), jnp.where(z == end - 1, end, z + 2))
    before = (jnp.clip(behind, 0, end), xl, 1, y, xh)
    mirror = jnp.where(z >= planes // 2, 1, 0)
    is_late = is_worker & (way != mirror)
    station_first = ((xh == 0) & (y == 0)) | ((xh == 1) & (y == stations - 1))
    station_last = ((xh == 0) & (y == stations - 1)) | ((xh == 1) & (y == 0))

    def member(slot, y_to, xh_to):
        return (low + slot // GROUP, (slot % GROUP) // 2, slot % 2, y_to, xh_to)

    def remote(source, target, send_sem, recv_sem, device):
        return pltpu.make_async_remote_copy(
            src_ref=source,
            dst_ref=target,
            send_sem=send_sem,
            recv_sem=recv_sem,
            device_id=device,
            device_id_type=MESH,
        )

    def arrived(target, sem):
        pltpu.make_async_copy(target, target, sem).wait()

    barrier = pltpu.get_barrier_semaphore()

    def greet(device):
        pl.semaphore_signal(barrier, inc=1, device_id=device, device_id_type=MESH)

    def greet_slot(slot, carried):
        @pl.when(slot != mine)
        def _():
            greet(member(slot, y, xh))

        greet(member(slot, y, 1 - xh))
        for step in (1, stations - 1):
            for xh_to in range(2):
                greet(member(slot, (y + step) % stations, xh_to))
        return carried

    lax.fori_loop(0, count, greet_slot, 0)

    @pl.when(has_next)
    def _():
        greet(after)

    @pl.when(has_prev)
    def _():
        greet(before)

    pl.semaphore_wait(
        barrier, 6 * count - 1 + jnp.where(has_next, 1, 0) + jnp.where(has_prev, 1, 0)
    )

    def chain(index):
        to_way = (index // 2 + jnp.where(z == end, 1, 0)) % 2
        to_col = index % 2
        to_start = ((to_way == 0) & (z == 0)) | ((to_way == 1) & (z == end))
        to_core = jnp.where(at_edge, jnp.where(to_start, 1, 0), 1)
        to_z = jnp.where(at_edge, z, low + to_way)
        own = (to_z == z) & (to_col == xl) & (to_core == core)
        return to_way, to_col, (to_z, to_col, to_core, y, xh), own

    def map_pairs(to_way, to_col):
        return (
            (left_maps.at[to_way, 0, to_col], lefts.at[mine]),
            (right_maps.at[to_way, 0, to_col], rights.at[mine]),
            (kets.at[to_col], ketses.at[mine]),
        )

    def send_map(index, carried):
        to_way, to_col, device, own = chain(index)

        @pl.when(own)
        def _():
            for kind, (source, target) in enumerate(map_pairs(to_way, to_col)):
                pltpu.make_async_copy(source, target, map_recv.at[mine, kind]).start()

        @pl.when(jnp.logical_not(own))
        def _():
            for kind, (source, target) in enumerate(map_pairs(to_way, to_col)):
                remote(
                    source, target, map_send.at[index, kind], map_recv.at[mine, kind], device
                ).start()

        return carried

    def map_sent(index, carried):
        to_way, to_col, device, own = chain(index)

        @pl.when(jnp.logical_not(own))
        def _():
            for kind, (source, target) in enumerate(map_pairs(to_way, to_col)):
                remote(
                    source, target, map_send.at[index, kind], map_recv.at[mine, kind], device
                ).wait_send()

        return carried

    lax.fori_loop(0, 4, send_map, 0)

    half = pl.ds(2 * xh, 2)

    def ket_across():
        device = (z, xl, core, y, 1 - xh)
        return remote(kets, row_kets.at[half], ket_send.at[0], ket_recv.at[xh], device)

    def ket_back():
        device = (z, xl, core, jnp.maximum(y - 1, 0), xh)
        return remote(kets.at[0], row_kets.at[4], ket_send.at[1], ket_recv.at[2], device)

    sends_back = (xh == 0) & (y > 0)
    extra = sends_back & (col == 0)
    gets_back = (xh == 0) & (y < stations - 1)
    ket_across().start()
    pltpu.make_async_copy(kets, row_kets.at[half], ket_recv.at[xh]).start()

    @pl.when(sends_back)
    def _():
        ket_back().start()

    @pl.when(is_worker)
    def _():
        for leg in range(4):
            row, lane = iota((WIDE, WIDE), 0), iota((WIDE, WIDE), 1)
            for _ in range(3):
                lane = jnp.where(lane >= CHI, lane - CHI, lane)
            select_one[:, leg * WIDE : (leg + 1) * WIDE] = jnp.where(
                row == 4 * lane + leg, 1.0, 0.0
            ).astype(BF16)
            row, lane = iota((256, WIDE), 0), iota((256, WIDE), 1)
            inner = row & 127
            select_two[leg * 256 : (leg + 1) * 256, :] = jnp.where(
                (lane == 4 * inner + leg) & (inner < CHI), 1.0, 0.0
            ).astype(BF16)

    @pl.when(is_first & (way == 0))
    def _():
        entered[...] = top_edge[col]

    @pl.when(is_first & (way == 1))
    def _():
        entered[...] = bottom_edge[col]


    def slot_at(number):
        return number + way * (count - 1 - 2 * number)

    def legs(m, g, o, f):
        return pick(way, m, o), f, pick(way, o, m), g

    def prepare(number):
        j = slot_at(number)
        for kind, target in enumerate((lefts, rights, ketses)):
            arrived(target.at[j], map_recv.at[j, kind])
        coeffs[...] = layer_rows(ketses[j], legs)
        apart = dot(jnp.concatenate(thirds(lefts[j]), axis=0), select_one[...])
        for leg in range(4):
            lanes = slice(leg * WIDE, (leg + 1) * WIDE)
            spread[leg] = apart[0:CHI, lanes] + (
                apart[CHI : 2 * CHI, lanes] + apart[2 * CHI : 3 * CHI, lanes]
            )
        high, mid, lowest = thirds(rights[j])
        main = dot_nt(select_two[...], padded((high, mid)))
        fine = dot_nt(select_two[...], padded((lowest,)))
        second[number] = main.astype(BF16)
        even = (iota((1024, 128), 0) & 128) == 0
        third[number] = jnp.where(even, fine, main[:, 0:128]).astype(BF16)
        fold_first(spread, coeffs, folded, number)

    def side_copy(number, source, xh_to, kind):
        return remote(
            source,
            sides.at[way, place],
            row_send.at[number, kind],
            side_recv.at[way, place],
            member(slot_at(number), y, xh_to),
        )

    def back_copy(number, source):
        return remote(
            source,
            sides.at[way, 4],
            row_send.at[number, 3],
            side_recv.at[way, 4],
            member(slot_at(number), jnp.maximum(y - 1, 0), xh),
        )

    def out_copy(number):
        return remote(
            normed.at[number + 1],
            outs.at[way, col],
            row_send.at[number, 2],
            out_recv.at[way, col],
            member(slot_at(number), y, xh),
        )

    def send_sides(number, source):
        own = slot_at(number) == mine

        @pl.when(own)
        def _():
            pltpu.make_async_copy(
                source, sides.at[way, place], side_recv.at[way, place]
            ).start()

        @pl.when(jnp.logical_not(own))
        def _():
            side_copy(number, source, xh, 0).start()

        side_copy(number, source, 1 - xh, 1).start()

        @pl.when(extra)
        def _():
            back_copy(number, source).start()

    def send_out(number, carried):
        own = slot_at(number) == mine

        @pl.when(own)
        def _():
            pltpu.make_async_copy(
                normed.at[number + 1], outs.at[way, col], out_recv.at[way, col]
            ).start()

        @pl.when(jnp.logical_not(own))
        def _():
            out_copy(number).start()

        return carried

    def hop():
        return remote(leaving, entered, hop_send, hop_recv, after)

    def tiles_of(value):
        return [value[leg * CHI : (leg + 1) * CHI] for leg in range(4)]

    def advance(number):
        @pl.when(number == 0)
        def _():
            @pl.when(has_prev)
            def _():
                arrived(entered, hop_recv)

            for leg, tile in enumerate(unpack(entered[...])):
                state[leg * CHI : (leg + 1) * CHI, :] = tile

        raw = is_first & (number == 0)
        closes = is_last & (number == count - 1)

        @pl.when(closes)
        def _():
            held = state[...]
            last_in[...] = pack(tiles_of(held)) * nrm_scale(held)
            send_sides(number, last_in)

        current = state[...]
        scale = jnp.where(raw, 1.0, nrm_scale(current))
        renewed = apply_layer(current, scale, folded, second, third, number, middle)
        normed[number] = pack(tiles_of(current)) * scale
        state[...] = renewed

        @pl.when(number == count - 1)
        def _():
            final = state[...]
            leaving[...] = pack(tiles_of(final))

            @pl.when(has_next)
            def _():
                hop().start()

            normed[count] = leaving[...] * nrm_scale(final)

        @pl.when(jnp.logical_not(closes))
        def _():
            send_sides(number, normed.at[number])

        @pl.when(number == count - 1)
        def _():
            lax.fori_loop(0, count, send_out, 0)


    def column_at(number):
        return number + xh * (3 - 2 * number)

    def env_legs(m, g, o, f):
        return pick(mirror, f, g), pick(xh, m, o), pick(mirror, g, f), pick(xh, o, m)

    def env_selects():
        for part in range(2):
            arrived(row_kets.at[pl.ds(2 * part, 2)], ket_recv.at[part])

        @pl.when(xh == 0)
        def _():
            row, lane = iota((2 * CHI, WIDE), 0), iota((2 * CHI, WIDE), 1)
            row = jnp.where(row >= CHI, row - CHI, row)
            for _ in range(3):
                lane = jnp.where(lane >= CHI, lane - CHI, lane)
            select_one[0 : 2 * CHI, 0:WIDE] = jnp.where(row == lane, 1.0, 0.0).astype(BF16)

        @pl.when(xh == 1)
        def _():
            for leg in range(4):
                row, lane = iota((WIDE, WIDE), 0), iota((WIDE, WIDE), 1)
                for _ in range(3):
                    lane = jnp.where(lane >= CHI, lane - CHI, lane)
                select_one[:, leg * WIDE : (leg + 1) * WIDE] = jnp.where(
                    row == leg * CHI + lane, 1.0, 0.0
                ).astype(BF16)
                row, lane = iota((256, WIDE), 0), iota((256, WIDE), 1)
                inner = row & 127
                select_two[leg * 256 : (leg + 1) * 256, :] = jnp.where(
                    (lane == leg * CHI + inner) & (inner < CHI), 1.0, 0.0
                ).astype(BF16)

    def env_fold(number):
        @pl.when(number == 0)
        def _():
            env_selects()

        column = column_at(number)
        arrived(sides.at[mirror, column], side_recv.at[mirror, column])
        coeffs[...] = layer_rows(row_kets[column], env_legs)
        early = jnp.concatenate(halves(sides[mirror, column]), axis=0)

        @pl.when(xh == 0)
        def _():
            turned = lax.dot_general(
                early,
                select_one[0 : 2 * CHI, 0:WIDE],
                (((0,), (0,)), ((), ())),
                preferred_element_type=F32,
            )
            for leg in range(4):
                spread[leg] = turned[leg * CHI : (leg + 1) * CHI]

        @pl.when(xh == 1)
        def _():
            apart = dot(early, select_one[...])
            for leg in range(4):
                lanes = slice(leg * WIDE, (leg + 1) * WIDE)
                spread[leg] = apart[0:CHI, lanes] + apart[CHI : 2 * CHI, lanes]

        fold_pair(spread, coeffs, env_folded, number)

    def env_prepare(number):
        column = column_at(number)
        arrived(sides.at[1 - mirror, column], side_recv.at[1 - mirror, column])

        @pl.when(xh == 0)
        def _():
            for leg, tile in enumerate(unpack(sides[1 - mirror, column])):
                high, lowest = halves(tile)
                both = jnp.concatenate(
                    [jnp.concatenate([high, lowest], axis=1), jnp.zeros((32, 256), BF16)], axis=0
                )
                env_second[number, leg * 256 : leg * 256 + 128, :] = both
                env_second[number, leg * 256 + 128 : leg * 256 + 256, :] = both

        @pl.when(xh == 1)
        def _():
            late = padded(halves(sides[1 - mirror, column]))
            env_second[number] = dot_nt(select_two[...], late).astype(BF16)

    def env_hop():
        device = (z, xl, core, jnp.clip(y + 1 - 2 * xh, 0, stations - 1), xh)
        return remote(env_leaving, env_entered, env_send, env_recv, device)

    def over(number):
        column = column_at(number)
        wraps = column == 0
        slot = jnp.where(wraps, 3, jnp.maximum(column - 1, 0))
        y_to = jnp.where(wraps, jnp.maximum(y - 1, 0), y)
        return remote(
            env_normed.at[number],
            from_right.at[slot],
            over_send.at[number],
            over_recv.at[slot],
            (z, xl, core, y_to, 0),
        )

    def sends_over(number):
        return (xh == 1) & ((y > 0) | (column_at(number) > 0))

    def flipped(tile):
        square = jnp.concatenate([tile, jnp.zeros((32, 128), F32)], axis=0)
        return square.T[0:CHI, :]

    def env_advance(number):
        @pl.when(number == 0)
        def _():
            @pl.when(jnp.logical_not(station_first))
            def _():
                arrived(env_entered, env_recv)
                for leg, tile in enumerate(unpack(env_entered[...])):
                    state[leg * CHI : (leg + 1) * CHI, :] = tile

            @pl.when(station_first)
            def _():
                edge = jnp.where(xh == 0, left_edge[0], right_edge[0])
                for leg, tile in enumerate(unpack(edge)):
                    state[leg * CHI : (leg + 1) * CHI, :] = jnp.where(
                        mirror == 1, flipped(tile), tile
                    )

        raw = station_first & (number == 0)

        @pl.when(jnp.logical_not(station_last & (number >= 2)))
        def _():
            current = state[...]
            scale = jnp.where(raw, 1.0, nrm_scale(current))
            renewed = apply_pair(current, scale, env_folded, env_second, number, middle)
            env_normed[number] = pack(tiles_of(current)) * scale
            state[...] = renewed

        @pl.when(station_last & (number >= 2))
        def _():
            current = state[...]
            env_normed[number] = pack(tiles_of(current)) * nrm_scale(current)

        @pl.when(jnp.logical_not(station_last) & (number == 3))
        def _():
            env_leaving[...] = pack(tiles_of(state[...]))
            env_hop().start()

        @pl.when(xh == 0)
        def _():
            from_left[number] = env_normed[number]

        @pl.when(sends_over(number))
        def _():
            over(number).start()


    total = jnp.where(is_worker, 2 * count, 0)
    before_fold = jnp.where(is_late, count, total)

    def task(index, carried):
        folds = (index >= before_fold) & (index < before_fold + 4)
        on_env = index >= total + 4
        on_boundary = jnp.logical_not(folds) & jnp.logical_not(on_env)
        step = jnp.where(index < before_fold, index, index - 4)
        prepares = (is_first & (step % 2 == 0)) | (jnp.logical_not(is_first) & (step < count))

        @pl.when(on_boundary & prepares)
        def _():
            prepare(jnp.where(is_first, step // 2, jnp.clip(step, 0, count - 1)))

        @pl.when(on_boundary & jnp.logical_not(prepares))
        def _():
            advance(jnp.where(is_first, step // 2, jnp.clip(step - count, 0, count - 1)))

        @pl.when(folds)
        def _():
            env_fold(jnp.clip(index - before_fold, 0, 3))

        late = index - (total + 4)
        readies = (station_first & (late % 2 == 0)) | (
            jnp.logical_not(station_first) & (late < 4)
        )

        @pl.when(on_env & readies)
        def _():
            env_prepare(jnp.where(station_first, late // 2, jnp.clip(late, 0, 3)))

        @pl.when(on_env & jnp.logical_not(readies))
        def _():
            env_advance(jnp.where(station_first, late // 2, jnp.clip(late - 4, 0, 3)))

        return carried

    lax.fori_loop(0, total + 12, task, 0)


    lax.fori_loop(0, 4, map_sent, 0)

    @pl.when(has_next)
    def _():
        hop().wait_send()

    def row_sent(number, carried):
        source = normed.at[number]
        side_copy(number, source, 1 - xh, 1).wait_send()

        @pl.when(extra)
        def _():
            back_copy(number, source).wait_send()

        @pl.when(slot_at(number) != mine)
        def _():
            side_copy(number, source, xh, 0).wait_send()
            out_copy(number).wait_send()

        return carried

    lax.fori_loop(0, total // 2, row_sent, 0)
    ket_across().wait_send()

    @pl.when(sends_back)
    def _():
        ket_back().wait_send()

    @pl.when(jnp.logical_not(station_last))
    def _():
        env_hop().wait_send()

    for number in range(4):

        @pl.when(sends_over(number))
        def _():
            over(number).wait_send()

    for direction in range(2):
        for column in range(2):
            arrived(outs.at[direction, column], out_recv.at[direction, column])

    @pl.when(gets_back)
    def _():
        for direction in range(2):
            arrived(sides.at[direction, 4], side_recv.at[direction, 4])
        arrived(row_kets.at[4], ket_recv.at[2])

    @pl.when(xh == 0)
    def _():
        for slot in range(3):
            arrived(from_right.at[slot], over_recv.at[slot])

    @pl.when(gets_back)
    def _():
        arrived(from_right.at[3], over_recv.at[3])


def run_sweep(kets, left_maps, right_maps, top_edge, bottom_edge, left_edge, right_edge):
    vmem = pl.BlockSpec(memory_space=pltpu.VMEM)
    anywhere = pl.BlockSpec(memory_space=pl.ANY)
    column = (CHI, WIDE)
    most = 2 * GROUP
    dma = pltpu.SemaphoreType.DMA
    return pl.pallas_call(
        sweep_kernel,
        out_shape=(
            jax.ShapeDtypeStruct((2, 2) + column, F32),
            jax.ShapeDtypeStruct((2, 5) + column, F32),
            jax.ShapeDtypeStruct((5, 32, 128), F32),
            jax.ShapeDtypeStruct((4,) + column, F32),
            jax.ShapeDtypeStruct((4,) + column, F32),
        ),
        in_specs=[vmem, anywhere, anywhere] + [vmem] * 4,
        out_specs=(vmem,) * 5,
        scratch_shapes=[
            pltpu.VMEM((most,) + column, F32),
            pltpu.VMEM((most,) + column, F32),
            pltpu.VMEM((most, 32, 128), F32),
            pltpu.VMEM((WIDE, 4 * WIDE), BF16),
            pltpu.VMEM((1024, WIDE), BF16),
            pltpu.VMEM((4,) + column, F32),
            pltpu.VMEM((64, WIDE), F32),
            pltpu.VMEM((most, 16 * CHI, 3 * WIDE), BF16),
            pltpu.VMEM((most, 1024, 256), BF16),
            pltpu.VMEM((most, 1024, 128), BF16),
            pltpu.VMEM((4, 16 * CHI, 2 * WIDE), BF16),
            pltpu.VMEM((4, 1024, 256), BF16),
            pltpu.VMEM((WIDE, 2048), BF16),
            pltpu.VMEM(column, F32),
            pltpu.VMEM(column, F32),
            pltpu.VMEM((WIDE, 128), F32),
            pltpu.VMEM((most + 1,) + column, F32),
            pltpu.VMEM(column, F32),
            pltpu.VMEM(column, F32),
            pltpu.VMEM(column, F32),
            pltpu.VMEM((4,) + column, F32),
            dma((4, 3)),
            dma((most, 3)),
            dma,
            dma,
            dma((most, 4)),
            dma((2, 2)),
            dma((2, 5)),
            dma((2,)),
            dma((3,)),
            dma,
            dma,
            dma((4,)),
            dma((4,)),
        ],
        compiler_params=pltpu.CompilerParams(
            collective_id=0, has_side_effects=True, vmem_limit_bytes=67043328
        ),
        name="sweep",
    )(kets, left_maps, right_maps, top_edge, bottom_edge, left_edge, right_edge)


def dot_general(left, right, dims):
    return lax.dot_general(left, right, (dims, ((), ())), preferred_element_type=F32)


def pad_rows(value):
    return jnp.concatenate([value, jnp.zeros((32, value.shape[1]), value.dtype)], axis=0)


def swap_legs(entry):
    return (entry & 0b10101) | ((entry >> 3) & 1) << 1 | ((entry >> 1) & 1) << 3


def open_site(ket, legs_at, wide, opened):
    def body(block, carried):
        begin = pl.multiple_of(block * 8, 8)
        half_done = {}
        for bra in range(8):
            u2, m2, d2 = bra >> 2, (bra >> 1) & 1, bra & 1
            tiles = []
            for top in range(8):
                u, m, d = top >> 2, (top >> 1) & 1, top & 1
                row = (2 * m + m2) * 4 + 2 * u + u2
                lane = (2 * d + d2) * 128
                tiles.append(wide[pl.ds(row * CHI + begin, 8), lane : lane + 128])
            for state in range(2):
                for out in range(2):
                    total = None
                    for top in range(8):
                        at = state * 16 + legs_at(top >> 2, (top >> 1) & 1, top & 1, out)
                        term = ket[at : at + 1, :] * tiles[top]
                        total = term if total is None else total + term
                    half_done[state, out, bra] = total
        for state in range(2):
            for out in range(2):
                for other in range(2):
                    for out2 in range(2):
                        total = None
                        for bra in range(8):
                            at = other * 16 + legs_at(bra >> 2, (bra >> 1) & 1, bra & 1, out2)
                            term = ket[at : at + 1, :] * half_done[state, out, bra]
                            total = term if total is None else total + term
                        row = (2 * out + out2) * CHI
                        opened[state * 2 + other, pl.ds(row + begin, 8), :] = total
        return carried

    lax.fori_loop(0, CHI // 8, body, 0)


def energy_kernel(
    term_rows,
    term_bonds,
    term_ops,
    operators,
    sides,
    row_kets,
    from_left,
    from_right,
    shares,
    wide,
    opened,
    closing,
    density,
    ket,
):
    way = lax.axis_index("cols_1")
    row_here = (
        lax.axis_index("rows_0") * GROUP + lax.axis_index("rows_1") * 2 + lax.axis_index("rows_2")
    )
    first = lax.axis_index("cols_0") * 4
    planes = lax.axis_size("rows_0")
    mirror = jnp.where(lax.axis_index("rows_0") >= planes // 2, 1, 0)

    def take_ket(column):
        for entry in range(32):
            ket[entry : entry + 1, :] = jnp.where(
                mirror == 1,
                row_kets[column, swap_legs(entry) : swap_legs(entry) + 1, :],
                row_kets[column, entry : entry + 1, :],
            )

    shares[...] = jnp.zeros((8, 128), F32)

    def hits(term, column):
        here = (term_rows[term] == row_here) & (term_bonds[term] == first + column)
        return here & (way == 0)

    def column_body(column, carried):
        count = 0
        for term in range(TERMS):
            count = count + jnp.where(hits(term, column), 1, 0)

        @pl.when(count > 0)
        def _():
            high, low = halves(sides[mirror, column])
            both = jnp.concatenate([high, low], axis=0)
            state_high, state_low = halves(jnp.concatenate(unpack(from_left[column]), axis=1))
            tn = ((0,), (0,))
            joined = dot_general(
                both, jnp.concatenate([state_high, state_high], axis=0), tn
            ) + dot_general(both, jnp.concatenate([state_low, state_low], axis=0), tn)
            below_high, below_low = halves(jnp.concatenate(unpack(sides[1 - mirror, column]), axis=1))
            main = jnp.concatenate([pad_rows(below_high), pad_rows(below_high)], axis=0)
            fine = jnp.concatenate([pad_rows(below_low), pad_rows(below_low)], axis=0)
            for leg in range(4):
                part = jnp.concatenate(halves(joined[:, leg * 128 : (leg + 1) * 128]), axis=1)
                wide[leg * WIDE : (leg + 1) * WIDE, :] = dot(part, main) + dot(part, fine)
            take_ket(column)
            open_site(
                ket,
                lambda u, m, d, out: u * 8 + m * 4 + d * 2 + out,
                wide,
                opened,
            )

            right = column + 1
            above = jnp.concatenate(unpack(sides[mirror, right]), axis=0)
            both = jnp.concatenate(halves(above), axis=1)
            state_high, state_low = halves(jnp.concatenate(unpack(from_right[column]), axis=1))
            state_high, state_low = pad_rows(state_high), pad_rows(state_low)
            joined = dot(both, jnp.concatenate([state_high, state_high], axis=0)) + dot(
                both, jnp.concatenate([state_low, state_low], axis=0)
            )
            below_high, below_low = halves(
                jnp.concatenate([pad_rows(tile) for tile in unpack(sides[1 - mirror, right])], axis=0)
            )
            main = jnp.concatenate([below_high, below_high], axis=1)
            fine = jnp.concatenate([below_low, below_low], axis=1)
            for leg in range(4):
                part = jnp.concatenate(halves(joined[:, leg * 128 : (leg + 1) * 128]), axis=1)
                wide[leg * WIDE : (leg + 1) * WIDE, :] = dot_nt(part, main) + dot_nt(part, fine)
            take_ket(right)
            open_site(
                ket,
                lambda u, m, d, out: u * 8 + out * 4 + d * 2 + m,
                wide,
                closing,
            )

            for pair in range(4):
                for other in range(4):
                    product = opened[pair] * closing[other]
                    at = pair * 4 + other
                    density[at : at + 1, :] = jnp.sum(product, axis=0, keepdims=True)
            rho = jnp.sum(density[...], axis=1, keepdims=True)
            index = iota((16, 1), 0)
            diagonal = (index == 0) | (index == 3) | (index == 12) | (index == 15)
            trace = jnp.sum(jnp.where(diagonal, rho, 0.0), axis=0, keepdims=True)
            spread = jnp.sqrt(jnp.sum(rho * rho, axis=0, keepdims=True))
            bottom = jnp.maximum(jnp.abs(trace), 0.25 * spread)

            def term_body(term, kept):
                @pl.when(hits(term, column))
                def _():
                    chosen = jnp.zeros((16, 1), F32)
                    for entry in range(16):
                        chosen = jnp.where(
                            index == entry, operators[term_ops[term], entry], chosen
                        )
                    value = jnp.sum(chosen * rho, axis=0, keepdims=True) / bottom
                    lane = iota((8, 128), 1)
                    shares[...] = jnp.where(lane == term, value, shares[...])

                return kept

            lax.fori_loop(0, TERMS, term_body, 0)

        return carried

    lax.fori_loop(0, 4, column_body, 0)


def run_energies(term_rows, term_bonds, term_ops, operators, sides, row_kets, lefts, rights):
    vmem = pl.BlockSpec(memory_space=pltpu.VMEM)
    smem = pl.BlockSpec(memory_space=pltpu.SMEM)
    return pl.pallas_call(
        energy_kernel,
        out_shape=jax.ShapeDtypeStruct((8, 128), F32),
        in_specs=[smem] * 4 + [vmem] * 4,
        out_specs=vmem,
        scratch_shapes=[
            pltpu.VMEM((16 * CHI, 512), F32),
            pltpu.VMEM((4, WIDE, 128), F32),
            pltpu.VMEM((4, WIDE, 128), F32),
            pltpu.VMEM((16, 128), F32),
            pltpu.VMEM((32, 128), F32),
        ],
        compiler_params=pltpu.CompilerParams(vmem_limit_bytes=32 * 1024 * 1024),
        name="energies",
    )(term_rows, term_bonds, term_ops, operators, sides, row_kets, lefts, rights)


def sum_kernel(shares, total, planes_in, plane_in, partial, send_one, recv_one, send_two, recv_two):
    z = lax.axis_index("rows_0")
    xl = lax.axis_index("rows_1")
    core = lax.axis_index("rows_2")
    y = lax.axis_index("cols_0")
    way = lax.axis_index("cols_1")
    place = y * 4 + xl * 2 + core
    barrier = pltpu.get_barrier_semaphore()

    def greet(device):
        pl.semaphore_signal(barrier, inc=1, device_id=device, device_id_type=MESH)

    def along(step):
        return ((z + step) % 8, xl, core, y, way)

    def within(step):
        other = (place * 2 + way + step) % 32
        return (z, (other // 4) % 2, (other // 2) % 2, other // 8, other % 2)

    for step in range(1, 8):
        greet(along(step))
    for step in range(1, 32):
        greet(within(step))
    pl.semaphore_wait(barrier, 38)

    def first(step):
        return pltpu.make_async_remote_copy(
            src_ref=shares,
            dst_ref=planes_in.at[z],
            send_sem=send_one.at[step],
            recv_sem=recv_one.at[z],
            device_id=along(step),
            device_id_type=MESH,
        )

    def second(step):
        return pltpu.make_async_remote_copy(
            src_ref=partial,
            dst_ref=plane_in.at[place],
            send_sem=send_two.at[step],
            recv_sem=recv_two.at[place],
            device_id=within(step),
            device_id_type=MESH,
        )

    @pl.when(way == 0)
    def _():
        for step in range(1, 8):
            first(step).start()
        pltpu.make_async_copy(shares, planes_in.at[z], recv_one.at[z]).start()
        added = None
        for plane in range(8):
            target = planes_in.at[plane]
            pltpu.make_async_copy(target, target, recv_one.at[plane]).wait()
        for plane in range(8):
            added = planes_in[plane] if added is None else added + planes_in[plane]
        partial[...] = added
        for step in range(1, 32):
            second(step).start()
        pltpu.make_async_copy(partial, plane_in.at[place], recv_two.at[place]).start()

    for other in range(16):
        target = plane_in.at[other]
        pltpu.make_async_copy(target, target, recv_two.at[other]).wait()
    added = None
    for other in range(16):
        added = plane_in[other] if added is None else added + plane_in[other]
    total[...] = added

    @pl.when(way == 0)
    def _():
        for step in range(1, 8):
            first(step).wait_send()
        for step in range(1, 32):
            second(step).wait_send()


def run_sum(shares):
    vmem = pl.BlockSpec(memory_space=pltpu.VMEM)
    return pl.pallas_call(
        sum_kernel,
        out_shape=jax.ShapeDtypeStruct((8, 128), F32),
        in_specs=[vmem],
        out_specs=vmem,
        scratch_shapes=[
            pltpu.VMEM((8, 8, 128), F32),
            pltpu.VMEM((16, 8, 128), F32),
            pltpu.VMEM((8, 128), F32),
            pltpu.SemaphoreType.DMA((8,)),
            pltpu.SemaphoreType.DMA((8,)),
            pltpu.SemaphoreType.DMA((32,)),
            pltpu.SemaphoreType.DMA((16,)),
        ],
        compiler_params=pltpu.CompilerParams(collective_id=2, has_side_effects=True),
        name="shares_sum",
    )(shares)


def shards(
    kets,
    left_maps,
    right_maps,
    top_edge,
    bottom_edge,
    left_edge,
    right_edge,
    term_rows,
    term_bonds,
    term_ops,
    operators,
):
    spread_kets = jnp.broadcast_to(kets[0][:, :, None], (kets.shape[1], 32, 128))
    outs, sides, row_kets, lefts, rights = run_sweep(
        spread_kets, left_maps, right_maps, top_edge, bottom_edge, left_edge, right_edge
    )
    shares = run_energies(
        term_rows, term_bonds, term_ops, operators, sides, row_kets, lefts, rights
    )
    energies = run_sum(shares)[0, :TERMS]
    return (outs[0][None], outs[1][None], energies)


def solution(mesh):
    torus = Mesh(
        mesh.devices.reshape(8, 2, 2, 4, 2), ("rows_0", "rows_1", "rows_2", "cols_0", "cols_1")
    )
    placed = (
        P(ROWS, COLS, None),
        P(None, ROWS, COLS, None, None),
        P(None, ROWS, COLS, None, None),
        P(COLS, None, None),
        P(COLS, None, None),
        P(ROWS, None, None),
        P(ROWS, None, None),
        P(),
        P(),
        P(),
        P(),
    )
    return jax.shard_map(
        shards,
        mesh=torus,
        in_specs=placed,
        out_specs=(P(ROWS, COLS, None, None), P(ROWS, COLS, None, None), P()),
        check_vma=False,
    )
```

```python
import functools

import jax
import jax.numpy as jnp
from jax import lax
from jax.experimental import pallas as pl
from jax.experimental.pallas import tpu as pltpu
from jax.sharding import Mesh
from jax.sharding import PartitionSpec as P

D = 2
D2 = 4
PHYS = 2
CHI = 96
WIDE = D2 * CHI
OPS = 4
TERMS = 16
GROUP = 4
ROWS = ("rows_0", "rows_1", "rows_2")
COLS = ("cols_0", "cols_1")
ROWS_COLS = ("rows_0", "rows_1", "rows_2", "cols_0", "cols_1")
MESH = pl.DeviceIdType.MESH

EPSILON = 1e-06
PRECISION_HIGH = lax.Precision.HIGHEST
F32 = jnp.float32
BF16 = jnp.bfloat16


def iota(shape, dim):
    return lax.broadcasted_iota(jnp.int32, shape, dim)


def halves(value):
    high = value.astype(BF16)
    low = (value - high.astype(F32)).astype(BF16)
    return high, low


def dot(left, right):
    return jnp.dot(left, right, preferred_element_type=F32)


def dot_nt(left, right):
    return lax.dot_general(left, right, (((1,), (1,)), ((), ())), preferred_element_type=F32)


def unpack(wide):
    one, two, three = wide[:, 0:128], wide[:, 128:256], wide[:, 256:384]
    lane = iota((CHI, 128), 1)
    parts = (
        one,
        pltpu.roll(jnp.where(lane >= 96, one, two), 32, 1),
        pltpu.roll(jnp.where(lane >= 64, two, three), 64, 1),
        pltpu.roll(three, 96, 1),
    )
    return [jnp.where(lane < CHI, part, 0.0) for part in parts]


def pack(tiles):
    lane = iota((CHI, 128), 1)
    first = tiles[0]
    second = pltpu.roll(tiles[1], 96, 1)
    third = pltpu.roll(tiles[2], 64, 1)
    fourth = pltpu.roll(tiles[3], 32, 1)
    return jnp.concatenate(
        [
            jnp.where(lane < 96, first, second),
            jnp.where(lane < 64, second, third),
            jnp.where(lane < 32, third, fourth),
        ],
        axis=1,
    )


def pick(mode, *choices):
    value = choices[-1]
    for index in range(len(choices) - 1):
        value = jnp.where(mode == index, choices[index], value)
    return value


def layer_picks(legs):
    shape = (PHYS * 256, 32)
    row, col = iota(shape, 0), iota(shape, 1)
    digits = ((row >> 6) & 3, (row >> 4) & 3, (row >> 2) & 3, row & 3)
    up, left, down, right = legs(*digits)
    base = (row >> 8) * 16
    ket_at = base + (up >> 1) * 8 + (left >> 1) * 4 + (down >> 1) * 2 + (right >> 1)
    bra_at = base + (up & 1) * 8 + (left & 1) * 4 + (down & 1) * 2 + (right & 1)
    return jnp.concatenate(
        [jnp.where(col == ket_at, 1.0, 0.0), jnp.where(col == bra_at, 1.0, 0.0)], axis=0
    ).astype(BF16)


def layer_rows(ket, picks):
    parts = dot(picks, jnp.concatenate(thirds(ket), axis=1))
    taken = parts[:, 0:128] + (parts[:, 128:256] + parts[:, 256:384])
    both = taken[0:512] * taken[512:1024]
    full = both[0:256] + both[256:512]
    lane = iota((64, 128), 1)
    at = [full[64 * m : 64 * (m + 1)] for m in range(4)]
    return jnp.concatenate(
        [
            jnp.where(lane < 96, at[0], at[1]),
            jnp.where(lane < 64, at[1], at[2]),
            jnp.where(lane < 32, at[2], at[3]),
        ],
        axis=1,
    )


def thirds(value):
    high = value.astype(BF16)
    rest = value - high.astype(F32)
    middle = rest.astype(BF16)
    low = (rest - middle.astype(F32)).astype(BF16)
    return high, middle, low


def fold_first(spread, coeffs, folded, slot):
    def body(index, carried):
        total = None
        for leg in range(4):
            term = coeffs[pl.ds(index * 4 + leg, 1), :] * spread[leg]
            total = term if total is None else total + term
        high, middle, low = thirds(total)
        rows = pl.ds(pl.multiple_of(index * CHI, CHI), CHI)
        folded[slot, rows, 0:WIDE] = low
        folded[slot, rows, WIDE : 2 * WIDE] = high
        folded[slot, rows, 2 * WIDE : 3 * WIDE] = middle
        return carried

    lax.fori_loop(0, 16, body, 0)


def padded(parts):
    blank = jnp.zeros((32, parts[0].shape[1]), BF16)
    return jnp.concatenate([piece for part in parts for piece in (part, blank)], axis=0)


def apply_layer(state, scale, folded, second, third, slot, middle):
    high, mid, low = thirds(state)
    once = jnp.concatenate([high, mid], axis=1)
    main = jnp.concatenate([once, once], axis=0)
    fine = jnp.concatenate([high, low], axis=0)
    for leg in range(4):
        rows = slice(leg * WIDE, (leg + 1) * WIDE)
        wide = dot(folded[slot, rows, WIDE : 3 * WIDE], main)
        rest = dot(folded[slot, rows, 0 : 2 * WIDE], fine)
        high, mid, low = thirds(wide[:, 0:128] + (wide[:, 128:256] + rest))
        for index, part in enumerate((high, mid)):
            middle[:, leg * 256 + index * 128 : leg * 256 + index * 128 + 128] = part
        for index, part in enumerate((high, low)):
            begin = 1024 + leg * 256 + index * 128
            middle[:, begin : begin + 128] = part
    wide = dot(middle[:, 0:1024], second[slot])
    rest = dot(middle[:, 1024:2048], third[slot])
    return (wide[:, 0:128] + (wide[:, 128:256] + rest)) * scale


def nrm_scale(state):
    total = jnp.sum(jnp.sum(state * state, axis=0, keepdims=True), axis=1, keepdims=True)
    return lax.rsqrt(total * (1.0 / (CHI * WIDE)) + EPSILON)


def fold_pair(spread, coeffs, folded, slot):
    def body(index, carried):
        total = None
        for leg in range(4):
            term = coeffs[pl.ds(index * 4 + leg, 1), :] * spread[leg]
            total = term if total is None else total + term
        high, low = halves(total)
        rows = pl.ds(pl.multiple_of(index * CHI, CHI), CHI)
        folded[slot, rows, 0:WIDE] = high
        folded[slot, rows, WIDE : 2 * WIDE] = low
        return carried

    lax.fori_loop(0, 16, body, 0)


def apply_pair(state, scale, folded, second, slot, middle):
    high, low = halves(state)
    once = jnp.concatenate([high, low], axis=1)
    twice = jnp.concatenate([once, once], axis=0)
    for leg in range(4):
        wide = dot(folded[slot, leg * WIDE : (leg + 1) * WIDE, :], twice)
        high, low = halves(wide[:, 0:128] + wide[:, 128:256])
        middle[:, leg * 256 : leg * 256 + 128] = high
        middle[:, leg * 256 + 128 : leg * 256 + 256] = low
    wide = dot(middle[:, 0:1024], second[slot])
    return (wide[:, 0:128] + wide[:, 128:256]) * scale


def sweep_kernel(
    kets,
    left_maps,
    right_maps,
    top_edge,
    bottom_edge,
    left_edge,
    right_edge,
    outs,
    sides,
    row_kets,
    from_left,
    from_right,
    lefts,
    rights,
    ketses,
    select_one,
    select_two,
    spread,
    coeffs,
    picks,
    folded,
    second,
    third,
    env_folded,
    env_second,
    middle,
    entered,
    leaving,
    state,
    normed,
    last_in,
    env_entered,
    env_leaving,
    env_normed,
    map_send,
    map_recv,
    hop_send,
    hop_recv,
    row_send,
    out_recv,
    side_recv,
    ket_send,
    ket_recv,
    edge_send,
    pass_send,
    back_send,
    env_send,
    env_recv,
    over_send,
    over_recv,
):
    z = lax.axis_index("rows_0")
    xl = lax.axis_index("rows_1")
    core = lax.axis_index("rows_2")
    y = lax.axis_index("cols_0")
    xh = lax.axis_index("cols_1")
    planes = lax.axis_size("rows_0")
    stations = lax.axis_size("cols_0")
    end = planes - 1
    at_edge = (z == 0) | (z == end)
    low = jnp.where(at_edge, z, 1 + 2 * (jnp.maximum(z - 1, 0) // 2))
    count = jnp.where(at_edge, GROUP, 2 * GROUP)
    col = xl
    is_worker = at_edge | (core == 1)
    way = jnp.where(z == 0, 1 - core, jnp.where(z == end, core, z % 2))
    starts = ((way == 0) & (z == 0)) | ((way == 1) & (z == end))
    is_first = at_edge & starts
    is_last = at_edge & jnp.logical_not(starts)
    has_next = is_worker & jnp.logical_not(is_last)
    has_prev = is_worker & jnp.logical_not(is_first)
    mine = (z - low) * GROUP + xl * 2 + core
    place = xh * 2 + col
    ahead = z + 2 - 4 * way
    ahead = jnp.clip(ahead, 0, end)
    after = (ahead, xl, jnp.where((ahead == 0) | (ahead == end), 0, 1), y, xh)
    behind = jnp.where(
        way == 0, jnp.where(z == end, end - 1, z - 2), jnp.where(z == 0, 1, z + 2)
    )
    before = (jnp.clip(behind, 0, end), xl, 1, y, xh)
    mirror = jnp.where(z >= planes // 2, 1, 0)
    in_middle = (z == planes // 2) | (z == planes // 2 - 1)
    is_late = is_worker & (way != mirror) & jnp.logical_not(in_middle)
    station_first = ((core == 0) & (y == 0)) | ((core == 1) & (y == stations - 1))
    station_last = ((core == 0) & (y == stations - 1)) | ((core == 1) & (y == 0))
    leader = jnp.where(y >= stations // 2, 1, 0)

    def member(slot, y_to, xh_to):
        return (low + slot // GROUP, (slot % GROUP) // 2, slot % 2, y_to, xh_to)

    def env_member(slot):
        return (low + slot // GROUP, slot % 2, leader, y, (slot % GROUP) // 2)

    def remote(source, target, send_sem, recv_sem, device):
        return pltpu.make_async_remote_copy(
            src_ref=source,
            dst_ref=target,
            send_sem=send_sem,
            recv_sem=recv_sem,
            device_id=device,
            device_id_type=MESH,
        )

    def arrived(target, sem):
        pltpu.make_async_copy(target, target, sem).wait()

    barrier = pltpu.get_barrier_semaphore()

    def greet(device):
        pl.semaphore_signal(barrier, inc=1, device_id=device, device_id_type=MESH)

    def greet_slot(slot, carried):
        @pl.when(slot != mine)
        def _():
            greet(member(slot, y, xh))

        greet(member(slot, y, 1 - xh))
        for step in (1, stations - 1):
            for xh_to in range(2):
                greet(member(slot, (y + step) % stations, xh_to))
        return carried

    lax.fori_loop(0, count, greet_slot, 0)

    @pl.when(has_next)
    def _():
        greet(after)

    @pl.when(has_prev)
    def _():
        greet(before)

    def legs(m, g, o, f):
        return pick(way, m, o), f, pick(way, o, m), g

    @pl.when(is_worker)
    def _():
        for leg in range(4):
            row, lane = iota((WIDE, WIDE), 0), iota((WIDE, WIDE), 1)
            for _ in range(3):
                lane = jnp.where(lane >= CHI, lane - CHI, lane)
            select_one[:, leg * WIDE : (leg + 1) * WIDE] = jnp.where(
                row == 4 * lane + leg, 1.0, 0.0
            ).astype(BF16)
            row, lane = iota((128, WIDE), 0), iota((128, WIDE), 1)
            select_two[leg * 128 : (leg + 1) * 128, :] = jnp.where(
                (lane == 4 * row + leg) & (row < CHI), 1.0, 0.0
            ).astype(BF16)
        picks[...] = layer_picks(legs)

    pl.semaphore_wait(
        barrier, 6 * count - 1 + jnp.where(has_next, 1, 0) + jnp.where(has_prev, 1, 0)
    )

    def chain(index):
        to_way = (index // 2 + jnp.where(z == end, 1, 0)) % 2
        to_col = index % 2
        to_start = ((to_way == 0) & (z == 0)) | ((to_way == 1) & (z == end))
        to_core = jnp.where(at_edge, jnp.where(to_start, 1, 0), 1)
        to_z = jnp.where(at_edge, z, low + 1 - to_way)
        own = (to_z == z) & (to_col == xl) & (to_core == core)
        return to_way, to_col, (to_z, to_col, to_core, y, xh), own

    def map_pairs(to_way, to_col):
        return (
            (left_maps.at[to_way, 0, to_col], lefts.at[mine]),
            (right_maps.at[to_way, 0, to_col], rights.at[mine]),
            (kets.at[to_col], ketses.at[mine]),
        )

    def send_map(index, carried):
        to_way, to_col, device, own = chain(index)

        @pl.when(own)
        def _():
            for kind, (source, target) in enumerate(map_pairs(to_way, to_col)):
                pltpu.make_async_copy(source, target, map_recv.at[mine, kind]).start()

        @pl.when(jnp.logical_not(own))
        def _():
            for kind, (source, target) in enumerate(map_pairs(to_way, to_col)):
                remote(
                    source, target, map_send.at[index, kind], map_recv.at[mine, kind], device
                ).start()

        return carried

    def map_sent(index, carried):
        to_way, to_col, device, own = chain(index)

        @pl.when(jnp.logical_not(own))
        def _():
            for kind, (source, target) in enumerate(map_pairs(to_way, to_col)):
                remote(
                    source, target, map_send.at[index, kind], map_recv.at[mine, kind], device
                ).wait_send()

        return carried

    lax.fori_loop(0, 4, send_map, 0)

    half = pl.ds(2 * xh, 2)
    at_home = (core == xl) & (xl == xh)

    def ket_copy(to_core):
        device = (z, core, to_core, y, xl)
        return remote(kets, row_kets.at[half], ket_send.at[to_core], ket_recv.at[xh], device)

    def ket_back():
        device = (z, core, 0, jnp.maximum(y - 1, 0), xl)
        return remote(kets.at[0], row_kets.at[4], ket_send.at[2], ket_recv.at[2], device)

    def edge_copy(edge, to_core):
        return remote(edge.at[0], env_entered, edge_send, env_recv, (z, core, to_core, y, xl))

    for to_core in range(2):

        @pl.when(at_home & (core == to_core))
        def _():
            pltpu.make_async_copy(kets, row_kets.at[half], ket_recv.at[xh]).start()

        @pl.when(jnp.logical_not(at_home & (core == to_core)))
        def _():
            ket_copy(to_core).start()

    sends_back = (core == 0) & (y > 0)
    gets_back = (core == 0) & (y < stations - 1)
    kets_back = (xh == 0) & (y > 0)

    @pl.when(kets_back)
    def _():
        ket_back().start()

    edges = ((left_edge, 0, 0), (right_edge, 1, stations - 1))
    for edge, to_core, y_of in edges:

        @pl.when((y == y_of) & (xh == xl) & at_home & (core == to_core))
        def _():
            pltpu.make_async_copy(edge.at[0], env_entered, env_recv).start()

        @pl.when((y == y_of) & (xh == xl) & jnp.logical_not(at_home & (core == to_core)))
        def _():
            edge_copy(edge, to_core).start()

    @pl.when(is_first & (way == 0))
    def _():
        entered[...] = top_edge[col]

    @pl.when(is_first & (way == 1))
    def _():
        entered[...] = bottom_edge[col]


    def slot_at(number):
        return number + way * (count - 1 - 2 * number)

    def prepare(step):
        ordered = slot_at(step)
        j = jnp.where(is_first, ordered, (mine + step) % count)
        number = j + way * (count - 1 - 2 * j)
        for kind, target in enumerate((lefts, rights, ketses)):
            arrived(target.at[j], map_recv.at[j, kind])
        coeffs[...] = layer_rows(ketses[j], picks[...])
        apart = dot(jnp.concatenate(thirds(lefts[j]), axis=0), select_one[...])
        for leg in range(4):
            lanes = slice(leg * WIDE, (leg + 1) * WIDE)
            spread[leg] = apart[0:CHI, lanes] + (
                apart[CHI : 2 * CHI, lanes] + apart[2 * CHI : 3 * CHI, lanes]
            )
        high, mid, lowest = thirds(rights[j])
        main = dot_nt(select_two[...], padded((high, mid)))
        fine = dot_nt(select_two[...], padded((lowest,)))
        main, fine = main.astype(BF16), fine.astype(BF16)
        for leg in range(4):
            rows = slice(leg * 128, (leg + 1) * 128)
            for copy in range(2):
                begin = leg * 256 + copy * 128
                second[number, begin : begin + 128, :] = main[rows]
            third[number, leg * 256 : leg * 256 + 128, :] = fine[rows]
            third[number, leg * 256 + 128 : leg * 256 + 256, :] = main[rows, 0:128]
        fold_first(spread, coeffs, folded, number)

    def side_copy(number, source):
        return remote(
            source,
            sides.at[way, place],
            row_send.at[number, 0],
            side_recv.at[way, place],
            env_member(slot_at(number)),
        )

    def side_own(number):
        slot = slot_at(number)
        same_core = (slot % 2 == xl) & (leader == core)
        return (low + slot // GROUP == z) & same_core & ((slot % GROUP) // 2 == xh)

    def out_copy(number):
        return remote(
            normed.at[number + 1],
            outs.at[way, col],
            row_send.at[number, 1],
            out_recv.at[way, col],
            member(slot_at(number), y, xh),
        )

    def send_sides(number, source):
        @pl.when(side_own(number))
        def _():
            pltpu.make_async_copy(
                source, sides.at[way, place], side_recv.at[way, place]
            ).start()

        @pl.when(jnp.logical_not(side_own(number)))
        def _():
            side_copy(number, source).start()

    def send_out(number, carried):
        own = slot_at(number) == mine

        @pl.when(own)
        def _():
            pltpu.make_async_copy(
                normed.at[number + 1], outs.at[way, col], out_recv.at[way, col]
            ).start()

        @pl.when(jnp.logical_not(own))
        def _():
            out_copy(number).start()

        return carried

    def hop():
        return remote(leaving, entered, hop_send, hop_recv, after)

    def tiles_of(value):
        return [value[leg * CHI : (leg + 1) * CHI] for leg in range(4)]

    def advance(number):
        @pl.when(number == 0)
        def _():
            @pl.when(has_prev)
            def _():
                arrived(entered, hop_recv)

            for leg, tile in enumerate(unpack(entered[...])):
                state[leg * CHI : (leg + 1) * CHI, :] = tile

        raw = is_first & (number == 0)
        closes = is_last & (number == count - 1)

        @pl.when(closes)
        def _():
            held = state[...]
            last_in[...] = pack(tiles_of(held)) * nrm_scale(held)
            send_sides(number, last_in)

        current = state[...]
        scale = jnp.where(raw, 1.0, nrm_scale(current))
        renewed = apply_layer(current, scale, folded, second, third, number, middle)
        normed[number] = pack(tiles_of(current)) * scale
        state[...] = renewed

        @pl.when(number == count - 1)
        def _():
            final = state[...]
            leaving[...] = pack(tiles_of(final))

            @pl.when(has_next)
            def _():
                hop().start()

            normed[count] = leaving[...] * nrm_scale(final)

        @pl.when(jnp.logical_not(closes))
        def _():
            send_sides(number, normed.at[number])

        @pl.when(number == count - 1)
        def _():
            lax.fori_loop(0, count, send_out, 0)


    def column_at(number):
        return number + core * (3 - 2 * number)

    def env_legs(m, g, o, f):
        return pick(mirror, f, g), pick(core, m, o), pick(mirror, g, f), pick(core, o, m)

    def env_selects():
        for part in range(2):
            arrived(row_kets.at[pl.ds(2 * part, 2)], ket_recv.at[part])
        picks[...] = layer_picks(env_legs)

        @pl.when(core == 0)
        def _():
            row, lane = iota((2 * CHI, WIDE), 0), iota((2 * CHI, WIDE), 1)
            row = jnp.where(row >= CHI, row - CHI, row)
            for _ in range(3):
                lane = jnp.where(lane >= CHI, lane - CHI, lane)
            select_one[0 : 2 * CHI, 0:WIDE] = jnp.where(row == lane, 1.0, 0.0).astype(BF16)

        @pl.when(core == 1)
        def _():
            for leg in range(4):
                row, lane = iota((WIDE, WIDE), 0), iota((WIDE, WIDE), 1)
                for _ in range(3):
                    lane = jnp.where(lane >= CHI, lane - CHI, lane)
                select_one[:, leg * WIDE : (leg + 1) * WIDE] = jnp.where(
                    row == leg * CHI + lane, 1.0, 0.0
                ).astype(BF16)
                row, lane = iota((128, WIDE), 0), iota((128, WIDE), 1)
                select_two[leg * 128 : (leg + 1) * 128, :] = jnp.where(
                    (lane == leg * CHI + row) & (row < CHI), 1.0, 0.0
                ).astype(BF16)

    def forward(side, column):
        target = sides.at[side, column]
        device = (z, xl, 1 - core, y, xh)
        return remote(
            target, target, pass_send.at[side, column], side_recv.at[side, column], device
        )

    def back(side):
        device = (z, xl, core, jnp.maximum(y - 1, 0), xh)
        return remote(
            sides.at[side, 0], sides.at[side, 4], back_send.at[side], side_recv.at[side, 4], device
        )

    def take_side(side, column):
        arrived(sides.at[side, column], side_recv.at[side, column])

        @pl.when(core == leader)
        def _():
            forward(side, column).start()

        @pl.when(sends_back & (column == 0))
        def _():
            back(side).start()

    def env_fold(number):
        @pl.when(number == 0)
        def _():
            env_selects()

        column = column_at(number)
        take_side(mirror, column)
        coeffs[...] = layer_rows(row_kets[column], picks[...])
        early = jnp.concatenate(halves(sides[mirror, column]), axis=0)

        @pl.when(core == 0)
        def _():
            turned = lax.dot_general(
                early,
                select_one[0 : 2 * CHI, 0:WIDE],
                (((0,), (0,)), ((), ())),
                preferred_element_type=F32,
            )
            for leg in range(4):
                spread[leg] = turned[leg * CHI : (leg + 1) * CHI]

        @pl.when(core == 1)
        def _():
            apart = dot(early, select_one[...])
            for leg in range(4):
                lanes = slice(leg * WIDE, (leg + 1) * WIDE)
                spread[leg] = apart[0:CHI, lanes] + apart[CHI : 2 * CHI, lanes]

        fold_pair(spread, coeffs, env_folded, number)

    def env_prepare(number):
        column = column_at(number)
        take_side(1 - mirror, column)

        @pl.when(core == 0)
        def _():
            for leg, tile in enumerate(unpack(sides[1 - mirror, column])):
                high, lowest = halves(tile)
                both = jnp.concatenate(
                    [jnp.concatenate([high, lowest], axis=1), jnp.zeros((32, 256), BF16)], axis=0
                )
                env_second[number, leg * 256 : leg * 256 + 128, :] = both
                env_second[number, leg * 256 + 128 : leg * 256 + 256, :] = both

        @pl.when(core == 1)
        def _():
            late = padded(halves(sides[1 - mirror, column]))
            turned = dot_nt(select_two[...], late).astype(BF16)
            for leg in range(4):
                for copy in range(2):
                    begin = leg * 256 + copy * 128
                    env_second[number, begin : begin + 128, :] = turned[leg * 128 : leg * 128 + 128]

    def env_hop():
        device = (z, xl, core, jnp.clip(y + 1 - 2 * core, 0, stations - 1), xh)
        return remote(env_leaving, env_entered, env_send, env_recv, device)

    def over(number):
        column = column_at(number)
        wraps = column == 0
        slot = jnp.where(wraps, 3, jnp.maximum(column - 1, 0))
        y_to = jnp.where(wraps, jnp.maximum(y - 1, 0), y)
        return remote(
            env_normed.at[number],
            from_right.at[slot],
            over_send.at[number],
            over_recv.at[slot],
            (z, xl, 0, y_to, xh),
        )

    def sends_over(number):
        return (core == 1) & ((y > 0) | (column_at(number) > 0))

    def flipped(tile):
        square = jnp.concatenate([tile, jnp.zeros((32, 128), F32)], axis=0)
        return square.T[0:CHI, :]

    def env_advance(number):
        @pl.when(number == 0)
        def _():
            arrived(env_entered, env_recv)
            flips = station_first & (mirror == 1)

            @pl.when(jnp.logical_not(flips))
            def _():
                for leg, tile in enumerate(unpack(env_entered[...])):
                    state[leg * CHI : (leg + 1) * CHI, :] = tile

            @pl.when(flips)
            def _():
                for leg, tile in enumerate(unpack(env_entered[...])):
                    state[leg * CHI : (leg + 1) * CHI, :] = flipped(tile)

        raw = station_first & (number == 0)

        @pl.when(jnp.logical_not(station_last & (number >= 2)))
        def _():
            current = state[...]
            scale = jnp.where(raw, 1.0, nrm_scale(current))
            renewed = apply_pair(current, scale, env_folded, env_second, number, middle)
            env_normed[number] = pack(tiles_of(current)) * scale
            state[...] = renewed

        @pl.when(station_last & (number >= 2))
        def _():
            current = state[...]
            env_normed[number] = pack(tiles_of(current)) * nrm_scale(current)

        @pl.when(jnp.logical_not(station_last) & (number == 3))
        def _():
            env_leaving[...] = pack(tiles_of(state[...]))
            env_hop().start()

        @pl.when(core == 0)
        def _():
            from_left[number] = env_normed[number]

        @pl.when(sends_over(number))
        def _():
            over(number).start()


    total = jnp.where(is_worker, 2 * count, 0)
    before_fold = jnp.where(is_late, count, total)

    def task(index, carried):
        folds = (index >= before_fold) & (index < before_fold + 4)
        on_env = index >= total + 4
        on_boundary = jnp.logical_not(folds) & jnp.logical_not(on_env)
        step = jnp.where(index < before_fold, index, index - 4)
        prepares = (is_first & (step % 2 == 0)) | (jnp.logical_not(is_first) & (step < count))

        @pl.when(on_boundary & prepares)
        def _():
            prepare(jnp.where(is_first, step // 2, jnp.clip(step, 0, count - 1)))

        @pl.when(on_boundary & jnp.logical_not(prepares))
        def _():
            advance(jnp.where(is_first, step // 2, jnp.clip(step - count, 0, count - 1)))

        @pl.when(folds)
        def _():
            env_fold(jnp.clip(index - before_fold, 0, 3))

        late = index - (total + 4)
        readies = (station_first & (late % 2 == 0)) | (
            jnp.logical_not(station_first) & (late < 4)
        )

        @pl.when(on_env & readies)
        def _():
            env_prepare(jnp.where(station_first, late // 2, jnp.clip(late, 0, 3)))

        @pl.when(on_env & jnp.logical_not(readies))
        def _():
            env_advance(jnp.where(station_first, late // 2, jnp.clip(late - 4, 0, 3)))

        return carried

    lax.fori_loop(0, total + 12, task, 0)


    lax.fori_loop(0, 4, map_sent, 0)

    @pl.when(has_next)
    def _():
        hop().wait_send()

    def row_sent(number, carried):
        @pl.when(jnp.logical_not(side_own(number)))
        def _():
            side_copy(number, normed.at[number]).wait_send()

        @pl.when(slot_at(number) != mine)
        def _():
            out_copy(number).wait_send()

        return carried

    lax.fori_loop(0, total // 2, row_sent, 0)

    for to_core in range(2):

        @pl.when(jnp.logical_not(at_home & (core == to_core)))
        def _():
            ket_copy(to_core).wait_send()

    @pl.when(kets_back)
    def _():
        ket_back().wait_send()

    for edge, to_core, y_of in edges:

        @pl.when((y == y_of) & (xh == xl) & jnp.logical_not(at_home & (core == to_core)))
        def _():
            edge_copy(edge, to_core).wait_send()

    for side in range(2):

        @pl.when(core == leader)
        def _():
            for column in range(4):
                forward(side, column).wait_send()

        @pl.when(sends_back)
        def _():
            back(side).wait_send()

    @pl.when(jnp.logical_not(station_last))
    def _():
        env_hop().wait_send()

    for number in range(4):

        @pl.when(sends_over(number))
        def _():
            over(number).wait_send()

    for direction in range(2):
        for column in range(2):
            arrived(outs.at[direction, column], out_recv.at[direction, column])

    @pl.when(gets_back)
    def _():
        for direction in range(2):
            arrived(sides.at[direction, 4], side_recv.at[direction, 4])
        arrived(row_kets.at[4], ket_recv.at[2])

    @pl.when(core == 0)
    def _():
        for slot in range(3):
            arrived(from_right.at[slot], over_recv.at[slot])

    @pl.when(gets_back)
    def _():
        arrived(from_right.at[3], over_recv.at[3])


def run_sweep(kets, left_maps, right_maps, top_edge, bottom_edge, left_edge, right_edge):
    vmem = pl.BlockSpec(memory_space=pltpu.VMEM)
    anywhere = pl.BlockSpec(memory_space=pl.ANY)
    column = (CHI, WIDE)
    most = 2 * GROUP
    dma = pltpu.SemaphoreType.DMA
    return pl.pallas_call(
        sweep_kernel,
        out_shape=(
            jax.ShapeDtypeStruct((2, 2) + column, F32),
            jax.ShapeDtypeStruct((2, 5) + column, F32),
            jax.ShapeDtypeStruct((5, 32, 128), F32),
            jax.ShapeDtypeStruct((4,) + column, F32),
            jax.ShapeDtypeStruct((4,) + column, F32),
        ),
        in_specs=[vmem, anywhere, anywhere] + [vmem] * 4,
        out_specs=(vmem,) * 5,
        scratch_shapes=[
            pltpu.VMEM((most,) + column, F32),
            pltpu.VMEM((most,) + column, F32),
            pltpu.VMEM((most, 32, 128), F32),
            pltpu.VMEM((WIDE, 4 * WIDE), BF16),
            pltpu.VMEM((512, WIDE), BF16),
            pltpu.VMEM((4,) + column, F32),
            pltpu.VMEM((64, WIDE), F32),
            pltpu.VMEM((1024, 32), BF16),
            pltpu.VMEM((most, 16 * CHI, 3 * WIDE), BF16),
            pltpu.VMEM((most, 1024, 256), BF16),
            pltpu.VMEM((most, 1024, 128), BF16),
            pltpu.VMEM((4, 16 * CHI, 2 * WIDE), BF16),
            pltpu.VMEM((4, 1024, 256), BF16),
            pltpu.VMEM((WIDE, 2048), BF16),
            pltpu.VMEM(column, F32),
            pltpu.VMEM(column, F32),
            pltpu.VMEM((WIDE, 128), F32),
            pltpu.VMEM((most + 1,) + column, F32),
            pltpu.VMEM(column, F32),
            pltpu.VMEM(column, F32),
            pltpu.VMEM(column, F32),
            pltpu.VMEM((4,) + column, F32),
            dma((4, 3)),
            dma((most, 3)),
            dma,
            dma,
            dma((most, 2)),
            dma((2, 2)),
            dma((2, 5)),
            dma((3,)),
            dma((3,)),
            dma,
            dma((2, 4)),
            dma((2,)),
            dma,
            dma,
            dma((4,)),
            dma((4,)),
        ],
        compiler_params=pltpu.CompilerParams(
            collective_id=0, has_side_effects=True, vmem_limit_bytes=67043328
        ),
        name="sweep",
    )(kets, left_maps, right_maps, top_edge, bottom_edge, left_edge, right_edge)


def dot_general(left, right, dims):
    return lax.dot_general(left, right, (dims, ((), ())), preferred_element_type=F32)


def pad_rows(value):
    return jnp.concatenate([value, jnp.zeros((32, value.shape[1]), value.dtype)], axis=0)


def swap_legs(entry):
    return (entry & 0b10101) | ((entry >> 3) & 1) << 1 | ((entry >> 1) & 1) << 3


def open_site(ket, legs_at, wide, opened):
    def body(block, carried):
        begin = pl.multiple_of(block * 8, 8)
        half_done = {}
        for bra in range(8):
            u2, m2, d2 = bra >> 2, (bra >> 1) & 1, bra & 1
            tiles = []
            for top in range(8):
                u, m, d = top >> 2, (top >> 1) & 1, top & 1
                row = (2 * m + m2) * 4 + 2 * u + u2
                lane = (2 * d + d2) * 128
                tiles.append(wide[pl.ds(row * CHI + begin, 8), lane : lane + 128])
            for state in range(2):
                for out in range(2):
                    total = None
                    for top in range(8):
                        at = state * 16 + legs_at(top >> 2, (top >> 1) & 1, top & 1, out)
                        term = ket[at : at + 1, :] * tiles[top]
                        total = term if total is None else total + term
                    half_done[state, out, bra] = total
        for state in range(2):
            for out in range(2):
                for other in range(2):
                    for out2 in range(2):
                        total = None
                        for bra in range(8):
                            at = other * 16 + legs_at(bra >> 2, (bra >> 1) & 1, bra & 1, out2)
                            term = ket[at : at + 1, :] * half_done[state, out, bra]
                            total = term if total is None else total + term
                        row = (2 * out + out2) * CHI
                        opened[state * 2 + other, pl.ds(row + begin, 8), :] = total
        return carried

    lax.fori_loop(0, CHI // 8, body, 0)


def energy_kernel(
    term_rows,
    term_bonds,
    term_ops,
    operators,
    all_sides,
    all_kets,
    all_left,
    all_right,
    shares,
    wide,
    opened,
    closing,
    density,
    ket,
    sides,
    row_kets,
    from_left,
    from_right,
    fetch,
):
    way = lax.axis_index("rows_2")
    row_here = (
        lax.axis_index("rows_0") * GROUP + lax.axis_index("cols_1") * 2 + lax.axis_index("rows_1")
    )
    first = lax.axis_index("cols_0") * 4
    planes = lax.axis_size("rows_0")
    mirror = jnp.where(lax.axis_index("rows_0") >= planes // 2, 1, 0)

    def take_ket(column):
        for entry in range(32):
            ket[entry : entry + 1, :] = jnp.where(
                mirror == 1,
                row_kets[column, swap_legs(entry) : swap_legs(entry) + 1, :],
                row_kets[column, entry : entry + 1, :],
            )

    shares[...] = jnp.zeros((8, 128), F32)

    def hits(term, column):
        here = (term_rows[term] == row_here) & (term_bonds[term] == first + column)
        return here & (way == 0)

    def column_body(column, carried):
        count = 0
        for term in range(TERMS):
            count = count + jnp.where(hits(term, column), 1, 0)

        @pl.when(count > 0)
        def _():
            copies = [
                pltpu.make_async_copy(
                    all_sides.at[:, pl.ds(column, 2)], sides, fetch.at[0]
                ),
                pltpu.make_async_copy(all_kets.at[pl.ds(column, 2)], row_kets, fetch.at[1]),
                pltpu.make_async_copy(all_left.at[column], from_left, fetch.at[2]),
                pltpu.make_async_copy(all_right.at[column], from_right, fetch.at[3]),
            ]
            for copy in copies:
                copy.start()
            for copy in copies:
                copy.wait()

            high, low = halves(sides[mirror, 0])
            both = jnp.concatenate([high, low], axis=0)
            state_high, state_low = halves(jnp.concatenate(unpack(from_left[...]), axis=1))
            tn = ((0,), (0,))
            joined = dot_general(
                both, jnp.concatenate([state_high, state_high], axis=0), tn
            ) + dot_general(both, jnp.concatenate([state_low, state_low], axis=0), tn)
            below_high, below_low = halves(jnp.concatenate(unpack(sides[1 - mirror, 0]), axis=1))
            main = jnp.concatenate([pad_rows(below_high), pad_rows(below_high)], axis=0)
            fine = jnp.concatenate([pad_rows(below_low), pad_rows(below_low)], axis=0)
            for leg in range(4):
                part = jnp.concatenate(halves(joined[:, leg * 128 : (leg + 1) * 128]), axis=1)
                wide[leg * WIDE : (leg + 1) * WIDE, :] = dot(part, main) + dot(part, fine)
            take_ket(0)
            open_site(
                ket,
                lambda u, m, d, out: u * 8 + m * 4 + d * 2 + out,
                wide,
                opened,
            )

            above = jnp.concatenate(unpack(sides[mirror, 1]), axis=0)
            both = jnp.concatenate(halves(above), axis=1)
            state_high, state_low = halves(jnp.concatenate(unpack(from_right[...]), axis=1))
            state_high, state_low = pad_rows(state_high), pad_rows(state_low)
            joined = dot(both, jnp.concatenate([state_high, state_high], axis=0)) + dot(
                both, jnp.concatenate([state_low, state_low], axis=0)
            )
            below_high, below_low = halves(
                jnp.concatenate([pad_rows(tile) for tile in unpack(sides[1 - mirror, 1])], axis=0)
            )
            main = jnp.concatenate([below_high, below_high], axis=1)
            fine = jnp.concatenate([below_low, below_low], axis=1)
            for leg in range(4):
                part = jnp.concatenate(halves(joined[:, leg * 128 : (leg + 1) * 128]), axis=1)
                wide[leg * WIDE : (leg + 1) * WIDE, :] = dot_nt(part, main) + dot_nt(part, fine)
            take_ket(1)
            open_site(
                ket,
                lambda u, m, d, out: u * 8 + out * 4 + d * 2 + m,
                wide,
                closing,
            )

            for pair in range(4):
                for other in range(4):
                    product = opened[pair] * closing[other]
                    at = pair * 4 + other
                    density[at : at + 1, :] = jnp.sum(product, axis=0, keepdims=True)
            rho = jnp.sum(density[...], axis=1, keepdims=True)
            index = iota((16, 1), 0)
            diagonal = (index == 0) | (index == 3) | (index == 12) | (index == 15)
            trace = jnp.sum(jnp.where(diagonal, rho, 0.0), axis=0, keepdims=True)
            spread = jnp.sqrt(jnp.sum(rho * rho, axis=0, keepdims=True))
            bottom = jnp.maximum(jnp.abs(trace), 0.25 * spread)

            def term_body(term, kept):
                @pl.when(hits(term, column))
                def _():
                    chosen = jnp.zeros((16, 1), F32)
                    for entry in range(16):
                        chosen = jnp.where(
                            index == entry, operators[term_ops[term], entry], chosen
                        )
                    value = jnp.sum(chosen * rho, axis=0, keepdims=True) / bottom
                    lane = iota((8, 128), 1)
                    shares[...] = jnp.where(lane == term, value, shares[...])

                return kept

            lax.fori_loop(0, TERMS, term_body, 0)

        return carried

    lax.fori_loop(0, 4, column_body, 0)


def run_energies(term_rows, term_bonds, term_ops, operators, sides, row_kets, lefts, rights):
    vmem = pl.BlockSpec(memory_space=pltpu.VMEM)
    smem = pl.BlockSpec(memory_space=pltpu.SMEM)
    return pl.pallas_call(
        energy_kernel,
        out_shape=jax.ShapeDtypeStruct((8, 128), F32),
        in_specs=[smem] * 4 + [pl.BlockSpec(memory_space=pl.ANY)] * 4,
        out_specs=vmem,
        scratch_shapes=[
            pltpu.VMEM((16 * CHI, 512), F32),
            pltpu.VMEM((4, WIDE, 128), F32),
            pltpu.VMEM((4, WIDE, 128), F32),
            pltpu.VMEM((16, 128), F32),
            pltpu.VMEM((32, 128), F32),
            pltpu.VMEM((2, 2, CHI, WIDE), F32),
            pltpu.VMEM((2, 32, 128), F32),
            pltpu.VMEM((CHI, WIDE), F32),
            pltpu.VMEM((CHI, WIDE), F32),
            pltpu.SemaphoreType.DMA((4,)),
        ],
        compiler_params=pltpu.CompilerParams(vmem_limit_bytes=32 * 1024 * 1024),
        name="energies",
    )(term_rows, term_bonds, term_ops, operators, sides, row_kets, lefts, rights)


def sum_kernel(shares, total, planes_in, plane_in, partial, send_one, recv_one, send_two, recv_two):
    z = lax.axis_index("rows_0")
    xl = lax.axis_index("rows_1")
    core = lax.axis_index("rows_2")
    y = lax.axis_index("cols_0")
    xh = lax.axis_index("cols_1")
    way = core
    place = y * 4 + xl * 2 + xh
    barrier = pltpu.get_barrier_semaphore()

    def greet(device):
        pl.semaphore_signal(barrier, inc=1, device_id=device, device_id_type=MESH)

    def along(step):
        return ((z + step) % 8, xl, core, y, xh)

    def within(step):
        other = (place * 2 + way + step) % 32
        return (z, (other // 4) % 2, other % 2, other // 8, (other // 2) % 2)

    for step in range(1, 8):
        greet(along(step))
    for step in range(1, 32):
        greet(within(step))
    pl.semaphore_wait(barrier, 38)

    def first(step):
        return pltpu.make_async_remote_copy(
            src_ref=shares,
            dst_ref=planes_in.at[z],
            send_sem=send_one.at[step],
            recv_sem=recv_one.at[z],
            device_id=along(step),
            device_id_type=MESH,
        )

    def second(step):
        return pltpu.make_async_remote_copy(
            src_ref=partial,
            dst_ref=plane_in.at[place],
            send_sem=send_two.at[step],
            recv_sem=recv_two.at[place],
            device_id=within(step),
            device_id_type=MESH,
        )

    @pl.when(way == 0)
    def _():
        for step in range(1, 8):
            first(step).start()
        pltpu.make_async_copy(shares, planes_in.at[z], recv_one.at[z]).start()
        added = None
        for plane in range(8):
            target = planes_in.at[plane]
            pltpu.make_async_copy(target, target, recv_one.at[plane]).wait()
        for plane in range(8):
            added = planes_in[plane] if added is None else added + planes_in[plane]
        partial[...] = added
        for step in range(1, 32):
            second(step).start()
        pltpu.make_async_copy(partial, plane_in.at[place], recv_two.at[place]).start()

    for other in range(16):
        target = plane_in.at[other]
        pltpu.make_async_copy(target, target, recv_two.at[other]).wait()
    added = None
    for other in range(16):
        added = plane_in[other] if added is None else added + plane_in[other]
    total[...] = added

    @pl.when(way == 0)
    def _():
        for step in range(1, 8):
            first(step).wait_send()
        for step in range(1, 32):
            second(step).wait_send()


def run_sum(shares):
    vmem = pl.BlockSpec(memory_space=pltpu.VMEM)
    return pl.pallas_call(
        sum_kernel,
        out_shape=jax.ShapeDtypeStruct((8, 128), F32),
        in_specs=[vmem],
        out_specs=vmem,
        scratch_shapes=[
            pltpu.VMEM((8, 8, 128), F32),
            pltpu.VMEM((16, 8, 128), F32),
            pltpu.VMEM((8, 128), F32),
            pltpu.SemaphoreType.DMA((8,)),
            pltpu.SemaphoreType.DMA((8,)),
            pltpu.SemaphoreType.DMA((32,)),
            pltpu.SemaphoreType.DMA((16,)),
        ],
        compiler_params=pltpu.CompilerParams(collective_id=2, has_side_effects=True),
        name="shares_sum",
    )(shares)


def shards(
    kets,
    left_maps,
    right_maps,
    top_edge,
    bottom_edge,
    left_edge,
    right_edge,
    term_rows,
    term_bonds,
    term_ops,
    operators,
):
    spread_kets = jnp.broadcast_to(kets[0][:, :, None], (kets.shape[1], 32, 128))
    outs, sides, row_kets, lefts, rights = run_sweep(
        spread_kets, left_maps, right_maps, top_edge, bottom_edge, left_edge, right_edge
    )
    shares = run_energies(
        term_rows, term_bonds, term_ops, operators, sides, row_kets, lefts, rights
    )
    energies = run_sum(shares)[0, :TERMS]
    return (outs[0][None], outs[1][None], energies)


def solution(mesh):
    torus = Mesh(
        mesh.devices.reshape(8, 2, 2, 4, 2), ("rows_0", "rows_1", "rows_2", "cols_0", "cols_1")
    )
    placed = (
        P(ROWS, COLS, None),
        P(None, ROWS, COLS, None, None),
        P(None, ROWS, COLS, None, None),
        P(COLS, None, None),
        P(COLS, None, None),
        P(ROWS, None, None),
        P(ROWS, None, None),
        P(),
        P(),
        P(),
        P(),
    )
    return jax.shard_map(
        shards,
        mesh=torus,
        in_specs=placed,
        out_specs=(P(ROWS, COLS, None, None), P(ROWS, COLS, None, None), P()),
        check_vma=False,
    )
```

```python
import functools

import jax
import jax.numpy as jnp
from jax import lax
from jax.experimental import pallas as pl
from jax.experimental.pallas import tpu as pltpu
from jax.sharding import Mesh
from jax.sharding import PartitionSpec as P

D = 2
D2 = 4
PHYS = 2
CHI = 96
WIDE = D2 * CHI
OPS = 4
TERMS = 16
GROUP = 4
ROWS = ("rows_0", "rows_1", "rows_2")
COLS = ("cols_0", "cols_1")
ROWS_COLS = ("rows_0", "rows_1", "rows_2", "cols_0", "cols_1")
MESH = pl.DeviceIdType.MESH

EPSILON = 1e-06
PRECISION_HIGH = lax.Precision.HIGHEST
F32 = jnp.float32
BF16 = jnp.bfloat16


def iota(shape, dim):
    return lax.broadcasted_iota(jnp.int32, shape, dim)


def halves(value):
    high = value.astype(BF16)
    low = (value - high.astype(F32)).astype(BF16)
    return high, low


def dot(left, right):
    return jnp.dot(left, right, preferred_element_type=F32)


def dot_nt(left, right):
    return lax.dot_general(left, right, (((1,), (1,)), ((), ())), preferred_element_type=F32)


def unpack(wide):
    one, two, three = wide[:, 0:128], wide[:, 128:256], wide[:, 256:384]
    lane = iota((CHI, 128), 1)
    parts = (
        one,
        pltpu.roll(jnp.where(lane >= 96, one, two), 32, 1),
        pltpu.roll(jnp.where(lane >= 64, two, three), 64, 1),
        pltpu.roll(three, 96, 1),
    )
    return [jnp.where(lane < CHI, part, 0.0) for part in parts]


def pack(tiles):
    lane = iota((CHI, 128), 1)
    first = tiles[0]
    second = pltpu.roll(tiles[1], 96, 1)
    third = pltpu.roll(tiles[2], 64, 1)
    fourth = pltpu.roll(tiles[3], 32, 1)
    return jnp.concatenate(
        [
            jnp.where(lane < 96, first, second),
            jnp.where(lane < 64, second, third),
            jnp.where(lane < 32, third, fourth),
        ],
        axis=1,
    )


def pick(mode, *choices):
    value = choices[-1]
    for index in range(len(choices) - 1):
        value = jnp.where(mode == index, choices[index], value)
    return value


def layer_picks(legs):
    shape = (PHYS * 256, 32)
    row, col = iota(shape, 0), iota(shape, 1)
    digits = ((row >> 6) & 3, (row >> 4) & 3, (row >> 2) & 3, row & 3)
    up, left, down, right = legs(*digits)
    base = (row >> 8) * 16
    ket_at = base + (up >> 1) * 8 + (left >> 1) * 4 + (down >> 1) * 2 + (right >> 1)
    bra_at = base + (up & 1) * 8 + (left & 1) * 4 + (down & 1) * 2 + (right & 1)
    return jnp.concatenate(
        [jnp.where(col == ket_at, 1.0, 0.0), jnp.where(col == bra_at, 1.0, 0.0)], axis=0
    ).astype(BF16)


def pair_values(ket, picks):
    parts = dot(picks, jnp.concatenate(thirds(ket), axis=1))
    taken = parts[:, 0:128] + (parts[:, 128:256] + parts[:, 256:384])
    both = taken[0:512] * taken[512:1024]
    return both[0:256] + both[256:512]


def layer_rows(ket, picks):
    full = pair_values(ket, picks)
    lane = iota((64, 128), 1)
    at = [full[64 * m : 64 * (m + 1)] for m in range(4)]
    return jnp.concatenate(
        [
            jnp.where(lane < 96, at[0], at[1]),
            jnp.where(lane < 64, at[1], at[2]),
            jnp.where(lane < 32, at[2], at[3]),
        ],
        axis=1,
    )


def thirds(value):
    high = value.astype(BF16)
    rest = value - high.astype(F32)
    middle = rest.astype(BF16)
    low = (rest - middle.astype(F32)).astype(BF16)
    return high, middle, low


ROOT = 0.7071067811865476


def symmetric(tiles):
    return [tiles[0], (tiles[1] + tiles[2]) * ROOT, tiles[3], (tiles[1] - tiles[2]) * ROOT]


def plain(tiles):
    return [tiles[0], (tiles[1] + tiles[3]) * ROOT, (tiles[1] - tiles[3]) * ROOT, tiles[2]]


def is_even(*legs):
    return sum(leg == 3 for leg in legs) % 2 == 0


def basis_turn():
    row, col = iota((256, 256), 0), iota((256, 256), 1)
    value = jnp.ones((256, 256), F32)
    for to_shift, from_shift in ((6, 4), (4, 2), (2, 0), (0, 6)):
        new, old = (row >> to_shift) & 3, (col >> from_shift) & 3
        one = jnp.where(old == 1, 1.0, 0.0)
        two = jnp.where(old == 2, 1.0, 0.0)
        ends = jnp.where(new == 0, jnp.where(old == 0, 1.0, 0.0), jnp.where(old == 3, 1.0, 0.0))
        middle = jnp.where(new == 1, one + two, one - two)
        value = value * jnp.where((new & 1) == 0, ends, middle)
    return value.astype(BF16)


def even_rows(full, turn):
    parts = dot(turn, jnp.concatenate(thirds(full), axis=1))
    row = iota((256, 128), 0)
    halved = (row & 1) + ((row >> 2) & 1) + ((row >> 4) & 1) + ((row >> 6) & 1)
    factor = jnp.where((halved & 1) == 1, ROOT, 1.0) * jnp.where(
        halved >= 4, 0.25, jnp.where(halved >= 2, 0.5, 1.0)
    )
    return (parts[:, 0:128] + (parts[:, 128:256] + parts[:, 256:384])) * factor


def padded(parts):
    blank = jnp.zeros((32, parts[0].shape[1]), BF16)
    return jnp.concatenate([piece for part in parts for piece in (part, blank)], axis=0)


def apply_layer(state, scale, first, layers, second, third, slot, joined, middle):
    def side_by_side(part):
        blank = jnp.zeros((32, 128), BF16)
        return jnp.concatenate(
            [
                jnp.concatenate([part[leg * CHI : (leg + 1) * CHI], blank], axis=0)
                for leg in range(4)
            ],
            axis=1,
        )

    high, mid, low = (side_by_side(part) for part in thirds(state))
    joined[...] = dot(first[slot], jnp.concatenate([high, high, mid, mid, high, low], axis=0))
    block = 16
    for begin in range(0, CHI, block):
        tiles = {}
        for f in range(4):
            for m in range(4):
                rows = slice(f * CHI + begin, f * CHI + begin + block)
                tiles[f, m] = joined[rows, m * 128 : (m + 1) * 128]
        for g in range(4):
            for o in range(4):
                total = None
                for f in range(4):
                    for m in range(4):
                        if is_even(g, o, f, m):
                            at = ((g * 4 + o) * 4 + f) * 4 + m
                            term = layers[slot, at : at + 1, :] * tiles[f, m]
                            total = term if total is None else total + term
                high, mid, low = thirds(total)
                rows = slice(o * CHI + begin, o * CHI + begin + block)
                for index, part in enumerate((high, mid)):
                    lane = g * 256 + index * 128
                    middle[rows, lane : lane + 128] = part
                for index, part in enumerate((high, low)):
                    lane = 1024 + g * 256 + index * 128
                    middle[rows, lane : lane + 128] = part
    wide = dot(middle[:, 0:1024], second[slot])
    rest = dot(middle[:, 1024:2048], third[slot])
    return (wide[:, 0:128] + (wide[:, 128:256] + rest)) * scale


def nrm_scale(state):
    total = jnp.sum(jnp.sum(state * state, axis=0, keepdims=True), axis=1, keepdims=True)
    return lax.rsqrt(total * (1.0 / (CHI * WIDE)) + EPSILON)


def fold_pair(spread, coeffs, folded, slot):
    def body(index, carried):
        total = None
        for leg in range(4):
            term = coeffs[pl.ds(index * 4 + leg, 1), :] * spread[leg]
            total = term if total is None else total + term
        high, low = halves(total)
        rows = pl.ds(pl.multiple_of(index * CHI, CHI), CHI)
        folded[slot, rows, 0:WIDE] = high
        folded[slot, rows, WIDE : 2 * WIDE] = low
        return carried

    lax.fori_loop(0, 16, body, 0)


def apply_pair(state, scale, folded, second, slot, middle):
    high, low = halves(state)
    once = jnp.concatenate([high, low], axis=1)
    twice = jnp.concatenate([once, once], axis=0)
    for leg in range(4):
        wide = dot(folded[slot, leg * WIDE : (leg + 1) * WIDE, :], twice)
        high, low = halves(wide[:, 0:128] + wide[:, 128:256])
        middle[:, leg * 256 : leg * 256 + 128] = high
        middle[:, leg * 256 + 128 : leg * 256 + 256] = low
    wide = dot(middle[:, 0:1024], second[slot])
    return (wide[:, 0:128] + wide[:, 128:256]) * scale


def sweep_kernel(
    kets,
    left_maps,
    right_maps,
    top_edge,
    bottom_edge,
    left_edge,
    right_edge,
    outs,
    sides,
    row_kets,
    from_left,
    from_right,
    lefts,
    rights,
    ketses,
    select_one,
    select_two,
    spread,
    coeffs,
    picks,
    turn,
    layers,
    first,
    joined,
    second,
    third,
    env_folded,
    env_second,
    middle,
    entered,
    leaving,
    state,
    normed,
    last_in,
    env_entered,
    env_leaving,
    env_normed,
    map_send,
    map_recv,
    hop_send,
    hop_recv,
    row_send,
    out_recv,
    side_recv,
    ket_send,
    ket_recv,
    edge_send,
    pass_send,
    back_send,
    env_send,
    env_recv,
    over_send,
    over_recv,
):
    z = lax.axis_index("rows_0")
    xl = lax.axis_index("rows_1")
    core = lax.axis_index("rows_2")
    y = lax.axis_index("cols_0")
    xh = lax.axis_index("cols_1")
    planes = lax.axis_size("rows_0")
    stations = lax.axis_size("cols_0")
    end = planes - 1
    at_edge = (z == 0) | (z == end)
    low = jnp.where(at_edge, z, 1 + 2 * (jnp.maximum(z - 1, 0) // 2))
    count = jnp.where(at_edge, GROUP, 2 * GROUP)
    col = xl
    is_worker = at_edge | (core == 1)
    way = jnp.where(z == 0, 1 - core, jnp.where(z == end, core, z % 2))
    starts = ((way == 0) & (z == 0)) | ((way == 1) & (z == end))
    is_first = at_edge & starts
    is_last = at_edge & jnp.logical_not(starts)
    has_next = is_worker & jnp.logical_not(is_last)
    has_prev = is_worker & jnp.logical_not(is_first)
    mine = (z - low) * GROUP + xl * 2 + core
    place = xh * 2 + col
    ahead = z + 2 - 4 * way
    ahead = jnp.clip(ahead, 0, end)
    after = (ahead, xl, jnp.where((ahead == 0) | (ahead == end), 0, 1), y, xh)
    behind = jnp.where(
        way == 0, jnp.where(z == end, end - 1, z - 2), jnp.where(z == 0, 1, z + 2)
    )
    before = (jnp.clip(behind, 0, end), xl, 1, y, xh)
    mirror = jnp.where(z >= planes // 2, 1, 0)
    in_middle = (z == planes // 2) | (z == planes // 2 - 1)
    is_late = is_worker & (way != mirror) & jnp.logical_not(in_middle)
    station_first = ((core == 0) & (y == 0)) | ((core == 1) & (y == stations - 1))
    station_last = ((core == 0) & (y == stations - 1)) | ((core == 1) & (y == 0))
    leader = jnp.where(y >= stations // 2, 1, 0)

    def member(slot, y_to, xh_to):
        return (low + slot // GROUP, (slot % GROUP) // 2, slot % 2, y_to, xh_to)

    def env_member(slot):
        return (low + slot // GROUP, slot % 2, leader, y, (slot % GROUP) // 2)

    def remote(source, target, send_sem, recv_sem, device):
        return pltpu.make_async_remote_copy(
            src_ref=source,
            dst_ref=target,
            send_sem=send_sem,
            recv_sem=recv_sem,
            device_id=device,
            device_id_type=MESH,
        )

    def arrived(target, sem):
        pltpu.make_async_copy(target, target, sem).wait()

    barrier = pltpu.get_barrier_semaphore()

    def greet(device):
        pl.semaphore_signal(barrier, inc=1, device_id=device, device_id_type=MESH)

    def greet_slot(slot, carried):
        @pl.when(slot != mine)
        def _():
            greet(member(slot, y, xh))

        greet(member(slot, y, 1 - xh))
        for step in (1, stations - 1):
            for xh_to in range(2):
                greet(member(slot, (y + step) % stations, xh_to))
        return carried

    lax.fori_loop(0, count, greet_slot, 0)

    @pl.when(has_next)
    def _():
        greet(after)

    @pl.when(has_prev)
    def _():
        greet(before)

    def legs(m, g, o, f):
        return pick(way, m, o), f, pick(way, o, m), g

    @pl.when(is_worker)
    def _():
        for leg in range(4):
            row, lane = iota((WIDE, 128), 0), iota((WIDE, 128), 1)
            select_one[:, leg * 128 : (leg + 1) * 128] = jnp.where(
                (row == 4 * lane + leg) & (lane < CHI), 1.0, 0.0
            ).astype(BF16)
            row, lane = iota((128, WIDE), 0), iota((128, WIDE), 1)
            select_two[leg * 128 : (leg + 1) * 128, :] = jnp.where(
                (lane == 4 * row + leg) & (row < CHI), 1.0, 0.0
            ).astype(BF16)
        picks[...] = layer_picks(legs)
        turn[...] = basis_turn()

    pl.semaphore_wait(
        barrier, 6 * count - 1 + jnp.where(has_next, 1, 0) + jnp.where(has_prev, 1, 0)
    )

    def chain(index):
        to_way = (index // 2 + jnp.where(z == end, 1, 0)) % 2
        to_col = index % 2
        to_start = ((to_way == 0) & (z == 0)) | ((to_way == 1) & (z == end))
        to_core = jnp.where(at_edge, jnp.where(to_start, 1, 0), 1)
        to_z = jnp.where(at_edge, z, low + 1 - to_way)
        own = (to_z == z) & (to_col == xl) & (to_core == core)
        return to_way, to_col, (to_z, to_col, to_core, y, xh), own

    def map_pairs(to_way, to_col):
        return (
            (left_maps.at[to_way, 0, to_col], lefts.at[mine]),
            (right_maps.at[to_way, 0, to_col], rights.at[mine]),
            (kets.at[to_col], ketses.at[mine]),
        )

    def send_map(index, carried):
        to_way, to_col, device, own = chain(index)

        @pl.when(own)
        def _():
            for kind, (source, target) in enumerate(map_pairs(to_way, to_col)):
                pltpu.make_async_copy(source, target, map_recv.at[mine, kind]).start()

        @pl.when(jnp.logical_not(own))
        def _():
            for kind, (source, target) in enumerate(map_pairs(to_way, to_col)):
                remote(
                    source, target, map_send.at[index, kind], map_recv.at[mine, kind], device
                ).start()

        return carried

    def map_sent(index, carried):
        to_way, to_col, device, own = chain(index)

        @pl.when(jnp.logical_not(own))
        def _():
            for kind, (source, target) in enumerate(map_pairs(to_way, to_col)):
                remote(
                    source, target, map_send.at[index, kind], map_recv.at[mine, kind], device
                ).wait_send()

        return carried

    lax.fori_loop(0, 4, send_map, 0)

    half = pl.ds(2 * xh, 2)
    at_home = (core == xl) & (xl == xh)

    def ket_copy(to_core):
        device = (z, core, to_core, y, xl)
        return remote(kets, row_kets.at[half], ket_send.at[to_core], ket_recv.at[xh], device)

    def ket_back():
        device = (z, core, 0, jnp.maximum(y - 1, 0), xl)
        return remote(kets.at[0], row_kets.at[4], ket_send.at[2], ket_recv.at[2], device)

    def edge_copy(edge, to_core):
        return remote(edge.at[0], env_entered, edge_send, env_recv, (z, core, to_core, y, xl))

    for to_core in range(2):

        @pl.when(at_home & (core == to_core))
        def _():
            pltpu.make_async_copy(kets, row_kets.at[half], ket_recv.at[xh]).start()

        @pl.when(jnp.logical_not(at_home & (core == to_core)))
        def _():
            ket_copy(to_core).start()

    sends_back = (core == 0) & (y > 0)
    gets_back = (core == 0) & (y < stations - 1)
    kets_back = (xh == 0) & (y > 0)

    @pl.when(kets_back)
    def _():
        ket_back().start()

    edges = ((left_edge, 0, 0), (right_edge, 1, stations - 1))
    for edge, to_core, y_of in edges:

        @pl.when((y == y_of) & (xh == xl) & at_home & (core == to_core))
        def _():
            pltpu.make_async_copy(edge.at[0], env_entered, env_recv).start()

        @pl.when((y == y_of) & (xh == xl) & jnp.logical_not(at_home & (core == to_core)))
        def _():
            edge_copy(edge, to_core).start()

    @pl.when(is_first & (way == 0))
    def _():
        entered[...] = top_edge[col]

    @pl.when(is_first & (way == 1))
    def _():
        entered[...] = bottom_edge[col]


    def slot_at(number):
        return number + way * (count - 1 - 2 * number)

    def prepare(step):
        ordered = slot_at(step)
        j = jnp.where(is_first, ordered, (mine + step) % count)
        number = j + way * (count - 1 - 2 * j)
        for kind, target in enumerate((lefts, rights, ketses)):
            arrived(target.at[j], map_recv.at[j, kind])
        layers[number] = even_rows(pair_values(ketses[j], picks[...]), turn[...])
        apart = dot(jnp.concatenate(thirds(lefts[j]), axis=0), select_one[:, 0:512])
        apart = apart[0:CHI] + (apart[CHI : 2 * CHI] + apart[2 * CHI : 3 * CHI])
        legs_of = symmetric([apart[:, leg * 128 : (leg + 1) * 128] for leg in range(4)])
        for leg, tile in enumerate(legs_of):
            high, mid, lowest = thirds(tile)
            for index, part in enumerate((high, mid, high, mid, lowest, high)):
                lanes = slice(index * 128, (index + 1) * 128)
                first[number, leg * CHI : (leg + 1) * CHI, lanes] = part
        high, mid, lowest = thirds(rights[j])
        main = dot_nt(select_two[...], padded((high, mid)))
        fine = dot_nt(select_two[...], padded((lowest,)))
        apart = main[:, 0:128] + (main[:, 128:256] + fine)
        legs_of = symmetric([apart[leg * 128 : (leg + 1) * 128] for leg in range(4)])
        for leg, tile in enumerate(legs_of):
            high, mid, lowest = thirds(tile)
            for copy in range(2):
                begin = leg * 256 + copy * 128
                second[number, begin : begin + 128, 0:128] = high
                second[number, begin : begin + 128, 128:256] = mid
            third[number, leg * 256 : leg * 256 + 128, :] = lowest
            third[number, leg * 256 + 128 : leg * 256 + 256, :] = high

    def side_copy(number, source):
        return remote(
            source,
            sides.at[way, place],
            row_send.at[number, 0],
            side_recv.at[way, place],
            env_member(slot_at(number)),
        )

    def side_own(number):
        slot = slot_at(number)
        same_core = (slot % 2 == xl) & (leader == core)
        return (low + slot // GROUP == z) & same_core & ((slot % GROUP) // 2 == xh)

    def out_copy(number):
        return remote(
            normed.at[number + 1],
            outs.at[way, col],
            row_send.at[number, 1],
            out_recv.at[way, col],
            member(slot_at(number), y, xh),
        )

    def send_sides(number, source):
        @pl.when(side_own(number))
        def _():
            pltpu.make_async_copy(
                source, sides.at[way, place], side_recv.at[way, place]
            ).start()

        @pl.when(jnp.logical_not(side_own(number)))
        def _():
            side_copy(number, source).start()

    def send_out(number, carried):
        own = slot_at(number) == mine

        @pl.when(own)
        def _():
            pltpu.make_async_copy(
                normed.at[number + 1], outs.at[way, col], out_recv.at[way, col]
            ).start()

        @pl.when(jnp.logical_not(own))
        def _():
            out_copy(number).start()

        return carried

    def hop():
        return remote(leaving, entered, hop_send, hop_recv, after)

    def tiles_of(value):
        return [value[leg * CHI : (leg + 1) * CHI] for leg in range(4)]

    def advance(number):
        @pl.when(number == 0)
        def _():
            @pl.when(has_prev)
            def _():
                arrived(entered, hop_recv)

            came = unpack(entered[...])
            for leg, (tile, turned) in enumerate(zip(came, symmetric(came))):
                state[leg * CHI : (leg + 1) * CHI, :] = jnp.where(is_first, turned, tile)

        raw = is_first & (number == 0)
        closes = is_last & (number == count - 1)

        @pl.when(closes)
        def _():
            held = state[...]
            last_in[...] = pack(plain(tiles_of(held))) * nrm_scale(held)
            send_sides(number, last_in)

        current = state[...]
        scale = jnp.where(raw, 1.0, nrm_scale(current))
        renewed = apply_layer(
            current, scale, first, layers, second, third, number, joined, middle
        )
        normed[number] = pack(plain(tiles_of(current))) * scale
        state[...] = renewed

        @pl.when(number == count - 1)
        def _():
            final = state[...]
            leaving[...] = pack(tiles_of(final))

            @pl.when(has_next)
            def _():
                hop().start()

            normed[count] = pack(plain(tiles_of(final))) * nrm_scale(final)

        @pl.when(jnp.logical_not(closes))
        def _():
            send_sides(number, normed.at[number])

        @pl.when(number == count - 1)
        def _():
            lax.fori_loop(0, count, send_out, 0)


    def column_at(number):
        return number + core * (3 - 2 * number)

    def env_legs(m, g, o, f):
        return pick(mirror, f, g), pick(core, m, o), pick(mirror, g, f), pick(core, o, m)

    def env_selects():
        for part in range(2):
            arrived(row_kets.at[pl.ds(2 * part, 2)], ket_recv.at[part])
        picks[...] = layer_picks(env_legs)

        @pl.when(core == 0)
        def _():
            row, lane = iota((2 * CHI, WIDE), 0), iota((2 * CHI, WIDE), 1)
            row = jnp.where(row >= CHI, row - CHI, row)
            for _ in range(3):
                lane = jnp.where(lane >= CHI, lane - CHI, lane)
            select_one[0 : 2 * CHI, 0:WIDE] = jnp.where(row == lane, 1.0, 0.0).astype(BF16)

        @pl.when(core == 1)
        def _():
            for leg in range(4):
                row, lane = iota((WIDE, WIDE), 0), iota((WIDE, WIDE), 1)
                for _ in range(3):
                    lane = jnp.where(lane >= CHI, lane - CHI, lane)
                select_one[:, leg * WIDE : (leg + 1) * WIDE] = jnp.where(
                    row == leg * CHI + lane, 1.0, 0.0
                ).astype(BF16)
                row, lane = iota((128, WIDE), 0), iota((128, WIDE), 1)
                select_two[leg * 128 : (leg + 1) * 128, :] = jnp.where(
                    (lane == leg * CHI + row) & (row < CHI), 1.0, 0.0
                ).astype(BF16)

    def forward(side, column):
        target = sides.at[side, column]
        device = (z, xl, 1 - core, y, xh)
        return remote(
            target, target, pass_send.at[side, column], side_recv.at[side, column], device
        )

    def back(side):
        device = (z, xl, core, jnp.maximum(y - 1, 0), xh)
        return remote(
            sides.at[side, 0], sides.at[side, 4], back_send.at[side], side_recv.at[side, 4], device
        )

    def take_side(side, column):
        arrived(sides.at[side, column], side_recv.at[side, column])

        @pl.when(core == leader)
        def _():
            forward(side, column).start()

        @pl.when(sends_back & (column == 0))
        def _():
            back(side).start()

    def env_fold(number):
        @pl.when(number == 0)
        def _():
            env_selects()

        column = column_at(number)
        take_side(mirror, column)
        coeffs[...] = layer_rows(row_kets[column], picks[...])
        early = jnp.concatenate(halves(sides[mirror, column]), axis=0)

        @pl.when(core == 0)
        def _():
            turned = lax.dot_general(
                early,
                select_one[0 : 2 * CHI, 0:WIDE],
                (((0,), (0,)), ((), ())),
                preferred_element_type=F32,
            )
            for leg in range(4):
                spread[leg] = turned[leg * CHI : (leg + 1) * CHI]

        @pl.when(core == 1)
        def _():
            apart = dot(early, select_one[...])
            for leg in range(4):
                lanes = slice(leg * WIDE, (leg + 1) * WIDE)
                spread[leg] = apart[0:CHI, lanes] + apart[CHI : 2 * CHI, lanes]

        fold_pair(spread, coeffs, env_folded, number)

    def env_prepare(number):
        column = column_at(number)
        take_side(1 - mirror, column)

        @pl.when(core == 0)
        def _():
            for leg, tile in enumerate(unpack(sides[1 - mirror, column])):
                high, lowest = halves(tile)
                both = jnp.concatenate(
                    [jnp.concatenate([high, lowest], axis=1), jnp.zeros((32, 256), BF16)], axis=0
                )
                env_second[number, leg * 256 : leg * 256 + 128, :] = both
                env_second[number, leg * 256 + 128 : leg * 256 + 256, :] = both

        @pl.when(core == 1)
        def _():
            late = padded(halves(sides[1 - mirror, column]))
            turned = dot_nt(select_two[...], late).astype(BF16)
            for leg in range(4):
                for copy in range(2):
                    begin = leg * 256 + copy * 128
                    env_second[number, begin : begin + 128, :] = turned[leg * 128 : leg * 128 + 128]

    def env_hop():
        device = (z, xl, core, jnp.clip(y + 1 - 2 * core, 0, stations - 1), xh)
        return remote(env_leaving, env_entered, env_send, env_recv, device)

    def over(number):
        column = column_at(number)
        wraps = column == 0
        slot = jnp.where(wraps, 3, jnp.maximum(column - 1, 0))
        y_to = jnp.where(wraps, jnp.maximum(y - 1, 0), y)
        return remote(
            env_normed.at[number],
            from_right.at[slot],
            over_send.at[number],
            over_recv.at[slot],
            (z, xl, 0, y_to, xh),
        )

    def sends_over(number):
        return (core == 1) & ((y > 0) | (column_at(number) > 0))

    def flipped(tile):
        square = jnp.concatenate([tile, jnp.zeros((32, 128), F32)], axis=0)
        return square.T[0:CHI, :]

    def env_advance(number):
        @pl.when(number == 0)
        def _():
            arrived(env_entered, env_recv)
            flips = station_first & (mirror == 1)

            @pl.when(jnp.logical_not(flips))
            def _():
                for leg, tile in enumerate(unpack(env_entered[...])):
                    state[leg * CHI : (leg + 1) * CHI, :] = tile

            @pl.when(flips)
            def _():
                for leg, tile in enumerate(unpack(env_entered[...])):
                    state[leg * CHI : (leg + 1) * CHI, :] = flipped(tile)

        raw = station_first & (number == 0)

        @pl.when(jnp.logical_not(station_last & (number >= 2)))
        def _():
            current = state[...]
            scale = jnp.where(raw, 1.0, nrm_scale(current))
            renewed = apply_pair(current, scale, env_folded, env_second, number, middle)
            env_normed[number] = pack(tiles_of(current)) * scale
            state[...] = renewed

        @pl.when(station_last & (number >= 2))
        def _():
            current = state[...]
            env_normed[number] = pack(tiles_of(current)) * nrm_scale(current)

        @pl.when(jnp.logical_not(station_last) & (number == 3))
        def _():
            env_leaving[...] = pack(tiles_of(state[...]))
            env_hop().start()

        @pl.when(core == 0)
        def _():
            from_left[number] = env_normed[number]

        @pl.when(sends_over(number))
        def _():
            over(number).start()


    total = jnp.where(is_worker, 2 * count, 0)
    before_fold = jnp.where(is_late, count, total)

    def task(index, carried):
        folds = (index >= before_fold) & (index < before_fold + 4)
        on_env = index >= total + 4
        on_boundary = jnp.logical_not(folds) & jnp.logical_not(on_env)
        step = jnp.where(index < before_fold, index, index - 4)
        prepares = (is_first & (step % 2 == 0)) | (jnp.logical_not(is_first) & (step < count))

        @pl.when(on_boundary & prepares)
        def _():
            prepare(jnp.where(is_first, step // 2, jnp.clip(step, 0, count - 1)))

        @pl.when(on_boundary & jnp.logical_not(prepares))
        def _():
            advance(jnp.where(is_first, step // 2, jnp.clip(step - count, 0, count - 1)))

        @pl.when(folds)
        def _():
            env_fold(jnp.clip(index - before_fold, 0, 3))

        late = index - (total + 4)
        readies = (station_first & (late % 2 == 0)) | (
            jnp.logical_not(station_first) & (late < 4)
        )

        @pl.when(on_env & readies)
        def _():
            env_prepare(jnp.where(station_first, late // 2, jnp.clip(late, 0, 3)))

        @pl.when(on_env & jnp.logical_not(readies))
        def _():
            env_advance(jnp.where(station_first, late // 2, jnp.clip(late - 4, 0, 3)))

        return carried

    lax.fori_loop(0, total + 12, task, 0)


    lax.fori_loop(0, 4, map_sent, 0)

    @pl.when(has_next)
    def _():
        hop().wait_send()

    def row_sent(number, carried):
        @pl.when(jnp.logical_not(side_own(number)))
        def _():
            side_copy(number, normed.at[number]).wait_send()

        @pl.when(slot_at(number) != mine)
        def _():
            out_copy(number).wait_send()

        return carried

    lax.fori_loop(0, total // 2, row_sent, 0)

    for to_core in range(2):

        @pl.when(jnp.logical_not(at_home & (core == to_core)))
        def _():
            ket_copy(to_core).wait_send()

    @pl.when(kets_back)
    def _():
        ket_back().wait_send()

    for edge, to_core, y_of in edges:

        @pl.when((y == y_of) & (xh == xl) & jnp.logical_not(at_home & (core == to_core)))
        def _():
            edge_copy(edge, to_core).wait_send()

    for side in range(2):

        @pl.when(core == leader)
        def _():
            for column in range(4):
                forward(side, column).wait_send()

        @pl.when(sends_back)
        def _():
            back(side).wait_send()

    @pl.when(jnp.logical_not(station_last))
    def _():
        env_hop().wait_send()

    for number in range(4):

        @pl.when(sends_over(number))
        def _():
            over(number).wait_send()

    for direction in range(2):
        for column in range(2):
            arrived(outs.at[direction, column], out_recv.at[direction, column])

    @pl.when(gets_back)
    def _():
        for direction in range(2):
            arrived(sides.at[direction, 4], side_recv.at[direction, 4])
        arrived(row_kets.at[4], ket_recv.at[2])

    @pl.when(core == 0)
    def _():
        for slot in range(3):
            arrived(from_right.at[slot], over_recv.at[slot])

    @pl.when(gets_back)
    def _():
        arrived(from_right.at[3], over_recv.at[3])


def run_sweep(kets, left_maps, right_maps, top_edge, bottom_edge, left_edge, right_edge):
    vmem = pl.BlockSpec(memory_space=pltpu.VMEM)
    anywhere = pl.BlockSpec(memory_space=pl.ANY)
    column = (CHI, WIDE)
    most = 2 * GROUP
    dma = pltpu.SemaphoreType.DMA
    return pl.pallas_call(
        sweep_kernel,
        out_shape=(
            jax.ShapeDtypeStruct((2, 2) + column, F32),
            jax.ShapeDtypeStruct((2, 5) + column, F32),
            jax.ShapeDtypeStruct((5, 32, 128), F32),
            jax.ShapeDtypeStruct((4,) + column, F32),
            jax.ShapeDtypeStruct((4,) + column, F32),
        ),
        in_specs=[vmem, anywhere, anywhere] + [vmem] * 4,
        out_specs=(vmem,) * 5,
        scratch_shapes=[
            pltpu.VMEM((most,) + column, F32),
            pltpu.VMEM((most,) + column, F32),
            pltpu.VMEM((most, 32, 128), F32),
            pltpu.VMEM((WIDE, 4 * WIDE), BF16),
            pltpu.VMEM((512, WIDE), BF16),
            pltpu.VMEM((4,) + column, F32),
            pltpu.VMEM((64, WIDE), F32),
            pltpu.VMEM((1024, 32), BF16),
            pltpu.VMEM((256, 256), BF16),
            pltpu.VMEM((most, 256, 128), F32),
            pltpu.VMEM((most, WIDE, 768), BF16),
            pltpu.VMEM((WIDE, 512), F32),
            pltpu.VMEM((most, 1024, 256), BF16),
            pltpu.VMEM((most, 1024, 128), BF16),
            pltpu.VMEM((4, 16 * CHI, 2 * WIDE), BF16),
            pltpu.VMEM((4, 1024, 256), BF16),
            pltpu.VMEM((WIDE, 2048), BF16),
            pltpu.VMEM(column, F32),
            pltpu.VMEM(column, F32),
            pltpu.VMEM((WIDE, 128), F32),
            pltpu.VMEM((most + 1,) + column, F32),
            pltpu.VMEM(column, F32),
            pltpu.VMEM(column, F32),
            pltpu.VMEM(column, F32),
            pltpu.VMEM((4,) + column, F32),
            dma((4, 3)),
            dma((most, 3)),
            dma,
            dma,
            dma((most, 2)),
            dma((2, 2)),
            dma((2, 5)),
            dma((3,)),
            dma((3,)),
            dma,
            dma((2, 4)),
            dma((2,)),
            dma,
            dma,
            dma((4,)),
            dma((4,)),
        ],
        compiler_params=pltpu.CompilerParams(
            collective_id=0, has_side_effects=True, vmem_limit_bytes=67043328
        ),
        name="sweep",
    )(kets, left_maps, right_maps, top_edge, bottom_edge, left_edge, right_edge)


def dot_general(left, right, dims):
    return lax.dot_general(left, right, (dims, ((), ())), preferred_element_type=F32)


def pad_rows(value):
    return jnp.concatenate([value, jnp.zeros((32, value.shape[1]), value.dtype)], axis=0)


def swap_legs(entry):
    return (entry & 0b10101) | ((entry >> 3) & 1) << 1 | ((entry >> 1) & 1) << 3


def open_site(ket, legs_at, wide, opened):
    def body(block, carried):
        begin = pl.multiple_of(block * 8, 8)
        half_done = {}
        for bra in range(8):
            u2, m2, d2 = bra >> 2, (bra >> 1) & 1, bra & 1
            tiles = []
            for top in range(8):
                u, m, d = top >> 2, (top >> 1) & 1, top & 1
                row = (2 * m + m2) * 4 + 2 * u + u2
                lane = (2 * d + d2) * 128
                tiles.append(wide[pl.ds(row * CHI + begin, 8), lane : lane + 128])
            for state in range(2):
                for out in range(2):
                    total = None
                    for top in range(8):
                        at = state * 16 + legs_at(top >> 2, (top >> 1) & 1, top & 1, out)
                        term = ket[at : at + 1, :] * tiles[top]
                        total = term if total is None else total + term
                    half_done[state, out, bra] = total
        for state in range(2):
            for out in range(2):
                for other in range(2):
                    for out2 in range(2):
                        total = None
                        for bra in range(8):
                            at = other * 16 + legs_at(bra >> 2, (bra >> 1) & 1, bra & 1, out2)
                            term = ket[at : at + 1, :] * half_done[state, out, bra]
                            total = term if total is None else total + term
                        row = (2 * out + out2) * CHI
                        opened[state * 2 + other, pl.ds(row + begin, 8), :] = total
        return carried

    lax.fori_loop(0, CHI // 8, body, 0)


def energy_kernel(
    term_rows,
    term_bonds,
    term_ops,
    operators,
    all_sides,
    all_kets,
    all_left,
    all_right,
    shares,
    wide,
    opened,
    closing,
    density,
    ket,
    sides,
    row_kets,
    from_left,
    from_right,
    fetch,
):
    way = lax.axis_index("rows_2")
    row_here = (
        lax.axis_index("rows_0") * GROUP + lax.axis_index("cols_1") * 2 + lax.axis_index("rows_1")
    )
    first = lax.axis_index("cols_0") * 4
    planes = lax.axis_size("rows_0")
    mirror = jnp.where(lax.axis_index("rows_0") >= planes // 2, 1, 0)

    def take_ket(column):
        for entry in range(32):
            ket[entry : entry + 1, :] = jnp.where(
                mirror == 1,
                row_kets[column, swap_legs(entry) : swap_legs(entry) + 1, :],
                row_kets[column, entry : entry + 1, :],
            )

    shares[...] = jnp.zeros((8, 128), F32)

    def hits(term, column):
        here = (term_rows[term] == row_here) & (term_bonds[term] == first + column)
        return here & (way == 0)

    def column_body(column, carried):
        count = 0
        for term in range(TERMS):
            count = count + jnp.where(hits(term, column), 1, 0)

        @pl.when(count > 0)
        def _():
            copies = [
                pltpu.make_async_copy(
                    all_sides.at[:, pl.ds(column, 2)], sides, fetch.at[0]
                ),
                pltpu.make_async_copy(all_kets.at[pl.ds(column, 2)], row_kets, fetch.at[1]),
                pltpu.make_async_copy(all_left.at[column], from_left, fetch.at[2]),
                pltpu.make_async_copy(all_right.at[column], from_right, fetch.at[3]),
            ]
            for copy in copies:
                copy.start()
            for copy in copies:
                copy.wait()

            high, low = halves(sides[mirror, 0])
            both = jnp.concatenate([high, low], axis=0)
            state_high, state_low = halves(jnp.concatenate(unpack(from_left[...]), axis=1))
            tn = ((0,), (0,))
            joined = dot_general(
                both, jnp.concatenate([state_high, state_high], axis=0), tn
            ) + dot_general(both, jnp.concatenate([state_low, state_low], axis=0), tn)
            below_high, below_low = halves(jnp.concatenate(unpack(sides[1 - mirror, 0]), axis=1))
            main = jnp.concatenate([pad_rows(below_high), pad_rows(below_high)], axis=0)
            fine = jnp.concatenate([pad_rows(below_low), pad_rows(below_low)], axis=0)
            for leg in range(4):
                part = jnp.concatenate(halves(joined[:, leg * 128 : (leg + 1) * 128]), axis=1)
                wide[leg * WIDE : (leg + 1) * WIDE, :] = dot(part, main) + dot(part, fine)
            take_ket(0)
            open_site(
                ket,
                lambda u, m, d, out: u * 8 + m * 4 + d * 2 + out,
                wide,
                opened,
            )

            above = jnp.concatenate(unpack(sides[mirror, 1]), axis=0)
            both = jnp.concatenate(halves(above), axis=1)
            state_high, state_low = halves(jnp.concatenate(unpack(from_right[...]), axis=1))
            state_high, state_low = pad_rows(state_high), pad_rows(state_low)
            joined = dot(both, jnp.concatenate([state_high, state_high], axis=0)) + dot(
                both, jnp.concatenate([state_low, state_low], axis=0)
            )
            below_high, below_low = halves(
                jnp.concatenate([pad_rows(tile) for tile in unpack(sides[1 - mirror, 1])], axis=0)
            )
            main = jnp.concatenate([below_high, below_high], axis=1)
            fine = jnp.concatenate([below_low, below_low], axis=1)
            for leg in range(4):
                part = jnp.concatenate(halves(joined[:, leg * 128 : (leg + 1) * 128]), axis=1)
                wide[leg * WIDE : (leg + 1) * WIDE, :] = dot_nt(part, main) + dot_nt(part, fine)
            take_ket(1)
            open_site(
                ket,
                lambda u, m, d, out: u * 8 + out * 4 + d * 2 + m,
                wide,
                closing,
            )

            for pair in range(4):
                for other in range(4):
                    product = opened[pair] * closing[other]
                    at = pair * 4 + other
                    density[at : at + 1, :] = jnp.sum(product, axis=0, keepdims=True)
            rho = jnp.sum(density[...], axis=1, keepdims=True)
            index = iota((16, 1), 0)
            diagonal = (index == 0) | (index == 3) | (index == 12) | (index == 15)
            trace = jnp.sum(jnp.where(diagonal, rho, 0.0), axis=0, keepdims=True)
            spread = jnp.sqrt(jnp.sum(rho * rho, axis=0, keepdims=True))
            bottom = jnp.maximum(jnp.abs(trace), 0.25 * spread)

            def term_body(term, kept):
                @pl.when(hits(term, column))
                def _():
                    chosen = jnp.zeros((16, 1), F32)
                    for entry in range(16):
                        chosen = jnp.where(
                            index == entry, operators[term_ops[term], entry], chosen
                        )
                    value = jnp.sum(chosen * rho, axis=0, keepdims=True) / bottom
                    lane = iota((8, 128), 1)
                    shares[...] = jnp.where(lane == term, value, shares[...])

                return kept

            lax.fori_loop(0, TERMS, term_body, 0)

        return carried

    lax.fori_loop(0, 4, column_body, 0)


def run_energies(term_rows, term_bonds, term_ops, operators, sides, row_kets, lefts, rights):
    vmem = pl.BlockSpec(memory_space=pltpu.VMEM)
    smem = pl.BlockSpec(memory_space=pltpu.SMEM)
    return pl.pallas_call(
        energy_kernel,
        out_shape=jax.ShapeDtypeStruct((8, 128), F32),
        in_specs=[smem] * 4 + [pl.BlockSpec(memory_space=pl.ANY)] * 4,
        out_specs=vmem,
        scratch_shapes=[
            pltpu.VMEM((16 * CHI, 512), F32),
            pltpu.VMEM((4, WIDE, 128), F32),
            pltpu.VMEM((4, WIDE, 128), F32),
            pltpu.VMEM((16, 128), F32),
            pltpu.VMEM((32, 128), F32),
            pltpu.VMEM((2, 2, CHI, WIDE), F32),
            pltpu.VMEM((2, 32, 128), F32),
            pltpu.VMEM((CHI, WIDE), F32),
            pltpu.VMEM((CHI, WIDE), F32),
            pltpu.SemaphoreType.DMA((4,)),
        ],
        compiler_params=pltpu.CompilerParams(vmem_limit_bytes=32 * 1024 * 1024),
        name="energies",
    )(term_rows, term_bonds, term_ops, operators, sides, row_kets, lefts, rights)


def sum_kernel(shares, total, planes_in, plane_in, partial, send_one, recv_one, send_two, recv_two):
    z = lax.axis_index("rows_0")
    xl = lax.axis_index("rows_1")
    core = lax.axis_index("rows_2")
    y = lax.axis_index("cols_0")
    xh = lax.axis_index("cols_1")
    way = core
    place = y * 4 + xl * 2 + xh
    barrier = pltpu.get_barrier_semaphore()

    def greet(device):
        pl.semaphore_signal(barrier, inc=1, device_id=device, device_id_type=MESH)

    def along(step):
        return ((z + step) % 8, xl, core, y, xh)

    def within(step):
        other = (place * 2 + way + step) % 32
        return (z, (other // 4) % 2, other % 2, other // 8, (other // 2) % 2)

    for step in range(1, 8):
        greet(along(step))
    for step in range(1, 32):
        greet(within(step))
    pl.semaphore_wait(barrier, 38)

    def first(step):
        return pltpu.make_async_remote_copy(
            src_ref=shares,
            dst_ref=planes_in.at[z],
            send_sem=send_one.at[step],
            recv_sem=recv_one.at[z],
            device_id=along(step),
            device_id_type=MESH,
        )

    def second(step):
        return pltpu.make_async_remote_copy(
            src_ref=partial,
            dst_ref=plane_in.at[place],
            send_sem=send_two.at[step],
            recv_sem=recv_two.at[place],
            device_id=within(step),
            device_id_type=MESH,
        )

    @pl.when(way == 0)
    def _():
        for step in range(1, 8):
            first(step).start()
        pltpu.make_async_copy(shares, planes_in.at[z], recv_one.at[z]).start()
        added = None
        for plane in range(8):
            target = planes_in.at[plane]
            pltpu.make_async_copy(target, target, recv_one.at[plane]).wait()
        for plane in range(8):
            added = planes_in[plane] if added is None else added + planes_in[plane]
        partial[...] = added
        for step in range(1, 32):
            second(step).start()
        pltpu.make_async_copy(partial, plane_in.at[place], recv_two.at[place]).start()

    for other in range(16):
        target = plane_in.at[other]
        pltpu.make_async_copy(target, target, recv_two.at[other]).wait()
    added = None
    for other in range(16):
        added = plane_in[other] if added is None else added + plane_in[other]
    total[...] = added

    @pl.when(way == 0)
    def _():
        for step in range(1, 8):
            first(step).wait_send()
        for step in range(1, 32):
            second(step).wait_send()


def run_sum(shares):
    vmem = pl.BlockSpec(memory_space=pltpu.VMEM)
    return pl.pallas_call(
        sum_kernel,
        out_shape=jax.ShapeDtypeStruct((8, 128), F32),
        in_specs=[vmem],
        out_specs=vmem,
        scratch_shapes=[
            pltpu.VMEM((8, 8, 128), F32),
            pltpu.VMEM((16, 8, 128), F32),
            pltpu.VMEM((8, 128), F32),
            pltpu.SemaphoreType.DMA((8,)),
            pltpu.SemaphoreType.DMA((8,)),
            pltpu.SemaphoreType.DMA((32,)),
            pltpu.SemaphoreType.DMA((16,)),
        ],
        compiler_params=pltpu.CompilerParams(collective_id=2, has_side_effects=True),
        name="shares_sum",
    )(shares)


def shards(
    kets,
    left_maps,
    right_maps,
    top_edge,
    bottom_edge,
    left_edge,
    right_edge,
    term_rows,
    term_bonds,
    term_ops,
    operators,
):
    spread_kets = jnp.broadcast_to(kets[0][:, :, None], (kets.shape[1], 32, 128))
    outs, sides, row_kets, lefts, rights = run_sweep(
        spread_kets, left_maps, right_maps, top_edge, bottom_edge, left_edge, right_edge
    )
    shares = run_energies(
        term_rows, term_bonds, term_ops, operators, sides, row_kets, lefts, rights
    )
    energies = run_sum(shares)[0, :TERMS]
    return (outs[0][None], outs[1][None], energies)


def solution(mesh):
    torus = Mesh(
        mesh.devices.reshape(8, 2, 2, 4, 2), ("rows_0", "rows_1", "rows_2", "cols_0", "cols_1")
    )
    placed = (
        P(ROWS, COLS, None),
        P(None, ROWS, COLS, None, None),
        P(None, ROWS, COLS, None, None),
        P(COLS, None, None),
        P(COLS, None, None),
        P(ROWS, None, None),
        P(ROWS, None, None),
        P(),
        P(),
        P(),
        P(),
    )
    return jax.shard_map(
        shards,
        mesh=torus,
        in_specs=placed,
        out_specs=(P(ROWS, COLS, None, None), P(ROWS, COLS, None, None), P()),
        check_vma=False,
    )
```

```python
import functools

import jax
import jax.numpy as jnp
from jax import lax
from jax.experimental import pallas as pl
from jax.experimental.pallas import tpu as pltpu
from jax.sharding import Mesh
from jax.sharding import PartitionSpec as P

D = 2
D2 = 4
PHYS = 2
CHI = 96
WIDE = D2 * CHI
OPS = 4
TERMS = 16
GROUP = 4
ROWS = ("rows_0", "rows_1", "rows_2")
COLS = ("cols_0", "cols_1")
ROWS_COLS = ("rows_0", "rows_1", "rows_2", "cols_0", "cols_1")
MESH = pl.DeviceIdType.MESH

EPSILON = 1e-06
PRECISION_HIGH = lax.Precision.HIGHEST
F32 = jnp.float32
BF16 = jnp.bfloat16


def iota(shape, dim):
    return lax.broadcasted_iota(jnp.int32, shape, dim)


def halves(value):
    high = value.astype(BF16)
    low = (value - high.astype(F32)).astype(BF16)
    return high, low


def dot(left, right):
    return jnp.dot(left, right, preferred_element_type=F32)


def dot_nt(left, right):
    return lax.dot_general(left, right, (((1,), (1,)), ((), ())), preferred_element_type=F32)


def unpack(wide):
    one, two, three = wide[:, 0:128], wide[:, 128:256], wide[:, 256:384]
    lane = iota((CHI, 128), 1)
    parts = (
        one,
        pltpu.roll(jnp.where(lane >= 96, one, two), 32, 1),
        pltpu.roll(jnp.where(lane >= 64, two, three), 64, 1),
        pltpu.roll(three, 96, 1),
    )
    return [jnp.where(lane < CHI, part, 0.0) for part in parts]


def pack(tiles):
    lane = iota((CHI, 128), 1)
    first = tiles[0]
    second = pltpu.roll(tiles[1], 96, 1)
    third = pltpu.roll(tiles[2], 64, 1)
    fourth = pltpu.roll(tiles[3], 32, 1)
    return jnp.concatenate(
        [
            jnp.where(lane < 96, first, second),
            jnp.where(lane < 64, second, third),
            jnp.where(lane < 32, third, fourth),
        ],
        axis=1,
    )


def pick(mode, *choices):
    value = choices[-1]
    for index in range(len(choices) - 1):
        value = jnp.where(mode == index, choices[index], value)
    return value


def layer_picks(legs):
    shape = (PHYS * 256, 32)
    row, col = iota(shape, 0), iota(shape, 1)
    digits = ((row >> 6) & 3, (row >> 4) & 3, (row >> 2) & 3, row & 3)
    up, left, down, right = legs(*digits)
    base = (row >> 8) * 16
    ket_at = base + (up >> 1) * 8 + (left >> 1) * 4 + (down >> 1) * 2 + (right >> 1)
    bra_at = base + (up & 1) * 8 + (left & 1) * 4 + (down & 1) * 2 + (right & 1)
    return jnp.concatenate(
        [jnp.where(col == ket_at, 1.0, 0.0), jnp.where(col == bra_at, 1.0, 0.0)], axis=0
    ).astype(BF16)


def pair_values(ket, picks):
    parts = dot(picks, jnp.concatenate(thirds(ket), axis=1))
    taken = parts[:, 0:128] + (parts[:, 128:256] + parts[:, 256:384])
    both = taken[0:512] * taken[512:1024]
    return both[0:256] + both[256:512]


def layer_rows(ket, picks):
    full = pair_values(ket, picks)
    lane = iota((64, 128), 1)
    at = [full[64 * m : 64 * (m + 1)] for m in range(4)]
    return jnp.concatenate(
        [
            jnp.where(lane < 96, at[0], at[1]),
            jnp.where(lane < 64, at[1], at[2]),
            jnp.where(lane < 32, at[2], at[3]),
        ],
        axis=1,
    )


def thirds(value):
    high = value.astype(BF16)
    rest = value - high.astype(F32)
    middle = rest.astype(BF16)
    low = (rest - middle.astype(F32)).astype(BF16)
    return high, middle, low


ROOT = 0.7071067811865476


def symmetric(tiles):
    return [tiles[0], (tiles[1] + tiles[2]) * ROOT, tiles[3], (tiles[1] - tiles[2]) * ROOT]


def plain(tiles):
    return [tiles[0], (tiles[1] + tiles[3]) * ROOT, (tiles[1] - tiles[3]) * ROOT, tiles[2]]


def is_even(*legs):
    return sum(leg == 3 for leg in legs) % 2 == 0


def basis_turn():
    row, col = iota((256, 256), 0), iota((256, 256), 1)
    value = jnp.ones((256, 256), F32)
    for to_shift, from_shift in ((6, 4), (4, 2), (2, 0), (0, 6)):
        new, old = (row >> to_shift) & 3, (col >> from_shift) & 3
        one = jnp.where(old == 1, 1.0, 0.0)
        two = jnp.where(old == 2, 1.0, 0.0)
        ends = jnp.where(new == 0, jnp.where(old == 0, 1.0, 0.0), jnp.where(old == 3, 1.0, 0.0))
        middle = jnp.where(new == 1, one + two, one - two)
        value = value * jnp.where((new & 1) == 0, ends, middle)
    return value.astype(BF16)


def even_rows(full, turn):
    parts = dot(turn, jnp.concatenate(thirds(full), axis=1))
    row = iota((256, 128), 0)
    halved = (row & 1) + ((row >> 2) & 1) + ((row >> 4) & 1) + ((row >> 6) & 1)
    factor = jnp.where((halved & 1) == 1, ROOT, 1.0) * jnp.where(
        halved >= 4, 0.25, jnp.where(halved >= 2, 0.5, 1.0)
    )
    return (parts[:, 0:128] + (parts[:, 128:256] + parts[:, 256:384])) * factor


def padded(parts):
    blank = jnp.zeros((32, parts[0].shape[1]), BF16)
    return jnp.concatenate([piece for part in parts for piece in (part, blank)], axis=0)


def apply_layer(state, scale, first, layers, second, third, slot, joined, middle):
    def side_by_side(part):
        blank = jnp.zeros((32, 128), BF16)
        return jnp.concatenate(
            [
                jnp.concatenate([part[leg * CHI : (leg + 1) * CHI], blank], axis=0)
                for leg in range(4)
            ],
            axis=1,
        )

    high, mid, low = (side_by_side(part) for part in thirds(state))
    joined[...] = dot(first[slot], jnp.concatenate([high, high, mid, mid, high, low], axis=0))
    block = 16
    for begin in range(0, CHI, block):
        tiles = {}
        for f in range(4):
            for m in range(4):
                rows = slice(f * CHI + begin, f * CHI + begin + block)
                tiles[f, m] = joined[rows, m * 128 : (m + 1) * 128]
        for g in range(4):
            for o in range(4):
                total = None
                for f in range(4):
                    for m in range(4):
                        if is_even(g, o, f, m):
                            at = ((g * 4 + o) * 4 + f) * 4 + m
                            term = layers[slot, at : at + 1, :] * tiles[f, m]
                            total = term if total is None else total + term
                high, mid, low = thirds(total)
                rows = slice(o * CHI + begin, o * CHI + begin + block)
                for index, part in enumerate((high, mid)):
                    lane = g * 256 + index * 128
                    middle[rows, lane : lane + 128] = part
                for index, part in enumerate((high, low)):
                    lane = 1024 + g * 256 + index * 128
                    middle[rows, lane : lane + 128] = part
    wide = dot(middle[:, 0:1024], second[slot])
    rest = dot(middle[:, 1024:2048], third[slot])
    return (wide[:, 0:128] + (wide[:, 128:256] + rest)) * scale


def nrm_scale(state):
    total = jnp.sum(jnp.sum(state * state, axis=0, keepdims=True), axis=1, keepdims=True)
    return lax.rsqrt(total * (1.0 / (CHI * WIDE)) + EPSILON)


def fold_pair(spread, coeffs, folded, slot):
    def body(index, carried):
        total = None
        for leg in range(4):
            term = coeffs[pl.ds(index * 4 + leg, 1), :] * spread[leg]
            total = term if total is None else total + term
        high, low = halves(total)
        rows = pl.ds(pl.multiple_of(index * CHI, CHI), CHI)
        folded[slot, rows, 0:WIDE] = high
        folded[slot, rows, WIDE : 2 * WIDE] = low
        return carried

    lax.fori_loop(0, 16, body, 0)


def apply_pair(state, scale, folded, second, slot, middle):
    high, low = halves(state)
    once = jnp.concatenate([high, low], axis=1)
    twice = jnp.concatenate([once, once], axis=0)
    for leg in range(4):
        wide = dot(folded[slot, leg * WIDE : (leg + 1) * WIDE, :], twice)
        high, low = halves(wide[:, 0:128] + wide[:, 128:256])
        middle[:, leg * 256 : leg * 256 + 128] = high
        middle[:, leg * 256 + 128 : leg * 256 + 256] = low
    wide = dot(middle[:, 0:1024], second[slot])
    return (wide[:, 0:128] + wide[:, 128:256]) * scale


def sweep_kernel(
    kets,
    left_maps,
    right_maps,
    top_edge,
    bottom_edge,
    left_edge,
    right_edge,
    outs,
    sides,
    row_kets,
    from_left,
    from_right,
    lefts,
    rights,
    ketses,
    select_one,
    select_two,
    spread,
    coeffs,
    picks,
    turn,
    layers,
    first,
    joined,
    second,
    third,
    env_folded,
    env_second,
    middle,
    entered,
    leaving,
    state,
    normed,
    last_in,
    env_entered,
    env_leaving,
    env_normed,
    map_send,
    map_recv,
    hop_send,
    hop_recv,
    row_send,
    out_recv,
    side_recv,
    ket_send,
    ket_recv,
    edge_send,
    pass_send,
    back_send,
    env_send,
    env_recv,
    over_send,
    over_recv,
):
    z = lax.axis_index("rows_0")
    xl = lax.axis_index("rows_1")
    core = lax.axis_index("rows_2")
    y = lax.axis_index("cols_0")
    xh = lax.axis_index("cols_1")
    planes = lax.axis_size("rows_0")
    stations = lax.axis_size("cols_0")
    end = planes - 1
    at_edge = (z == 0) | (z == end)
    low = jnp.where(at_edge, z, 1 + 2 * (jnp.maximum(z - 1, 0) // 2))
    count = jnp.where(at_edge, GROUP, 2 * GROUP)
    col = xl
    is_worker = at_edge | (core == 1)
    way = jnp.where(z == 0, 1 - core, jnp.where(z == end, core, z % 2))
    starts = ((way == 0) & (z == 0)) | ((way == 1) & (z == end))
    is_first = at_edge & starts
    is_last = at_edge & jnp.logical_not(starts)
    has_next = is_worker & jnp.logical_not(is_last)
    has_prev = is_worker & jnp.logical_not(is_first)
    mine = (z - low) * GROUP + xl * 2 + core
    place = xh * 2 + col
    ahead = z + 2 - 4 * way
    ahead = jnp.clip(ahead, 0, end)
    after = (ahead, xl, jnp.where((ahead == 0) | (ahead == end), 0, 1), y, xh)
    behind = jnp.where(
        way == 0, jnp.where(z == end, end - 1, z - 2), jnp.where(z == 0, 1, z + 2)
    )
    before = (jnp.clip(behind, 0, end), xl, 1, y, xh)
    mirror = jnp.where(z >= planes // 2, 1, 0)
    in_middle = (z == planes // 2) | (z == planes // 2 - 1)
    is_late = is_worker & (way != mirror) & jnp.logical_not(in_middle)
    station_first = ((core == 0) & (y == 0)) | ((core == 1) & (y == stations - 1))
    station_last = ((core == 0) & (y == stations - 1)) | ((core == 1) & (y == 0))
    leader = jnp.where(y >= stations // 2, 1, 0)

    def member(slot, y_to, xh_to):
        return (low + slot // GROUP, (slot % GROUP) // 2, slot % 2, y_to, xh_to)

    def env_member(slot):
        return (low + slot // GROUP, slot % 2, leader, y, (slot % GROUP) // 2)

    def remote(source, target, send_sem, recv_sem, device):
        return pltpu.make_async_remote_copy(
            src_ref=source,
            dst_ref=target,
            send_sem=send_sem,
            recv_sem=recv_sem,
            device_id=device,
            device_id_type=MESH,
        )

    def arrived(target, sem):
        pltpu.make_async_copy(target, target, sem).wait()

    barrier = pltpu.get_barrier_semaphore()

    def greet(device):
        pl.semaphore_signal(barrier, inc=1, device_id=device, device_id_type=MESH)

    def greet_slot(slot, carried):
        @pl.when(slot != mine)
        def _():
            greet(member(slot, y, xh))

        greet(member(slot, y, 1 - xh))
        for step in (1, stations - 1):
            for xh_to in range(2):
                greet(member(slot, (y + step) % stations, xh_to))
        return carried

    lax.fori_loop(0, count, greet_slot, 0)

    @pl.when(has_next)
    def _():
        greet(after)

    @pl.when(has_prev)
    def _():
        greet(before)

    def legs(m, g, o, f):
        return pick(way, m, o), f, pick(way, o, m), g

    @pl.when(is_worker)
    def _():
        for leg in range(4):
            row, lane = iota((WIDE, 128), 0), iota((WIDE, 128), 1)
            select_one[:, leg * 128 : (leg + 1) * 128] = jnp.where(
                (row == 4 * lane + leg) & (lane < CHI), 1.0, 0.0
            ).astype(BF16)
            row, lane = iota((128, WIDE), 0), iota((128, WIDE), 1)
            select_two[leg * 128 : (leg + 1) * 128, :] = jnp.where(
                (lane == 4 * row + leg) & (row < CHI), 1.0, 0.0
            ).astype(BF16)
        picks[...] = layer_picks(legs)
        turn[...] = basis_turn()

    pl.semaphore_wait(
        barrier, 6 * count - 1 + jnp.where(has_next, 1, 0) + jnp.where(has_prev, 1, 0)
    )

    def chain(index):
        to_way = (index // 2 + mirror) % 2
        to_col = index % 2
        to_start = ((to_way == 0) & (z == 0)) | ((to_way == 1) & (z == end))
        to_core = jnp.where(at_edge, jnp.where(to_start, 1, 0), 1)
        to_z = jnp.where(at_edge, z, low + 1 - to_way)
        own = (to_z == z) & (to_col == xl) & (to_core == core)
        return to_way, to_col, (to_z, to_col, to_core, y, xh), own

    def map_pairs(to_way, to_col):
        return (
            (left_maps.at[to_way, 0, to_col], lefts.at[mine]),
            (right_maps.at[to_way, 0, to_col], rights.at[mine]),
            (kets.at[to_col], ketses.at[mine]),
        )

    def send_map(index, carried):
        to_way, to_col, device, own = chain(index)

        @pl.when(own)
        def _():
            for kind, (source, target) in enumerate(map_pairs(to_way, to_col)):
                pltpu.make_async_copy(source, target, map_recv.at[mine, kind]).start()

        @pl.when(jnp.logical_not(own))
        def _():
            for kind, (source, target) in enumerate(map_pairs(to_way, to_col)):
                remote(
                    source, target, map_send.at[index, kind], map_recv.at[mine, kind], device
                ).start()

        return carried

    def map_sent(index, carried):
        to_way, to_col, device, own = chain(index)

        @pl.when(jnp.logical_not(own))
        def _():
            for kind, (source, target) in enumerate(map_pairs(to_way, to_col)):
                remote(
                    source, target, map_send.at[index, kind], map_recv.at[mine, kind], device
                ).wait_send()

        return carried

    def send_rest():
        lax.fori_loop(0, 2, map_sent, 0)
        lax.fori_loop(2, 4, send_map, 0)

    on_early = is_worker & (way == mirror)
    lax.fori_loop(0, 2, send_map, 0)

    half = pl.ds(2 * xh, 2)
    at_home = (core == xl) & (xl == xh)

    def ket_copy(to_core):
        device = (z, core, to_core, y, xl)
        return remote(kets, row_kets.at[half], ket_send.at[to_core], ket_recv.at[xh], device)

    def ket_back():
        device = (z, core, 0, jnp.maximum(y - 1, 0), xl)
        return remote(kets.at[0], row_kets.at[4], ket_send.at[2], ket_recv.at[2], device)

    def edge_copy(edge, to_core):
        return remote(edge.at[0], env_entered, edge_send, env_recv, (z, core, to_core, y, xl))

    for to_core in range(2):

        @pl.when(at_home & (core == to_core))
        def _():
            pltpu.make_async_copy(kets, row_kets.at[half], ket_recv.at[xh]).start()

        @pl.when(jnp.logical_not(at_home & (core == to_core)))
        def _():
            ket_copy(to_core).start()

    sends_back = (core == 0) & (y > 0)
    gets_back = (core == 0) & (y < stations - 1)
    kets_back = (xh == 0) & (y > 0)

    @pl.when(kets_back)
    def _():
        ket_back().start()

    edges = ((left_edge, 0, 0), (right_edge, 1, stations - 1))
    for edge, to_core, y_of in edges:

        @pl.when((y == y_of) & (xh == xl) & at_home & (core == to_core))
        def _():
            pltpu.make_async_copy(edge.at[0], env_entered, env_recv).start()

        @pl.when((y == y_of) & (xh == xl) & jnp.logical_not(at_home & (core == to_core)))
        def _():
            edge_copy(edge, to_core).start()

    @pl.when(is_first & (way == 0))
    def _():
        entered[...] = top_edge[col]

    @pl.when(is_first & (way == 1))
    def _():
        entered[...] = bottom_edge[col]


    def slot_at(number):
        return number + way * (count - 1 - 2 * number)

    def prepare(step):
        ordered = slot_at(step)
        j = jnp.where(is_first, ordered, (mine + step) % count)
        number = j + way * (count - 1 - 2 * j)
        for kind, target in enumerate((lefts, rights, ketses)):
            arrived(target.at[j], map_recv.at[j, kind])
        layers[number] = even_rows(pair_values(ketses[j], picks[...]), turn[...])
        apart = dot(jnp.concatenate(thirds(lefts[j]), axis=0), select_one[:, 0:512])
        apart = apart[0:CHI] + (apart[CHI : 2 * CHI] + apart[2 * CHI : 3 * CHI])
        legs_of = symmetric([apart[:, leg * 128 : (leg + 1) * 128] for leg in range(4)])
        for leg, tile in enumerate(legs_of):
            high, mid, lowest = thirds(tile)
            for index, part in enumerate((high, mid, high, mid, lowest, high)):
                lanes = slice(index * 128, (index + 1) * 128)
                first[number, leg * CHI : (leg + 1) * CHI, lanes] = part
        high, mid, lowest = thirds(rights[j])
        main = dot_nt(select_two[...], padded((high, mid)))
        fine = dot_nt(select_two[...], padded((lowest,)))
        apart = main[:, 0:128] + (main[:, 128:256] + fine)
        legs_of = symmetric([apart[leg * 128 : (leg + 1) * 128] for leg in range(4)])
        for leg, tile in enumerate(legs_of):
            high, mid, lowest = thirds(tile)
            for copy in range(2):
                begin = leg * 256 + copy * 128
                second[number, begin : begin + 128, 0:128] = high
                second[number, begin : begin + 128, 128:256] = mid
            third[number, leg * 256 : leg * 256 + 128, :] = lowest
            third[number, leg * 256 + 128 : leg * 256 + 256, :] = high

    def side_copy(number, source):
        return remote(
            source,
            sides.at[way, place],
            row_send.at[number, 0],
            side_recv.at[way, place],
            env_member(slot_at(number)),
        )

    def side_own(number):
        slot = slot_at(number)
        same_core = (slot % 2 == xl) & (leader == core)
        return (low + slot // GROUP == z) & same_core & ((slot % GROUP) // 2 == xh)

    def out_copy(number):
        return remote(
            normed.at[number + 1],
            outs.at[way, col],
            row_send.at[number, 1],
            out_recv.at[way, col],
            member(slot_at(number), y, xh),
        )

    def send_sides(number, source):
        @pl.when(side_own(number))
        def _():
            pltpu.make_async_copy(
                source, sides.at[way, place], side_recv.at[way, place]
            ).start()

        @pl.when(jnp.logical_not(side_own(number)))
        def _():
            side_copy(number, source).start()

    def send_out(number, carried):
        own = slot_at(number) == mine

        @pl.when(own)
        def _():
            pltpu.make_async_copy(
                normed.at[number + 1], outs.at[way, col], out_recv.at[way, col]
            ).start()

        @pl.when(jnp.logical_not(own))
        def _():
            out_copy(number).start()

        return carried

    def hop():
        return remote(leaving, entered, hop_send, hop_recv, after)

    def tiles_of(value):
        return [value[leg * CHI : (leg + 1) * CHI] for leg in range(4)]

    def advance(number):
        @pl.when(number == 0)
        def _():
            @pl.when(has_prev)
            def _():
                arrived(entered, hop_recv)

            came = unpack(entered[...])
            for leg, (tile, turned) in enumerate(zip(came, symmetric(came))):
                state[leg * CHI : (leg + 1) * CHI, :] = jnp.where(is_first, turned, tile)

        raw = is_first & (number == 0)
        closes = is_last & (number == count - 1)

        @pl.when(closes)
        def _():
            held = state[...]
            last_in[...] = pack(plain(tiles_of(held))) * nrm_scale(held)
            send_sides(number, last_in)

        current = state[...]
        scale = jnp.where(raw, 1.0, nrm_scale(current))
        renewed = apply_layer(
            current, scale, first, layers, second, third, number, joined, middle
        )
        normed[number] = pack(plain(tiles_of(current))) * scale
        state[...] = renewed

        @pl.when(number == count - 1)
        def _():
            final = state[...]
            leaving[...] = pack(tiles_of(final))

            @pl.when(has_next)
            def _():
                hop().start()

            normed[count] = pack(plain(tiles_of(final))) * nrm_scale(final)

        @pl.when(jnp.logical_not(closes))
        def _():
            send_sides(number, normed.at[number])

        @pl.when(number == count - 1)
        def _():
            lax.fori_loop(0, count, send_out, 0)


    def column_at(number):
        return number + core * (3 - 2 * number)

    def env_legs(m, g, o, f):
        return pick(mirror, f, g), pick(core, m, o), pick(mirror, g, f), pick(core, o, m)

    def env_selects():
        for part in range(2):
            arrived(row_kets.at[pl.ds(2 * part, 2)], ket_recv.at[part])
        picks[...] = layer_picks(env_legs)

        @pl.when(core == 0)
        def _():
            row, lane = iota((2 * CHI, WIDE), 0), iota((2 * CHI, WIDE), 1)
            row = jnp.where(row >= CHI, row - CHI, row)
            for _ in range(3):
                lane = jnp.where(lane >= CHI, lane - CHI, lane)
            select_one[0 : 2 * CHI, 0:WIDE] = jnp.where(row == lane, 1.0, 0.0).astype(BF16)

        @pl.when(core == 1)
        def _():
            for leg in range(4):
                row, lane = iota((WIDE, WIDE), 0), iota((WIDE, WIDE), 1)
                for _ in range(3):
                    lane = jnp.where(lane >= CHI, lane - CHI, lane)
                select_one[:, leg * WIDE : (leg + 1) * WIDE] = jnp.where(
                    row == leg * CHI + lane, 1.0, 0.0
                ).astype(BF16)
                row, lane = iota((128, WIDE), 0), iota((128, WIDE), 1)
                select_two[leg * 128 : (leg + 1) * 128, :] = jnp.where(
                    (lane == leg * CHI + row) & (row < CHI), 1.0, 0.0
                ).astype(BF16)

    def forward(side, column):
        target = sides.at[side, column]
        device = (z, xl, 1 - core, y, xh)
        return remote(
            target, target, pass_send.at[side, column], side_recv.at[side, column], device
        )

    def back(side):
        device = (z, xl, core, jnp.maximum(y - 1, 0), xh)
        return remote(
            sides.at[side, 0], sides.at[side, 4], back_send.at[side], side_recv.at[side, 4], device
        )

    def take_side(side, column):
        arrived(sides.at[side, column], side_recv.at[side, column])

        @pl.when(core == leader)
        def _():
            forward(side, column).start()

        @pl.when(sends_back & (column == 0))
        def _():
            back(side).start()

    def env_fold(number):
        @pl.when(number == 0)
        def _():
            env_selects()

        column = column_at(number)
        take_side(mirror, column)
        coeffs[...] = layer_rows(row_kets[column], picks[...])
        early = jnp.concatenate(halves(sides[mirror, column]), axis=0)

        @pl.when(core == 0)
        def _():
            turned = lax.dot_general(
                early,
                select_one[0 : 2 * CHI, 0:WIDE],
                (((0,), (0,)), ((), ())),
                preferred_element_type=F32,
            )
            for leg in range(4):
                spread[leg] = turned[leg * CHI : (leg + 1) * CHI]

        @pl.when(core == 1)
        def _():
            apart = dot(early, select_one[...])
            for leg in range(4):
                lanes = slice(leg * WIDE, (leg + 1) * WIDE)
                spread[leg] = apart[0:CHI, lanes] + apart[CHI : 2 * CHI, lanes]

        fold_pair(spread, coeffs, env_folded, number)

    def env_prepare(number):
        column = column_at(number)
        take_side(1 - mirror, column)

        @pl.when(core == 0)
        def _():
            for leg, tile in enumerate(unpack(sides[1 - mirror, column])):
                high, lowest = halves(tile)
                both = jnp.concatenate(
                    [jnp.concatenate([high, lowest], axis=1), jnp.zeros((32, 256), BF16)], axis=0
                )
                env_second[number, leg * 256 : leg * 256 + 128, :] = both
                env_second[number, leg * 256 + 128 : leg * 256 + 256, :] = both

        @pl.when(core == 1)
        def _():
            late = padded(halves(sides[1 - mirror, column]))
            turned = dot_nt(select_two[...], late).astype(BF16)
            for leg in range(4):
                for copy in range(2):
                    begin = leg * 256 + copy * 128
                    env_second[number, begin : begin + 128, :] = turned[leg * 128 : leg * 128 + 128]

    def env_hop():
        device = (z, xl, core, jnp.clip(y + 1 - 2 * core, 0, stations - 1), xh)
        return remote(env_leaving, env_entered, env_send, env_recv, device)

    def over(number):
        column = column_at(number)
        wraps = column == 0
        slot = jnp.where(wraps, 3, jnp.maximum(column - 1, 0))
        y_to = jnp.where(wraps, jnp.maximum(y - 1, 0), y)
        return remote(
            env_normed.at[number],
            from_right.at[slot],
            over_send.at[number],
            over_recv.at[slot],
            (z, xl, 0, y_to, xh),
        )

    def sends_over(number):
        return (core == 1) & ((y > 0) | (column_at(number) > 0))

    def flipped(tile):
        square = jnp.concatenate([tile, jnp.zeros((32, 128), F32)], axis=0)
        return square.T[0:CHI, :]

    def env_advance(number):
        @pl.when(number == 0)
        def _():
            arrived(env_entered, env_recv)
            flips = station_first & (mirror == 1)

            @pl.when(jnp.logical_not(flips))
            def _():
                for leg, tile in enumerate(unpack(env_entered[...])):
                    state[leg * CHI : (leg + 1) * CHI, :] = tile

            @pl.when(flips)
            def _():
                for leg, tile in enumerate(unpack(env_entered[...])):
                    state[leg * CHI : (leg + 1) * CHI, :] = flipped(tile)

        raw = station_first & (number == 0)

        @pl.when(jnp.logical_not(station_last & (number >= 2)))
        def _():
            current = state[...]
            scale = jnp.where(raw, 1.0, nrm_scale(current))
            renewed = apply_pair(current, scale, env_folded, env_second, number, middle)
            env_normed[number] = pack(tiles_of(current)) * scale
            state[...] = renewed

        @pl.when(station_last & (number >= 2))
        def _():
            current = state[...]
            env_normed[number] = pack(tiles_of(current)) * nrm_scale(current)

        @pl.when(jnp.logical_not(station_last) & (number == 3))
        def _():
            env_leaving[...] = pack(tiles_of(state[...]))
            env_hop().start()

        @pl.when(core == 0)
        def _():
            from_left[number] = env_normed[number]

        @pl.when(sends_over(number))
        def _():
            over(number).start()


    @pl.when(jnp.logical_not(on_early))
    def _():
        send_rest()

    turn_at = jnp.where(at_edge, 4, 1)
    total = jnp.where(is_worker, 2 * count, 0)
    before_fold = jnp.where(is_late, count, total)

    def task(index, carried):
        @pl.when(on_early & (index == turn_at))
        def _():
            send_rest()

        folds = (index >= before_fold) & (index < before_fold + 4)
        on_env = index >= total + 4
        on_boundary = jnp.logical_not(folds) & jnp.logical_not(on_env)
        step = jnp.where(index < before_fold, index, index - 4)
        prepares = (is_first & (step % 2 == 0)) | (jnp.logical_not(is_first) & (step < count))

        @pl.when(on_boundary & prepares)
        def _():
            prepare(jnp.where(is_first, step // 2, jnp.clip(step, 0, count - 1)))

        @pl.when(on_boundary & jnp.logical_not(prepares))
        def _():
            advance(jnp.where(is_first, step // 2, jnp.clip(step - count, 0, count - 1)))

        @pl.when(folds)
        def _():
            env_fold(jnp.clip(index - before_fold, 0, 3))

        late = index - (total + 4)
        readies = (station_first & (late % 2 == 0)) | (
            jnp.logical_not(station_first) & (late < 4)
        )

        @pl.when(on_env & readies)
        def _():
            env_prepare(jnp.where(station_first, late // 2, jnp.clip(late, 0, 3)))

        @pl.when(on_env & jnp.logical_not(readies))
        def _():
            env_advance(jnp.where(station_first, late // 2, jnp.clip(late - 4, 0, 3)))

        return carried

    lax.fori_loop(0, total + 12, task, 0)


    lax.fori_loop(2, 4, map_sent, 0)

    @pl.when(has_next)
    def _():
        hop().wait_send()

    def row_sent(number, carried):
        @pl.when(jnp.logical_not(side_own(number)))
        def _():
            side_copy(number, normed.at[number]).wait_send()

        @pl.when(slot_at(number) != mine)
        def _():
            out_copy(number).wait_send()

        return carried

    lax.fori_loop(0, total // 2, row_sent, 0)

    for to_core in range(2):

        @pl.when(jnp.logical_not(at_home & (core == to_core)))
        def _():
            ket_copy(to_core).wait_send()

    @pl.when(kets_back)
    def _():
        ket_back().wait_send()

    for edge, to_core, y_of in edges:

        @pl.when((y == y_of) & (xh == xl) & jnp.logical_not(at_home & (core == to_core)))
        def _():
            edge_copy(edge, to_core).wait_send()

    for side in range(2):

        @pl.when(core == leader)
        def _():
            for column in range(4):
                forward(side, column).wait_send()

        @pl.when(sends_back)
        def _():
            back(side).wait_send()

    @pl.when(jnp.logical_not(station_last))
    def _():
        env_hop().wait_send()

    for number in range(4):

        @pl.when(sends_over(number))
        def _():
            over(number).wait_send()

    for direction in range(2):
        for column in range(2):
            arrived(outs.at[direction, column], out_recv.at[direction, column])

    @pl.when(gets_back)
    def _():
        for direction in range(2):
            arrived(sides.at[direction, 4], side_recv.at[direction, 4])
        arrived(row_kets.at[4], ket_recv.at[2])

    @pl.when(core == 0)
    def _():
        for slot in range(3):
            arrived(from_right.at[slot], over_recv.at[slot])

    @pl.when(gets_back)
    def _():
        arrived(from_right.at[3], over_recv.at[3])


def run_sweep(kets, left_maps, right_maps, top_edge, bottom_edge, left_edge, right_edge):
    vmem = pl.BlockSpec(memory_space=pltpu.VMEM)
    anywhere = pl.BlockSpec(memory_space=pl.ANY)
    column = (CHI, WIDE)
    most = 2 * GROUP
    dma = pltpu.SemaphoreType.DMA
    return pl.pallas_call(
        sweep_kernel,
        out_shape=(
            jax.ShapeDtypeStruct((2, 2) + column, F32),
            jax.ShapeDtypeStruct((2, 5) + column, F32),
            jax.ShapeDtypeStruct((5, 32, 128), F32),
            jax.ShapeDtypeStruct((4,) + column, F32),
            jax.ShapeDtypeStruct((4,) + column, F32),
        ),
        in_specs=[vmem, anywhere, anywhere] + [vmem] * 4,
        out_specs=(vmem,) * 5,
        scratch_shapes=[
            pltpu.VMEM((most,) + column, F32),
            pltpu.VMEM((most,) + column, F32),
            pltpu.VMEM((most, 32, 128), F32),
            pltpu.VMEM((WIDE, 4 * WIDE), BF16),
            pltpu.VMEM((512, WIDE), BF16),
            pltpu.VMEM((4,) + column, F32),
            pltpu.VMEM((64, WIDE), F32),
            pltpu.VMEM((1024, 32), BF16),
            pltpu.VMEM((256, 256), BF16),
            pltpu.VMEM((most, 256, 128), F32),
            pltpu.VMEM((most, WIDE, 768), BF16),
            pltpu.VMEM((WIDE, 512), F32),
            pltpu.VMEM((most, 1024, 256), BF16),
            pltpu.VMEM((most, 1024, 128), BF16),
            pltpu.VMEM((4, 16 * CHI, 2 * WIDE), BF16),
            pltpu.VMEM((4, 1024, 256), BF16),
            pltpu.VMEM((WIDE, 2048), BF16),
            pltpu.VMEM(column, F32),
            pltpu.VMEM(column, F32),
            pltpu.VMEM((WIDE, 128), F32),
            pltpu.VMEM((most + 1,) + column, F32),
            pltpu.VMEM(column, F32),
            pltpu.VMEM(column, F32),
            pltpu.VMEM(column, F32),
            pltpu.VMEM((4,) + column, F32),
            dma((4, 3)),
            dma((most, 3)),
            dma,
            dma,
            dma((most, 2)),
            dma((2, 2)),
            dma((2, 5)),
            dma((3,)),
            dma((3,)),
            dma,
            dma((2, 4)),
            dma((2,)),
            dma,
            dma,
            dma((4,)),
            dma((4,)),
        ],
        compiler_params=pltpu.CompilerParams(
            collective_id=0, has_side_effects=True, vmem_limit_bytes=67043328
        ),
        name="sweep",
    )(kets, left_maps, right_maps, top_edge, bottom_edge, left_edge, right_edge)


def dot_general(left, right, dims):
    return lax.dot_general(left, right, (dims, ((), ())), preferred_element_type=F32)


def pad_rows(value):
    return jnp.concatenate([value, jnp.zeros((32, value.shape[1]), value.dtype)], axis=0)


def swap_legs(entry):
    return (entry & 0b10101) | ((entry >> 3) & 1) << 1 | ((entry >> 1) & 1) << 3


def open_site(ket, legs_at, wide, opened):
    def body(block, carried):
        begin = pl.multiple_of(block * 8, 8)
        half_done = {}
        for bra in range(8):
            u2, m2, d2 = bra >> 2, (bra >> 1) & 1, bra & 1
            tiles = []
            for top in range(8):
                u, m, d = top >> 2, (top >> 1) & 1, top & 1
                row = (2 * m + m2) * 4 + 2 * u + u2
                lane = (2 * d + d2) * 128
                tiles.append(wide[pl.ds(row * CHI + begin, 8), lane : lane + 128])
            for state in range(2):
                for out in range(2):
                    total = None
                    for top in range(8):
                        at = state * 16 + legs_at(top >> 2, (top >> 1) & 1, top & 1, out)
                        term = ket[at : at + 1, :] * tiles[top]
                        total = term if total is None else total + term
                    half_done[state, out, bra] = total
        for state in range(2):
            for out in range(2):
                for other in range(2):
                    for out2 in range(2):
                        total = None
                        for bra in range(8):
                            at = other * 16 + legs_at(bra >> 2, (bra >> 1) & 1, bra & 1, out2)
                            term = ket[at : at + 1, :] * half_done[state, out, bra]
                            total = term if total is None else total + term
                        row = (2 * out + out2) * CHI
                        opened[state * 2 + other, pl.ds(row + begin, 8), :] = total
        return carried

    lax.fori_loop(0, CHI // 8, body, 0)


def energy_kernel(
    term_rows,
    term_bonds,
    term_ops,
    operators,
    all_sides,
    all_kets,
    all_left,
    all_right,
    shares,
    wide,
    opened,
    closing,
    density,
    ket,
    sides,
    row_kets,
    from_left,
    from_right,
    fetch,
):
    way = lax.axis_index("rows_2")
    row_here = (
        lax.axis_index("rows_0") * GROUP + lax.axis_index("cols_1") * 2 + lax.axis_index("rows_1")
    )
    first = lax.axis_index("cols_0") * 4
    planes = lax.axis_size("rows_0")
    mirror = jnp.where(lax.axis_index("rows_0") >= planes // 2, 1, 0)

    def take_ket(column):
        for entry in range(32):
            ket[entry : entry + 1, :] = jnp.where(
                mirror == 1,
                row_kets[column, swap_legs(entry) : swap_legs(entry) + 1, :],
                row_kets[column, entry : entry + 1, :],
            )

    shares[...] = jnp.zeros((8, 128), F32)

    def hits(term, column):
        here = (term_rows[term] == row_here) & (term_bonds[term] == first + column)
        return here & (way == 0)

    def column_body(column, carried):
        count = 0
        for term in range(TERMS):
            count = count + jnp.where(hits(term, column), 1, 0)

        @pl.when(count > 0)
        def _():
            copies = [
                pltpu.make_async_copy(
                    all_sides.at[:, pl.ds(column, 2)], sides, fetch.at[0]
                ),
                pltpu.make_async_copy(all_kets.at[pl.ds(column, 2)], row_kets, fetch.at[1]),
                pltpu.make_async_copy(all_left.at[column], from_left, fetch.at[2]),
                pltpu.make_async_copy(all_right.at[column], from_right, fetch.at[3]),
            ]
            for copy in copies:
                copy.start()
            for copy in copies:
                copy.wait()

            high, low = halves(sides[mirror, 0])
            both = jnp.concatenate([high, low], axis=0)
            state_high, state_low = halves(jnp.concatenate(unpack(from_left[...]), axis=1))
            tn = ((0,), (0,))
            joined = dot_general(
                both, jnp.concatenate([state_high, state_high], axis=0), tn
            ) + dot_general(both, jnp.concatenate([state_low, state_low], axis=0), tn)
            below_high, below_low = halves(jnp.concatenate(unpack(sides[1 - mirror, 0]), axis=1))
            main = jnp.concatenate([pad_rows(below_high), pad_rows(below_high)], axis=0)
            fine = jnp.concatenate([pad_rows(below_low), pad_rows(below_low)], axis=0)
            for leg in range(4):
                part = jnp.concatenate(halves(joined[:, leg * 128 : (leg + 1) * 128]), axis=1)
                wide[leg * WIDE : (leg + 1) * WIDE, :] = dot(part, main) + dot(part, fine)
            take_ket(0)
            open_site(
                ket,
                lambda u, m, d, out: u * 8 + m * 4 + d * 2 + out,
                wide,
                opened,
            )

            above = jnp.concatenate(unpack(sides[mirror, 1]), axis=0)
            both = jnp.concatenate(halves(above), axis=1)
            state_high, state_low = halves(jnp.concatenate(unpack(from_right[...]), axis=1))
            state_high, state_low = pad_rows(state_high), pad_rows(state_low)
            joined = dot(both, jnp.concatenate([state_high, state_high], axis=0)) + dot(
                both, jnp.concatenate([state_low, state_low], axis=0)
            )
            below_high, below_low = halves(
                jnp.concatenate([pad_rows(tile) for tile in unpack(sides[1 - mirror, 1])], axis=0)
            )
            main = jnp.concatenate([below_high, below_high], axis=1)
            fine = jnp.concatenate([below_low, below_low], axis=1)
            for leg in range(4):
                part = jnp.concatenate(halves(joined[:, leg * 128 : (leg + 1) * 128]), axis=1)
                wide[leg * WIDE : (leg + 1) * WIDE, :] = dot_nt(part, main) + dot_nt(part, fine)
            take_ket(1)
            open_site(
                ket,
                lambda u, m, d, out: u * 8 + out * 4 + d * 2 + m,
                wide,
                closing,
            )

            for pair in range(4):
                for other in range(4):
                    product = opened[pair] * closing[other]
                    at = pair * 4 + other
                    density[at : at + 1, :] = jnp.sum(product, axis=0, keepdims=True)
            rho = jnp.sum(density[...], axis=1, keepdims=True)
            index = iota((16, 1), 0)
            diagonal = (index == 0) | (index == 3) | (index == 12) | (index == 15)
            trace = jnp.sum(jnp.where(diagonal, rho, 0.0), axis=0, keepdims=True)
            spread = jnp.sqrt(jnp.sum(rho * rho, axis=0, keepdims=True))
            bottom = jnp.maximum(jnp.abs(trace), 0.25 * spread)

            def term_body(term, kept):
                @pl.when(hits(term, column))
                def _():
                    chosen = jnp.zeros((16, 1), F32)
                    for entry in range(16):
                        chosen = jnp.where(
                            index == entry, operators[term_ops[term], entry], chosen
                        )
                    value = jnp.sum(chosen * rho, axis=0, keepdims=True) / bottom
                    lane = iota((8, 128), 1)
                    shares[...] = jnp.where(lane == term, value, shares[...])

                return kept

            lax.fori_loop(0, TERMS, term_body, 0)

        return carried

    lax.fori_loop(0, 4, column_body, 0)


def run_energies(term_rows, term_bonds, term_ops, operators, sides, row_kets, lefts, rights):
    vmem = pl.BlockSpec(memory_space=pltpu.VMEM)
    smem = pl.BlockSpec(memory_space=pltpu.SMEM)
    return pl.pallas_call(
        energy_kernel,
        out_shape=jax.ShapeDtypeStruct((8, 128), F32),
        in_specs=[smem] * 4 + [pl.BlockSpec(memory_space=pl.ANY)] * 4,
        out_specs=vmem,
        scratch_shapes=[
            pltpu.VMEM((16 * CHI, 512), F32),
            pltpu.VMEM((4, WIDE, 128), F32),
            pltpu.VMEM((4, WIDE, 128), F32),
            pltpu.VMEM((16, 128), F32),
            pltpu.VMEM((32, 128), F32),
            pltpu.VMEM((2, 2, CHI, WIDE), F32),
            pltpu.VMEM((2, 32, 128), F32),
            pltpu.VMEM((CHI, WIDE), F32),
            pltpu.VMEM((CHI, WIDE), F32),
            pltpu.SemaphoreType.DMA((4,)),
        ],
        compiler_params=pltpu.CompilerParams(vmem_limit_bytes=67043328),
        name="energies",
    )(term_rows, term_bonds, term_ops, operators, sides, row_kets, lefts, rights)


def sum_kernel(shares, total, planes_in, plane_in, partial, send_one, recv_one, send_two, recv_two):
    z = lax.axis_index("rows_0")
    xl = lax.axis_index("rows_1")
    core = lax.axis_index("rows_2")
    y = lax.axis_index("cols_0")
    xh = lax.axis_index("cols_1")
    way = core
    place = y * 4 + xl * 2 + xh
    barrier = pltpu.get_barrier_semaphore()

    def greet(device):
        pl.semaphore_signal(barrier, inc=1, device_id=device, device_id_type=MESH)

    def along(step):
        return ((z + step) % 8, xl, core, y, xh)

    def within(step):
        other = (place * 2 + way + step) % 32
        return (z, (other // 4) % 2, other % 2, other // 8, (other // 2) % 2)

    for step in range(1, 8):
        greet(along(step))
    for step in range(1, 32):
        greet(within(step))
    pl.semaphore_wait(barrier, 38)

    def first(step):
        return pltpu.make_async_remote_copy(
            src_ref=shares,
            dst_ref=planes_in.at[z],
            send_sem=send_one.at[step],
            recv_sem=recv_one.at[z],
            device_id=along(step),
            device_id_type=MESH,
        )

    def second(step):
        return pltpu.make_async_remote_copy(
            src_ref=partial,
            dst_ref=plane_in.at[place],
            send_sem=send_two.at[step],
            recv_sem=recv_two.at[place],
            device_id=within(step),
            device_id_type=MESH,
        )

    @pl.when(way == 0)
    def _():
        for step in range(1, 8):
            first(step).start()
        pltpu.make_async_copy(shares, planes_in.at[z], recv_one.at[z]).start()
        added = None
        for plane in range(8):
            target = planes_in.at[plane]
            pltpu.make_async_copy(target, target, recv_one.at[plane]).wait()
        for plane in range(8):
            added = planes_in[plane] if added is None else added + planes_in[plane]
        partial[...] = added
        for step in range(1, 32):
            second(step).start()
        pltpu.make_async_copy(partial, plane_in.at[place], recv_two.at[place]).start()

    for other in range(16):
        target = plane_in.at[other]
        pltpu.make_async_copy(target, target, recv_two.at[other]).wait()
    added = None
    for other in range(16):
        added = plane_in[other] if added is None else added + plane_in[other]
    total[...] = added[0:1, 0:TERMS]

    @pl.when(way == 0)
    def _():
        for step in range(1, 8):
            first(step).wait_send()
        for step in range(1, 32):
            second(step).wait_send()


def run_sum(shares):
    vmem = pl.BlockSpec(memory_space=pltpu.VMEM)
    return pl.pallas_call(
        sum_kernel,
        out_shape=jax.ShapeDtypeStruct((1, TERMS), F32),
        in_specs=[vmem],
        out_specs=vmem,
        scratch_shapes=[
            pltpu.VMEM((8, 8, 128), F32),
            pltpu.VMEM((16, 8, 128), F32),
            pltpu.VMEM((8, 128), F32),
            pltpu.SemaphoreType.DMA((8,)),
            pltpu.SemaphoreType.DMA((8,)),
            pltpu.SemaphoreType.DMA((32,)),
            pltpu.SemaphoreType.DMA((16,)),
        ],
        compiler_params=pltpu.CompilerParams(
            collective_id=2, has_side_effects=True, vmem_limit_bytes=67043328
        ),
        name="shares_sum",
    )(shares)


def shards(
    kets,
    left_maps,
    right_maps,
    top_edge,
    bottom_edge,
    left_edge,
    right_edge,
    term_rows,
    term_bonds,
    term_ops,
    operators,
):
    spread_kets = jnp.broadcast_to(kets[0][:, :, None], (kets.shape[1], 32, 128))
    outs, sides, row_kets, lefts, rights = run_sweep(
        spread_kets, left_maps, right_maps, top_edge, bottom_edge, left_edge, right_edge
    )
    shares = run_energies(
        term_rows, term_bonds, term_ops, operators, sides, row_kets, lefts, rights
    )
    energies = run_sum(shares).reshape(TERMS)
    return (outs[0][None], outs[1][None], energies)


def solution(mesh):
    torus = Mesh(
        mesh.devices.reshape(8, 2, 2, 4, 2), ("rows_0", "rows_1", "rows_2", "cols_0", "cols_1")
    )
    placed = (
        P(ROWS, COLS, None),
        P(None, ROWS, COLS, None, None),
        P(None, ROWS, COLS, None, None),
        P(COLS, None, None),
        P(COLS, None, None),
        P(ROWS, None, None),
        P(ROWS, None, None),
        P(),
        P(),
        P(),
        P(),
    )
    return jax.shard_map(
        shards,
        mesh=torus,
        in_specs=placed,
        out_specs=(P(ROWS, COLS, None, None), P(ROWS, COLS, None, None), P()),
        check_vma=False,
    )
```

```python
import functools

import jax
import jax.numpy as jnp
from jax import lax
from jax.experimental import pallas as pl
from jax.experimental.pallas import tpu as pltpu
from jax.sharding import Mesh
from jax.sharding import PartitionSpec as P

D = 2
D2 = 4
PHYS = 2
CHI = 96
WIDE = D2 * CHI
OPS = 4
TERMS = 16
GROUP = 4
ROWS = ("rows_0", "rows_1", "rows_2")
COLS = ("cols_0", "cols_1")
ROWS_COLS = ("rows_0", "rows_1", "rows_2", "cols_0", "cols_1")
MESH = pl.DeviceIdType.MESH

EPSILON = 1e-06
PRECISION_HIGH = lax.Precision.HIGHEST
F32 = jnp.float32
BF16 = jnp.bfloat16


def iota(shape, dim):
    return lax.broadcasted_iota(jnp.int32, shape, dim)


def halves(value):
    high = value.astype(BF16)
    low = (value - high.astype(F32)).astype(BF16)
    return high, low


def dot(left, right):
    return jnp.dot(left, right, preferred_element_type=F32)


def dot_nt(left, right):
    return lax.dot_general(left, right, (((1,), (1,)), ((), ())), preferred_element_type=F32)


def unpack(wide):
    one, two, three = wide[:, 0:128], wide[:, 128:256], wide[:, 256:384]
    lane = iota((CHI, 128), 1)
    parts = (
        one,
        pltpu.roll(jnp.where(lane >= 96, one, two), 32, 1),
        pltpu.roll(jnp.where(lane >= 64, two, three), 64, 1),
        pltpu.roll(three, 96, 1),
    )
    return [jnp.where(lane < CHI, part, 0.0) for part in parts]


def pack(tiles):
    lane = iota((CHI, 128), 1)
    first = tiles[0]
    second = pltpu.roll(tiles[1], 96, 1)
    third = pltpu.roll(tiles[2], 64, 1)
    fourth = pltpu.roll(tiles[3], 32, 1)
    return jnp.concatenate(
        [
            jnp.where(lane < 96, first, second),
            jnp.where(lane < 64, second, third),
            jnp.where(lane < 32, third, fourth),
        ],
        axis=1,
    )


def pick(mode, *choices):
    value = choices[-1]
    for index in range(len(choices) - 1):
        value = jnp.where(mode == index, choices[index], value)
    return value


def layer_picks(legs):
    shape = (PHYS * 256, 32)
    row, col = iota(shape, 0), iota(shape, 1)
    digits = ((row >> 6) & 3, (row >> 4) & 3, (row >> 2) & 3, row & 3)
    up, left, down, right = legs(*digits)
    base = (row >> 8) * 16
    ket_at = base + (up >> 1) * 8 + (left >> 1) * 4 + (down >> 1) * 2 + (right >> 1)
    bra_at = base + (up & 1) * 8 + (left & 1) * 4 + (down & 1) * 2 + (right & 1)
    return jnp.concatenate(
        [jnp.where(col == ket_at, 1.0, 0.0), jnp.where(col == bra_at, 1.0, 0.0)], axis=0
    ).astype(BF16)


def pair_values(ket, picks):
    parts = dot(picks, jnp.concatenate(thirds(ket), axis=1))
    taken = parts[:, 0:128] + (parts[:, 128:256] + parts[:, 256:384])
    both = taken[0:512] * taken[512:1024]
    return both[0:256] + both[256:512]


def layer_rows(ket, picks):
    full = pair_values(ket, picks)
    lane = iota((64, 128), 1)
    at = [full[64 * m : 64 * (m + 1)] for m in range(4)]
    return jnp.concatenate(
        [
            jnp.where(lane < 96, at[0], at[1]),
            jnp.where(lane < 64, at[1], at[2]),
            jnp.where(lane < 32, at[2], at[3]),
        ],
        axis=1,
    )


def thirds(value):
    high = value.astype(BF16)
    rest = value - high.astype(F32)
    middle = rest.astype(BF16)
    low = (rest - middle.astype(F32)).astype(BF16)
    return high, middle, low


ROOT = 0.7071067811865476


def symmetric(tiles):
    return [tiles[0], (tiles[1] + tiles[2]) * ROOT, tiles[3], (tiles[1] - tiles[2]) * ROOT]


def plain(tiles):
    return [tiles[0], (tiles[1] + tiles[3]) * ROOT, (tiles[1] - tiles[3]) * ROOT, tiles[2]]


def is_even(*legs):
    return sum(leg == 3 for leg in legs) % 2 == 0


def basis_turn():
    row, col = iota((256, 256), 0), iota((256, 256), 1)
    value = jnp.ones((256, 256), F32)
    for to_shift, from_shift in ((6, 4), (4, 2), (2, 0), (0, 6)):
        new, old = (row >> to_shift) & 3, (col >> from_shift) & 3
        one = jnp.where(old == 1, 1.0, 0.0)
        two = jnp.where(old == 2, 1.0, 0.0)
        ends = jnp.where(new == 0, jnp.where(old == 0, 1.0, 0.0), jnp.where(old == 3, 1.0, 0.0))
        middle = jnp.where(new == 1, one + two, one - two)
        value = value * jnp.where((new & 1) == 0, ends, middle)
    return value.astype(BF16)


def even_rows(full, turn):
    parts = dot(turn, jnp.concatenate(thirds(full), axis=1))
    row = iota((256, 128), 0)
    halved = (row & 1) + ((row >> 2) & 1) + ((row >> 4) & 1) + ((row >> 6) & 1)
    factor = jnp.where((halved & 1) == 1, ROOT, 1.0) * jnp.where(
        halved >= 4, 0.25, jnp.where(halved >= 2, 0.5, 1.0)
    )
    return (parts[:, 0:128] + (parts[:, 128:256] + parts[:, 256:384])) * factor


def padded(parts):
    blank = jnp.zeros((32, parts[0].shape[1]), BF16)
    return jnp.concatenate([piece for part in parts for piece in (part, blank)], axis=0)


def apply_layer(state, scale, first, layers, second, third, slot, joined, middle):
    def side_by_side(part):
        blank = jnp.zeros((32, 128), BF16)
        return jnp.concatenate(
            [
                jnp.concatenate([part[leg * CHI : (leg + 1) * CHI], blank], axis=0)
                for leg in range(4)
            ],
            axis=1,
        )

    high, mid, low = (side_by_side(part) for part in thirds(state))
    joined[...] = dot(first[slot], jnp.concatenate([high, high, mid, mid, high, low], axis=0))
    block = 16
    for begin in range(0, CHI, block):
        tiles = {}
        for f in range(4):
            for m in range(4):
                rows = slice(f * CHI + begin, f * CHI + begin + block)
                tiles[f, m] = joined[rows, m * 128 : (m + 1) * 128]
        for g in range(4):
            for o in range(4):
                total = None
                for f in range(4):
                    for m in range(4):
                        if is_even(g, o, f, m):
                            at = ((g * 4 + o) * 4 + f) * 4 + m
                            term = layers[slot, at : at + 1, :] * tiles[f, m]
                            total = term if total is None else total + term
                high, mid, low = thirds(total)
                rows = slice(o * CHI + begin, o * CHI + begin + block)
                for index, part in enumerate((high, mid)):
                    lane = g * 256 + index * 128
                    middle[rows, lane : lane + 128] = part
                for index, part in enumerate((high, low)):
                    lane = 1024 + g * 256 + index * 128
                    middle[rows, lane : lane + 128] = part
    wide = dot(middle[:, 0:1024], second[slot])
    rest = dot(middle[:, 1024:2048], third[slot])
    return (wide[:, 0:128] + (wide[:, 128:256] + rest)) * scale


def nrm_scale(state):
    total = jnp.sum(jnp.sum(state * state, axis=0, keepdims=True), axis=1, keepdims=True)
    return lax.rsqrt(total * (1.0 / (CHI * WIDE)) + EPSILON)


def fold_pair(spread, coeffs, folded, slot):
    def body(index, carried):
        total = None
        for leg in range(4):
            term = coeffs[pl.ds(index * 4 + leg, 1), :] * spread[leg]
            total = term if total is None else total + term
        high, low = halves(total)
        rows = pl.ds(pl.multiple_of(index * CHI, CHI), CHI)
        folded[slot, rows, 0:WIDE] = high
        folded[slot, rows, WIDE : 2 * WIDE] = low
        return carried

    lax.fori_loop(0, 16, body, 0)


def apply_pair(state, scale, folded, second, slot, middle):
    high, low = halves(state)
    once = jnp.concatenate([high, low], axis=1)
    twice = jnp.concatenate([once, once], axis=0)
    for leg in range(4):
        wide = dot(folded[slot, leg * WIDE : (leg + 1) * WIDE, :], twice)
        high, low = halves(wide[:, 0:128] + wide[:, 128:256])
        middle[:, leg * 256 : leg * 256 + 128] = high
        middle[:, leg * 256 + 128 : leg * 256 + 256] = low
    wide = dot(middle[:, 0:1024], second[slot])
    return (wide[:, 0:128] + wide[:, 128:256]) * scale


def sweep_kernel(
    own_kets,
    left_maps,
    right_maps,
    top_edge,
    bottom_edge,
    left_edge,
    right_edge,
    outs,
    sides,
    row_kets,
    from_left,
    from_right,
    kets,
    lefts,
    rights,
    ketses,
    select_one,
    select_two,
    spread,
    coeffs,
    picks,
    turn,
    layers,
    first,
    joined,
    second,
    third,
    env_folded,
    env_second,
    middle,
    entered,
    leaving,
    state,
    normed,
    last_in,
    env_entered,
    env_leaving,
    env_normed,
    map_send,
    map_recv,
    hop_send,
    hop_recv,
    row_send,
    out_recv,
    side_recv,
    ket_send,
    ket_recv,
    edge_send,
    pass_send,
    back_send,
    env_send,
    env_recv,
    over_send,
    over_recv,
):
    z = lax.axis_index("rows_0")
    xl = lax.axis_index("rows_1")
    core = lax.axis_index("rows_2")
    y = lax.axis_index("cols_0")
    xh = lax.axis_index("cols_1")
    planes = lax.axis_size("rows_0")
    stations = lax.axis_size("cols_0")
    end = planes - 1
    at_edge = (z == 0) | (z == end)
    low = jnp.where(at_edge, z, 1 + 2 * (jnp.maximum(z - 1, 0) // 2))
    count = jnp.where(at_edge, GROUP, 2 * GROUP)
    col = xl
    is_worker = at_edge | (core == 1)
    way = jnp.where(z == 0, 1 - core, jnp.where(z == end, core, z % 2))
    starts = ((way == 0) & (z == 0)) | ((way == 1) & (z == end))
    is_first = at_edge & starts
    is_last = at_edge & jnp.logical_not(starts)
    has_next = is_worker & jnp.logical_not(is_last)
    has_prev = is_worker & jnp.logical_not(is_first)
    mine = (z - low) * GROUP + xl * 2 + core
    place = xh * 2 + col
    ahead = z + 2 - 4 * way
    ahead = jnp.clip(ahead, 0, end)
    after = (ahead, xl, jnp.where((ahead == 0) | (ahead == end), 0, 1), y, xh)
    behind = jnp.where(
        way == 0, jnp.where(z == end, end - 1, z - 2), jnp.where(z == 0, 1, z + 2)
    )
    before = (jnp.clip(behind, 0, end), xl, 1, y, xh)
    mirror = jnp.where(z >= planes // 2, 1, 0)
    in_middle = (z == planes // 2) | (z == planes // 2 - 1)
    is_late = is_worker & (way != mirror) & jnp.logical_not(in_middle)
    station_first = ((core == 0) & (y == 0)) | ((core == 1) & (y == stations - 1))
    station_last = ((core == 0) & (y == stations - 1)) | ((core == 1) & (y == 0))
    leader = jnp.where(y >= stations // 2, 1, 0)

    def member(slot, y_to, xh_to):
        return (low + slot // GROUP, (slot % GROUP) // 2, slot % 2, y_to, xh_to)

    def env_member(slot):
        return (low + slot // GROUP, slot % 2, leader, y, (slot % GROUP) // 2)

    def remote(source, target, send_sem, recv_sem, device):
        return pltpu.make_async_remote_copy(
            src_ref=source,
            dst_ref=target,
            send_sem=send_sem,
            recv_sem=recv_sem,
            device_id=device,
            device_id_type=MESH,
        )

    def arrived(target, sem):
        pltpu.make_async_copy(target, target, sem).wait()

    barrier = pltpu.get_barrier_semaphore()

    def greet(device):
        pl.semaphore_signal(barrier, inc=1, device_id=device, device_id_type=MESH)

    def greet_slot(slot, carried):
        @pl.when(slot != mine)
        def _():
            greet(member(slot, y, xh))

        greet(member(slot, y, 1 - xh))
        for step in (1, stations - 1):
            for xh_to in range(2):
                greet(member(slot, (y + step) % stations, xh_to))
        return carried

    lax.fori_loop(0, count, greet_slot, 0)

    @pl.when(has_next)
    def _():
        greet(after)

    @pl.when(has_prev)
    def _():
        greet(before)

    for local in range(2):
        chosen = iota((32, 32), 0) == iota((32, 32), 1)
        spaced = jnp.where(chosen, own_kets[local : local + 1, :], 0.0)
        ones = jnp.ones((32, 128), BF16)
        high, mid, lowest = (dot(part, ones) for part in thirds(spaced))
        kets[local] = high + (mid + lowest)

    def legs(m, g, o, f):
        return pick(way, m, o), f, pick(way, o, m), g

    @pl.when(is_worker)
    def _():
        for leg in range(4):
            row, lane = iota((WIDE, 128), 0), iota((WIDE, 128), 1)
            select_one[:, leg * 128 : (leg + 1) * 128] = jnp.where(
                (row == 4 * lane + leg) & (lane < CHI), 1.0, 0.0
            ).astype(BF16)
            row, lane = iota((128, WIDE), 0), iota((128, WIDE), 1)
            select_two[leg * 128 : (leg + 1) * 128, :] = jnp.where(
                (lane == 4 * row + leg) & (row < CHI), 1.0, 0.0
            ).astype(BF16)
        picks[...] = layer_picks(legs)
        turn[...] = basis_turn()

    pl.semaphore_wait(
        barrier, 6 * count - 1 + jnp.where(has_next, 1, 0) + jnp.where(has_prev, 1, 0)
    )

    def chain(index):
        to_way = (index // 2 + mirror) % 2
        to_col = index % 2
        to_start = ((to_way == 0) & (z == 0)) | ((to_way == 1) & (z == end))
        to_core = jnp.where(at_edge, jnp.where(to_start, 1, 0), 1)
        to_z = jnp.where(at_edge, z, low + 1 - to_way)
        own = (to_z == z) & (to_col == xl) & (to_core == core)
        return to_way, to_col, (to_z, to_col, to_core, y, xh), own

    def map_pairs(to_way, to_col):
        return (
            (left_maps.at[to_way, 0, to_col], lefts.at[mine]),
            (right_maps.at[to_way, 0, to_col], rights.at[mine]),
            (kets.at[to_col], ketses.at[mine]),
        )

    def send_map(index, carried):
        to_way, to_col, device, own = chain(index)

        @pl.when(own)
        def _():
            for kind, (source, target) in enumerate(map_pairs(to_way, to_col)):
                pltpu.make_async_copy(source, target, map_recv.at[mine, kind]).start()

        @pl.when(jnp.logical_not(own))
        def _():
            for kind, (source, target) in enumerate(map_pairs(to_way, to_col)):
                remote(
                    source, target, map_send.at[index, kind], map_recv.at[mine, kind], device
                ).start()

        return carried

    def map_sent(index, carried):
        to_way, to_col, device, own = chain(index)

        @pl.when(jnp.logical_not(own))
        def _():
            for kind, (source, target) in enumerate(map_pairs(to_way, to_col)):
                remote(
                    source, target, map_send.at[index, kind], map_recv.at[mine, kind], device
                ).wait_send()

        return carried

    def send_rest():
        lax.fori_loop(0, 2, map_sent, 0)
        lax.fori_loop(2, 4, send_map, 0)

    on_early = is_worker & (way == mirror)
    lax.fori_loop(0, 2, send_map, 0)

    half = pl.ds(2 * xh, 2)
    at_home = (core == xl) & (xl == xh)

    def ket_copy(to_core):
        device = (z, core, to_core, y, xl)
        return remote(kets, row_kets.at[half], ket_send.at[to_core], ket_recv.at[xh], device)

    def ket_back():
        device = (z, core, 0, jnp.maximum(y - 1, 0), xl)
        return remote(kets.at[0], row_kets.at[4], ket_send.at[2], ket_recv.at[2], device)

    def edge_copy(edge, to_core):
        return remote(edge.at[0], env_entered, edge_send, env_recv, (z, core, to_core, y, xl))

    for to_core in range(2):

        @pl.when(at_home & (core == to_core))
        def _():
            pltpu.make_async_copy(kets, row_kets.at[half], ket_recv.at[xh]).start()

        @pl.when(jnp.logical_not(at_home & (core == to_core)))
        def _():
            ket_copy(to_core).start()

    sends_back = (core == 0) & (y > 0)
    gets_back = (core == 0) & (y < stations - 1)
    kets_back = (xh == 0) & (y > 0)

    @pl.when(kets_back)
    def _():
        ket_back().start()

    edges = ((left_edge, 0, 0), (right_edge, 1, stations - 1))
    for edge, to_core, y_of in edges:

        @pl.when((y == y_of) & (xh == xl) & at_home & (core == to_core))
        def _():
            pltpu.make_async_copy(edge.at[0], env_entered, env_recv).start()

        @pl.when((y == y_of) & (xh == xl) & jnp.logical_not(at_home & (core == to_core)))
        def _():
            edge_copy(edge, to_core).start()

    @pl.when(is_first & (way == 0))
    def _():
        entered[...] = top_edge[col]

    @pl.when(is_first & (way == 1))
    def _():
        entered[...] = bottom_edge[col]


    def slot_at(number):
        return number + way * (count - 1 - 2 * number)

    def prepare(step):
        ordered = slot_at(step)
        j = jnp.where(is_first, ordered, (mine + step) % count)
        number = j + way * (count - 1 - 2 * j)
        for kind, target in enumerate((lefts, rights, ketses)):
            arrived(target.at[j], map_recv.at[j, kind])
        layers[number] = even_rows(pair_values(ketses[j], picks[...]), turn[...])
        apart = dot(jnp.concatenate(thirds(lefts[j]), axis=0), select_one[:, 0:512])
        apart = apart[0:CHI] + (apart[CHI : 2 * CHI] + apart[2 * CHI : 3 * CHI])
        legs_of = symmetric([apart[:, leg * 128 : (leg + 1) * 128] for leg in range(4)])
        for leg, tile in enumerate(legs_of):
            high, mid, lowest = thirds(tile)
            for index, part in enumerate((high, mid, high, mid, lowest, high)):
                lanes = slice(index * 128, (index + 1) * 128)
                first[number, leg * CHI : (leg + 1) * CHI, lanes] = part
        high, mid, lowest = thirds(rights[j])
        main = dot_nt(select_two[...], padded((high, mid)))
        fine = dot_nt(select_two[...], padded((lowest,)))
        apart = main[:, 0:128] + (main[:, 128:256] + fine)
        legs_of = symmetric([apart[leg * 128 : (leg + 1) * 128] for leg in range(4)])
        for leg, tile in enumerate(legs_of):
            high, mid, lowest = thirds(tile)
            for copy in range(2):
                begin = leg * 256 + copy * 128
                second[number, begin : begin + 128, 0:128] = high
                second[number, begin : begin + 128, 128:256] = mid
            third[number, leg * 256 : leg * 256 + 128, :] = lowest
            third[number, leg * 256 + 128 : leg * 256 + 256, :] = high

    def side_copy(number, source):
        return remote(
            source,
            sides.at[way, place],
            row_send.at[number, 0],
            side_recv.at[way, place],
            env_member(slot_at(number)),
        )

    def side_own(number):
        slot = slot_at(number)
        same_core = (slot % 2 == xl) & (leader == core)
        return (low + slot // GROUP == z) & same_core & ((slot % GROUP) // 2 == xh)

    def out_copy(number):
        return remote(
            normed.at[number + 1],
            outs.at[way, col],
            row_send.at[number, 1],
            out_recv.at[way, col],
            member(slot_at(number), y, xh),
        )

    def send_sides(number, source):
        @pl.when(side_own(number))
        def _():
            pltpu.make_async_copy(
                source, sides.at[way, place], side_recv.at[way, place]
            ).start()

        @pl.when(jnp.logical_not(side_own(number)))
        def _():
            side_copy(number, source).start()

    def send_out(number, carried):
        own = slot_at(number) == mine

        @pl.when(own)
        def _():
            pltpu.make_async_copy(
                normed.at[number + 1], outs.at[way, col], out_recv.at[way, col]
            ).start()

        @pl.when(jnp.logical_not(own))
        def _():
            out_copy(number).start()

        return carried

    def hop():
        return remote(leaving, entered, hop_send, hop_recv, after)

    def tiles_of(value):
        return [value[leg * CHI : (leg + 1) * CHI] for leg in range(4)]

    def advance(number, carried):
        @pl.when(number == 0)
        def _():
            @pl.when(has_prev)
            def _():
                arrived(entered, hop_recv)

            came = unpack(entered[...])
            for leg, (tile, turned) in enumerate(zip(came, symmetric(came))):
                state[leg * CHI : (leg + 1) * CHI, :] = jnp.where(is_first, turned, tile)

        raw = is_first & (number == 0)
        closes = is_last & (number == count - 1)

        @pl.when(closes)
        def _():
            held = state[...]
            last_in[...] = pack(plain(tiles_of(held))) * nrm_scale(held)
            send_sides(number, last_in)

        current = state[...]
        scale = jnp.where(raw, 1.0, nrm_scale(current))
        renewed = apply_layer(
            current, scale, first, layers, second, third, number, joined, middle
        )
        normed[number] = pack(plain(tiles_of(current))) * scale
        state[...] = renewed

        @pl.when(number == count - 1)
        def _():
            final = state[...]
            leaving[...] = pack(tiles_of(final))

            @pl.when(has_next)
            def _():
                hop().start()

            normed[count] = pack(plain(tiles_of(final))) * nrm_scale(final)

        @pl.when(jnp.logical_not(closes))
        def _():
            send_sides(number, normed.at[number])

        @pl.when(number == count - 1)
        def _():
            lax.fori_loop(0, count, send_out, 0)

        return carried


    def column_at(number):
        return number + core * (3 - 2 * number)

    def env_legs(m, g, o, f):
        return pick(mirror, f, g), pick(core, m, o), pick(mirror, g, f), pick(core, o, m)

    def env_selects():
        for part in range(2):
            arrived(row_kets.at[pl.ds(2 * part, 2)], ket_recv.at[part])
        picks[...] = layer_picks(env_legs)

        @pl.when(core == 0)
        def _():
            row, lane = iota((2 * CHI, WIDE), 0), iota((2 * CHI, WIDE), 1)
            row = jnp.where(row >= CHI, row - CHI, row)
            for _ in range(3):
                lane = jnp.where(lane >= CHI, lane - CHI, lane)
            select_one[0 : 2 * CHI, 0:WIDE] = jnp.where(row == lane, 1.0, 0.0).astype(BF16)

        @pl.when(core == 1)
        def _():
            for leg in range(4):
                row, lane = iota((WIDE, WIDE), 0), iota((WIDE, WIDE), 1)
                for _ in range(3):
                    lane = jnp.where(lane >= CHI, lane - CHI, lane)
                select_one[:, leg * WIDE : (leg + 1) * WIDE] = jnp.where(
                    row == leg * CHI + lane, 1.0, 0.0
                ).astype(BF16)
                row, lane = iota((128, WIDE), 0), iota((128, WIDE), 1)
                select_two[leg * 128 : (leg + 1) * 128, :] = jnp.where(
                    (lane == leg * CHI + row) & (row < CHI), 1.0, 0.0
                ).astype(BF16)

    def forward(side, column):
        target = sides.at[side, column]
        device = (z, xl, 1 - core, y, xh)
        return remote(
            target, target, pass_send.at[side, column], side_recv.at[side, column], device
        )

    def back(side):
        device = (z, xl, core, jnp.maximum(y - 1, 0), xh)
        return remote(
            sides.at[side, 0], sides.at[side, 4], back_send.at[side], side_recv.at[side, 4], device
        )

    def take_side(side, column):
        arrived(sides.at[side, column], side_recv.at[side, column])

        @pl.when(core == leader)
        def _():
            forward(side, column).start()

        @pl.when(sends_back & (column == 0))
        def _():
            back(side).start()

    def env_fold(number):
        @pl.when(number == 0)
        def _():
            env_selects()

        column = column_at(number)
        take_side(mirror, column)
        coeffs[...] = layer_rows(row_kets[column], picks[...])
        early = jnp.concatenate(halves(sides[mirror, column]), axis=0)

        @pl.when(core == 0)
        def _():
            turned = lax.dot_general(
                early,
                select_one[0 : 2 * CHI, 0:WIDE],
                (((0,), (0,)), ((), ())),
                preferred_element_type=F32,
            )
            for leg in range(4):
                spread[leg] = turned[leg * CHI : (leg + 1) * CHI]

        @pl.when(core == 1)
        def _():
            apart = dot(early, select_one[...])
            for leg in range(4):
                lanes = slice(leg * WIDE, (leg + 1) * WIDE)
                spread[leg] = apart[0:CHI, lanes] + apart[CHI : 2 * CHI, lanes]

        fold_pair(spread, coeffs, env_folded, number)

    def env_prepare(number):
        column = column_at(number)
        take_side(1 - mirror, column)

        @pl.when(core == 0)
        def _():
            for leg, tile in enumerate(unpack(sides[1 - mirror, column])):
                high, lowest = halves(tile)
                both = jnp.concatenate(
                    [jnp.concatenate([high, lowest], axis=1), jnp.zeros((32, 256), BF16)], axis=0
                )
                env_second[number, leg * 256 : leg * 256 + 128, :] = both
                env_second[number, leg * 256 + 128 : leg * 256 + 256, :] = both

        @pl.when(core == 1)
        def _():
            late = padded(halves(sides[1 - mirror, column]))
            turned = dot_nt(select_two[...], late).astype(BF16)
            for leg in range(4):
                for copy in range(2):
                    begin = leg * 256 + copy * 128
                    env_second[number, begin : begin + 128, :] = turned[leg * 128 : leg * 128 + 128]

    def env_hop():
        device = (z, xl, core, jnp.clip(y + 1 - 2 * core, 0, stations - 1), xh)
        return remote(env_leaving, env_entered, env_send, env_recv, device)

    def over(number):
        column = column_at(number)
        wraps = column == 0
        slot = jnp.where(wraps, 3, jnp.maximum(column - 1, 0))
        y_to = jnp.where(wraps, jnp.maximum(y - 1, 0), y)
        return remote(
            env_normed.at[number],
            from_right.at[slot],
            over_send.at[number],
            over_recv.at[slot],
            (z, xl, 0, y_to, xh),
        )

    def sends_over(number):
        return (core == 1) & ((y > 0) | (column_at(number) > 0))

    def flipped(tile):
        square = jnp.concatenate([tile, jnp.zeros((32, 128), F32)], axis=0)
        return square.T[0:CHI, :]

    def env_advance(number):
        @pl.when(number == 0)
        def _():
            arrived(env_entered, env_recv)
            flips = station_first & (mirror == 1)

            @pl.when(jnp.logical_not(flips))
            def _():
                for leg, tile in enumerate(unpack(env_entered[...])):
                    state[leg * CHI : (leg + 1) * CHI, :] = tile

            @pl.when(flips)
            def _():
                for leg, tile in enumerate(unpack(env_entered[...])):
                    state[leg * CHI : (leg + 1) * CHI, :] = flipped(tile)

        raw = station_first & (number == 0)

        @pl.when(jnp.logical_not(station_last & (number >= 2)))
        def _():
            current = state[...]
            scale = jnp.where(raw, 1.0, nrm_scale(current))
            renewed = apply_pair(current, scale, env_folded, env_second, number, middle)
            env_normed[number] = pack(tiles_of(current)) * scale
            state[...] = renewed

        @pl.when(station_last & (number >= 2))
        def _():
            current = state[...]
            env_normed[number] = pack(tiles_of(current)) * nrm_scale(current)

        @pl.when(jnp.logical_not(station_last) & (number == 3))
        def _():
            env_leaving[...] = pack(tiles_of(state[...]))
            env_hop().start()

        @pl.when(core == 0)
        def _():
            from_left[number] = env_normed[number]

        @pl.when(sends_over(number))
        def _():
            over(number).start()


    @pl.when(jnp.logical_not(on_early))
    def _():
        send_rest()

    turn_at = jnp.where(at_edge, 4, 1)
    total = jnp.where(is_worker, 2 * count, 0)
    before_fold = jnp.where(is_late, count, total)

    def task(index, carried):
        @pl.when(on_early & (index == turn_at))
        def _():
            send_rest()

        folds = (index >= before_fold) & (index < before_fold + 4)
        on_env = index >= total + 4
        on_boundary = jnp.logical_not(folds) & jnp.logical_not(on_env)
        step = jnp.where(index < before_fold, index, index - 4)
        prepares = (is_first & (step % 2 == 0)) | (jnp.logical_not(is_first) & (step < count))

        @pl.when(on_boundary & prepares)
        def _():
            prepare(jnp.where(is_first, step // 2, jnp.clip(step, 0, count - 1)))

        @pl.when(on_boundary & jnp.logical_not(prepares))
        def _():
            begin = jnp.where(is_first, step // 2, 0)
            stop = jnp.where(is_first, begin + 1, jnp.where(step == count, count, 0))
            lax.fori_loop(begin, stop, advance, 0)

        @pl.when(folds)
        def _():
            env_fold(jnp.clip(index - before_fold, 0, 3))

        late = index - (total + 4)
        readies = (station_first & (late % 2 == 0)) | (
            jnp.logical_not(station_first) & (late < 4)
        )

        @pl.when(on_env & readies)
        def _():
            env_prepare(jnp.where(station_first, late // 2, jnp.clip(late, 0, 3)))

        @pl.when(on_env & jnp.logical_not(readies))
        def _():
            env_advance(jnp.where(station_first, late // 2, jnp.clip(late - 4, 0, 3)))

        return carried

    lax.fori_loop(0, total + 12, task, 0)


    lax.fori_loop(2, 4, map_sent, 0)

    @pl.when(has_next)
    def _():
        hop().wait_send()

    def row_sent(number, carried):
        @pl.when(jnp.logical_not(side_own(number)))
        def _():
            side_copy(number, normed.at[number]).wait_send()

        @pl.when(slot_at(number) != mine)
        def _():
            out_copy(number).wait_send()

        return carried

    lax.fori_loop(0, total // 2, row_sent, 0)

    for to_core in range(2):

        @pl.when(jnp.logical_not(at_home & (core == to_core)))
        def _():
            ket_copy(to_core).wait_send()

    @pl.when(kets_back)
    def _():
        ket_back().wait_send()

    for edge, to_core, y_of in edges:

        @pl.when((y == y_of) & (xh == xl) & jnp.logical_not(at_home & (core == to_core)))
        def _():
            edge_copy(edge, to_core).wait_send()

    for side in range(2):

        @pl.when(core == leader)
        def _():
            for column in range(4):
                forward(side, column).wait_send()

        @pl.when(sends_back)
        def _():
            back(side).wait_send()

    @pl.when(jnp.logical_not(station_last))
    def _():
        env_hop().wait_send()

    for number in range(4):

        @pl.when(sends_over(number))
        def _():
            over(number).wait_send()

    for direction in range(2):
        for column in range(2):
            arrived(outs.at[direction, column], out_recv.at[direction, column])

    @pl.when(gets_back)
    def _():
        for direction in range(2):
            arrived(sides.at[direction, 4], side_recv.at[direction, 4])
        arrived(row_kets.at[4], ket_recv.at[2])

    @pl.when(core == 0)
    def _():
        for slot in range(3):
            arrived(from_right.at[slot], over_recv.at[slot])

    @pl.when(gets_back)
    def _():
        arrived(from_right.at[3], over_recv.at[3])


def run_sweep(kets, left_maps, right_maps, top_edge, bottom_edge, left_edge, right_edge):
    vmem = pl.BlockSpec(memory_space=pltpu.VMEM)
    anywhere = pl.BlockSpec(memory_space=pl.ANY)
    column = (CHI, WIDE)
    most = 2 * GROUP
    dma = pltpu.SemaphoreType.DMA
    return pl.pallas_call(
        sweep_kernel,
        out_shape=(
            jax.ShapeDtypeStruct((2, 2) + column, F32),
            jax.ShapeDtypeStruct((2, 5) + column, F32),
            jax.ShapeDtypeStruct((5, 32, 128), F32),
            jax.ShapeDtypeStruct((4,) + column, F32),
            jax.ShapeDtypeStruct((4,) + column, F32),
        ),
        in_specs=[vmem, anywhere, anywhere] + [vmem] * 4,
        out_specs=(vmem,) * 5,
        scratch_shapes=[
            pltpu.VMEM((2, 32, 128), F32),
            pltpu.VMEM((most,) + column, F32),
            pltpu.VMEM((most,) + column, F32),
            pltpu.VMEM((most, 32, 128), F32),
            pltpu.VMEM((WIDE, 4 * WIDE), BF16),
            pltpu.VMEM((512, WIDE), BF16),
            pltpu.VMEM((4,) + column, F32),
            pltpu.VMEM((64, WIDE), F32),
            pltpu.VMEM((1024, 32), BF16),
            pltpu.VMEM((256, 256), BF16),
            pltpu.VMEM((most, 256, 128), F32),
            pltpu.VMEM((most, WIDE, 768), BF16),
            pltpu.VMEM((WIDE, 512), F32),
            pltpu.VMEM((most, 1024, 256), BF16),
            pltpu.VMEM((most, 1024, 128), BF16),
            pltpu.VMEM((4, 16 * CHI, 2 * WIDE), BF16),
            pltpu.VMEM((4, 1024, 256), BF16),
            pltpu.VMEM((WIDE, 2048), BF16),
            pltpu.VMEM(column, F32),
            pltpu.VMEM(column, F32),
            pltpu.VMEM((WIDE, 128), F32),
            pltpu.VMEM((most + 1,) + column, F32),
            pltpu.VMEM(column, F32),
            pltpu.VMEM(column, F32),
            pltpu.VMEM(column, F32),
            pltpu.VMEM((4,) + column, F32),
            dma((4, 3)),
            dma((most, 3)),
            dma,
            dma,
            dma((most, 2)),
            dma((2, 2)),
            dma((2, 5)),
            dma((3,)),
            dma((3,)),
            dma,
            dma((2, 4)),
            dma((2,)),
            dma,
            dma,
            dma((4,)),
            dma((4,)),
        ],
        compiler_params=pltpu.CompilerParams(
            collective_id=0, has_side_effects=True, vmem_limit_bytes=67043328
        ),
        name="sweep",
    )(kets, left_maps, right_maps, top_edge, bottom_edge, left_edge, right_edge)


def dot_general(left, right, dims):
    return lax.dot_general(left, right, (dims, ((), ())), preferred_element_type=F32)


def pad_rows(value):
    return jnp.concatenate([value, jnp.zeros((32, value.shape[1]), value.dtype)], axis=0)


def swap_legs(entry):
    return (entry & 0b10101) | ((entry >> 3) & 1) << 1 | ((entry >> 1) & 1) << 3


def open_site(ket, legs_at, wide, opened):
    def body(block, carried):
        begin = pl.multiple_of(block * 8, 8)
        half_done = {}
        for bra in range(8):
            u2, m2, d2 = bra >> 2, (bra >> 1) & 1, bra & 1
            tiles = []
            for top in range(8):
                u, m, d = top >> 2, (top >> 1) & 1, top & 1
                row = (2 * m + m2) * 4 + 2 * u + u2
                lane = (2 * d + d2) * 128
                tiles.append(wide[pl.ds(row * CHI + begin, 8), lane : lane + 128])
            for state in range(2):
                for out in range(2):
                    total = None
                    for top in range(8):
                        at = state * 16 + legs_at(top >> 2, (top >> 1) & 1, top & 1, out)
                        term = ket[at : at + 1, :] * tiles[top]
                        total = term if total is None else total + term
                    half_done[state, out, bra] = total
        for state in range(2):
            for out in range(2):
                for other in range(2):
                    for out2 in range(2):
                        total = None
                        for bra in range(8):
                            at = other * 16 + legs_at(bra >> 2, (bra >> 1) & 1, bra & 1, out2)
                            term = ket[at : at + 1, :] * half_done[state, out, bra]
                            total = term if total is None else total + term
                        row = (2 * out + out2) * CHI
                        opened[state * 2 + other, pl.ds(row + begin, 8), :] = total
        return carried

    lax.fori_loop(0, CHI // 8, body, 0)


def energy_kernel(
    term_rows,
    term_bonds,
    term_ops,
    operators,
    all_sides,
    all_kets,
    all_left,
    all_right,
    shares,
    wide,
    opened,
    closing,
    density,
    ket,
    sides,
    row_kets,
    from_left,
    from_right,
    fetch,
):
    way = lax.axis_index("rows_2")
    row_here = (
        lax.axis_index("rows_0") * GROUP + lax.axis_index("cols_1") * 2 + lax.axis_index("rows_1")
    )
    first = lax.axis_index("cols_0") * 4
    planes = lax.axis_size("rows_0")
    mirror = jnp.where(lax.axis_index("rows_0") >= planes // 2, 1, 0)

    def take_ket(column):
        for entry in range(32):
            ket[entry : entry + 1, :] = jnp.where(
                mirror == 1,
                row_kets[column, swap_legs(entry) : swap_legs(entry) + 1, :],
                row_kets[column, entry : entry + 1, :],
            )

    shares[...] = jnp.zeros((8, 128), F32)

    def hits(term, column):
        here = (term_rows[term] == row_here) & (term_bonds[term] == first + column)
        return here & (way == 0)

    def column_body(column, carried):
        count = 0
        for term in range(TERMS):
            count = count + jnp.where(hits(term, column), 1, 0)

        @pl.when(count > 0)
        def _():
            copies = [
                pltpu.make_async_copy(
                    all_sides.at[:, pl.ds(column, 2)], sides, fetch.at[0]
                ),
                pltpu.make_async_copy(all_kets.at[pl.ds(column, 2)], row_kets, fetch.at[1]),
                pltpu.make_async_copy(all_left.at[column], from_left, fetch.at[2]),
                pltpu.make_async_copy(all_right.at[column], from_right, fetch.at[3]),
            ]
            for copy in copies:
                copy.start()
            for copy in copies:
                copy.wait()

            high, low = halves(sides[mirror, 0])
            both = jnp.concatenate([high, low], axis=0)
            state_high, state_low = halves(jnp.concatenate(unpack(from_left[...]), axis=1))
            tn = ((0,), (0,))
            joined = dot_general(
                both, jnp.concatenate([state_high, state_high], axis=0), tn
            ) + dot_general(both, jnp.concatenate([state_low, state_low], axis=0), tn)
            below_high, below_low = halves(jnp.concatenate(unpack(sides[1 - mirror, 0]), axis=1))
            main = jnp.concatenate([pad_rows(below_high), pad_rows(below_high)], axis=0)
            fine = jnp.concatenate([pad_rows(below_low), pad_rows(below_low)], axis=0)
            for leg in range(4):
                part = jnp.concatenate(halves(joined[:, leg * 128 : (leg + 1) * 128]), axis=1)
                wide[leg * WIDE : (leg + 1) * WIDE, :] = dot(part, main) + dot(part, fine)
            take_ket(0)
            open_site(
                ket,
                lambda u, m, d, out: u * 8 + m * 4 + d * 2 + out,
                wide,
                opened,
            )

            above = jnp.concatenate(unpack(sides[mirror, 1]), axis=0)
            both = jnp.concatenate(halves(above), axis=1)
            state_high, state_low = halves(jnp.concatenate(unpack(from_right[...]), axis=1))
            state_high, state_low = pad_rows(state_high), pad_rows(state_low)
            joined = dot(both, jnp.concatenate([state_high, state_high], axis=0)) + dot(
                both, jnp.concatenate([state_low, state_low], axis=0)
            )
            below_high, below_low = halves(
                jnp.concatenate([pad_rows(tile) for tile in unpack(sides[1 - mirror, 1])], axis=0)
            )
            main = jnp.concatenate([below_high, below_high], axis=1)
            fine = jnp.concatenate([below_low, below_low], axis=1)
            for leg in range(4):
                part = jnp.concatenate(halves(joined[:, leg * 128 : (leg + 1) * 128]), axis=1)
                wide[leg * WIDE : (leg + 1) * WIDE, :] = dot_nt(part, main) + dot_nt(part, fine)
            take_ket(1)
            open_site(
                ket,
                lambda u, m, d, out: u * 8 + out * 4 + d * 2 + m,
                wide,
                closing,
            )

            for pair in range(4):
                for other in range(4):
                    product = opened[pair] * closing[other]
                    at = pair * 4 + other
                    density[at : at + 1, :] = jnp.sum(product, axis=0, keepdims=True)
            rho = jnp.sum(density[...], axis=1, keepdims=True)
            index = iota((16, 1), 0)
            diagonal = (index == 0) | (index == 3) | (index == 12) | (index == 15)
            trace = jnp.sum(jnp.where(diagonal, rho, 0.0), axis=0, keepdims=True)
            spread = jnp.sqrt(jnp.sum(rho * rho, axis=0, keepdims=True))
            bottom = jnp.maximum(jnp.abs(trace), 0.25 * spread)

            def term_body(term, kept):
                @pl.when(hits(term, column))
                def _():
                    chosen = jnp.zeros((16, 1), F32)
                    for entry in range(16):
                        chosen = jnp.where(
                            index == entry, operators[term_ops[term], entry], chosen
                        )
                    value = jnp.sum(chosen * rho, axis=0, keepdims=True) / bottom
                    lane = iota((8, 128), 1)
                    shares[...] = jnp.where(lane == term, value, shares[...])

                return kept

            lax.fori_loop(0, TERMS, term_body, 0)

        return carried

    lax.fori_loop(0, 4, column_body, 0)


def run_energies(term_rows, term_bonds, term_ops, operators, sides, row_kets, lefts, rights):
    vmem = pl.BlockSpec(memory_space=pltpu.VMEM)
    smem = pl.BlockSpec(memory_space=pltpu.SMEM)
    return pl.pallas_call(
        energy_kernel,
        out_shape=jax.ShapeDtypeStruct((8, 128), F32),
        in_specs=[smem] * 4 + [pl.BlockSpec(memory_space=pl.ANY)] * 4,
        out_specs=vmem,
        scratch_shapes=[
            pltpu.VMEM((16 * CHI, 512), F32),
            pltpu.VMEM((4, WIDE, 128), F32),
            pltpu.VMEM((4, WIDE, 128), F32),
            pltpu.VMEM((16, 128), F32),
            pltpu.VMEM((32, 128), F32),
            pltpu.VMEM((2, 2, CHI, WIDE), F32),
            pltpu.VMEM((2, 32, 128), F32),
            pltpu.VMEM((CHI, WIDE), F32),
            pltpu.VMEM((CHI, WIDE), F32),
            pltpu.SemaphoreType.DMA((4,)),
        ],
        compiler_params=pltpu.CompilerParams(vmem_limit_bytes=67043328),
        name="energies",
    )(term_rows, term_bonds, term_ops, operators, sides, row_kets, lefts, rights)


def sum_kernel(shares, total, planes_in, plane_in, partial, send_one, recv_one, send_two, recv_two):
    z = lax.axis_index("rows_0")
    xl = lax.axis_index("rows_1")
    core = lax.axis_index("rows_2")
    y = lax.axis_index("cols_0")
    xh = lax.axis_index("cols_1")
    way = core
    place = y * 4 + xl * 2 + xh
    barrier = pltpu.get_barrier_semaphore()

    def greet(device):
        pl.semaphore_signal(barrier, inc=1, device_id=device, device_id_type=MESH)

    def along(step):
        return ((z + step) % 8, xl, core, y, xh)

    def within(step):
        other = (place * 2 + way + step) % 32
        return (z, (other // 4) % 2, other % 2, other // 8, (other // 2) % 2)

    for step in range(1, 8):
        greet(along(step))
    for step in range(1, 32):
        greet(within(step))
    pl.semaphore_wait(barrier, 38)

    def first(step):
        return pltpu.make_async_remote_copy(
            src_ref=shares,
            dst_ref=planes_in.at[z],
            send_sem=send_one.at[step],
            recv_sem=recv_one.at[z],
            device_id=along(step),
            device_id_type=MESH,
        )

    def second(step):
        return pltpu.make_async_remote_copy(
            src_ref=partial,
            dst_ref=plane_in.at[place],
            send_sem=send_two.at[step],
            recv_sem=recv_two.at[place],
            device_id=within(step),
            device_id_type=MESH,
        )

    @pl.when(way == 0)
    def _():
        for step in range(1, 8):
            first(step).start()
        pltpu.make_async_copy(shares, planes_in.at[z], recv_one.at[z]).start()
        added = None
        for plane in range(8):
            target = planes_in.at[plane]
            pltpu.make_async_copy(target, target, recv_one.at[plane]).wait()
        for plane in range(8):
            added = planes_in[plane] if added is None else added + planes_in[plane]
        partial[...] = added
        for step in range(1, 32):
            second(step).start()
        pltpu.make_async_copy(partial, plane_in.at[place], recv_two.at[place]).start()

    for other in range(16):
        target = plane_in.at[other]
        pltpu.make_async_copy(target, target, recv_two.at[other]).wait()
    added = None
    for other in range(16):
        added = plane_in[other] if added is None else added + plane_in[other]
    total[...] = added[0:1, 0:TERMS]

    @pl.when(way == 0)
    def _():
        for step in range(1, 8):
            first(step).wait_send()
        for step in range(1, 32):
            second(step).wait_send()


def run_sum(shares):
    vmem = pl.BlockSpec(memory_space=pltpu.VMEM)
    return pl.pallas_call(
        sum_kernel,
        out_shape=jax.ShapeDtypeStruct((1, TERMS), F32),
        in_specs=[vmem],
        out_specs=vmem,
        scratch_shapes=[
            pltpu.VMEM((8, 8, 128), F32),
            pltpu.VMEM((16, 8, 128), F32),
            pltpu.VMEM((8, 128), F32),
            pltpu.SemaphoreType.DMA((8,)),
            pltpu.SemaphoreType.DMA((8,)),
            pltpu.SemaphoreType.DMA((32,)),
            pltpu.SemaphoreType.DMA((16,)),
        ],
        compiler_params=pltpu.CompilerParams(
            collective_id=2, has_side_effects=True, vmem_limit_bytes=67043328
        ),
        name="shares_sum",
    )(shares)


def shards(
    kets,
    left_maps,
    right_maps,
    top_edge,
    bottom_edge,
    left_edge,
    right_edge,
    term_rows,
    term_bonds,
    term_ops,
    operators,
):
    outs, sides, row_kets, lefts, rights = run_sweep(
        kets[0], left_maps, right_maps, top_edge, bottom_edge, left_edge, right_edge
    )
    shares = run_energies(
        term_rows, term_bonds, term_ops, operators, sides, row_kets, lefts, rights
    )
    energies = run_sum(shares).reshape(TERMS)
    return (outs[0][None], outs[1][None], energies)


def solution(mesh):
    torus = Mesh(
        mesh.devices.reshape(8, 2, 2, 4, 2), ("rows_0", "rows_1", "rows_2", "cols_0", "cols_1")
    )
    placed = (
        P(ROWS, COLS, None),
        P(None, ROWS, COLS, None, None),
        P(None, ROWS, COLS, None, None),
        P(COLS, None, None),
        P(COLS, None, None),
        P(ROWS, None, None),
        P(ROWS, None, None),
        P(),
        P(),
        P(),
        P(),
    )
    return jax.shard_map(
        shards,
        mesh=torus,
        in_specs=placed,
        out_specs=(P(ROWS, COLS, None, None), P(ROWS, COLS, None, None), P()),
        check_vma=False,
    )
```
